512 devices in a mesh: row: 64 (over y_hi, z, core), head: 8 (over x, y_lo).
Axes of the slice: x: 4, y: 4 (y_hi: 2, y_lo: 2; y = y_hi * 2 + y_lo), z: 16, core: 2. Of those that a mesh axis runs over, the one named last changes fastest.
Arguments:
- pair_input: bfloat16 [512, 512, 128], P(('row', 'head')), may hold values from -6 to 6
- cotangent: bfloat16 [512, 512, 128], P(('row', 'head')), may hold values from -24 to 24
- residue_mask: int32 [512], replicated, may hold values from 0 to 1, as said below
- norm_gain: float32 [2, 128], replicated, may hold values from 0.5 to 1.5
- norm_shift: float32 [2, 128], replicated, may hold values from -3 to 3
- proj_weights: bfloat16 [2, 4, 128, 128], replicated, may hold values from -0.5 to 0.5
- gate_bias: float32 [2, 128], replicated, may hold values from -4 to 4
- out_weights: bfloat16 [2, 128, 128], replicated, may hold values from -1.0546875 to 1.0546875
- bias_weights: bfloat16 [2, 128, 4], replicated, may hold values from -1.06066017 to 1.06066017
Outputs:
- pair_grad: float32 [512, 512, 128], P(('row', 'head'))
- proj_grad: float32 [2, 4, 128, 128], replicated
- gate_bias_grad: float32 [2, 128], replicated
- out_grad: float32 [2, 128, 128], replicated
- bias_weight_grad: float32 [2, 128, 4], replicated
- gain_grad: float32 [2, 128], replicated
- shift_grad: float32 [2, 128], replicated
The draws below stay inside these ranges and needn't reach their ends.
Inputs may be any that keep to these rules, and one draw needn't show every extreme that they name: `residue_mask`: 1 for the first residues of the crop and 0 for the padding after them; at least half of the 512 residues are 1.
All inputs are finite; a program needn't handle non-finite values.
Results may differ from the reference program's by a relative error of at most 0.02.
The reference program's roundings to bfloat16 on the way count: a program that leaves them out, or rounds other values in their place, can miss the bound.
Values may be sent and summed in bfloat16 or wider, within the bound.
No kernel may reach another device: no remote copies, remote signals or barrier semaphores. Data moves between devices by JAX's collectives and lax.ppermute only.
A program may use at most 64 MiB of HBM per device.

```python
import math
import jax
import jax.numpy as jnp
from jax import lax

PAIR = 128
HEADS = 4
HDIM = 32
ROW_DEV = 1
NRES = 512
N_ROW = 64
N_HEAD = 8


def draw_residue_mask(key, part):
    length = jax.random.randint(key, (), NRES // 2, NRES + 1)
    return (jnp.arange(NRES) < length).astype(jnp.int32)


def draw_bias_weights(key, part):
    base = jnp.clip(jax.random.normal(key, (2, PAIR, HEADS), jnp.float32), -4.0, 4.0) / math.sqrt(PAIR)
    return base.astype(jnp.bfloat16)


def spiked(result, own_key, source, target, shards_of, factor):
    def block_of(dim):
        return (jnp.arange(result.shape[dim]) // (result.shape[dim] // shards_of)).reshape((-1,) + (1,) * (result.ndim - 1 - dim))

    first = jax.random.permutation(own_key, shards_of)[block_of(target)]
    other_side = (block_of(target) + shards_of // 2) % shards_of
    return jnp.where((block_of(source) == first) | (block_of(source) == other_side), factor * result, result)


def block_levels(key, shape, split, smallest, largest):
    factor_of, own = 1.0, jax.random.fold_in(key, 6)
    for dim, parts in split:
        steps = jnp.exp(jax.random.uniform(jax.random.fold_in(own, dim), (parts,), jnp.float32, smallest / len(split), largest / len(split)))
        factor_of = factor_of * jnp.repeat(steps, shape[dim] // parts).reshape([-1 if axis == dim else 1 for axis in range(len(shape))])
    return factor_of


def scatter_about(rng, shape, deviation, limit, pieces=(), kind=jnp.bfloat16):
    factor_of = block_levels(rng, shape, pieces, -0.22, 0.18) if pieces else 1.0
    values = jax.random.normal(rng, shape, jnp.float32) * deviation * factor_of
    return jnp.minimum(jnp.maximum(values, -limit), limit).astype(kind)


def gaussian_with(own_key, dims, spread, most, pieces, heavy, held_as=jnp.bfloat16):
    drawn = spread * jax.random.normal(own_key, dims, jnp.float32)
    if pieces:
        drawn = drawn * block_levels(own_key, dims, pieces, -0.22, 0.18)
    return jnp.clip(spiked(drawn, jax.random.fold_in(own_key, 3), *heavy), -most, most).astype(held_as)


def setup_inputs(seed: int = 0) -> dict:
    key_of = jax.random.split(jax.random.key(seed), 10)
    return {
        "pair_input": scatter_about(key_of[0], (NRES, NRES, PAIR), 1.0, 6.0, ((0, 512),)),
        "cotangent": gaussian_with(key_of[1], (NRES, NRES, PAIR), 1.0, 24.0, ((0, 512),), (0, 2, 128, 5.5)),
        "residue_mask": draw_residue_mask(jax.random.fold_in(key_of[9], 71), 0),
        "norm_gain": jnp.clip(1.0 + 0.1 * jax.random.normal(key_of[3], (2, PAIR), jnp.float32), 0.5, 1.5),
        "norm_shift": scatter_about(key_of[4], (2, PAIR), 0.5, 3.0, (), jnp.float32),
        "proj_weights": scatter_about(key_of[5], (2, 4, PAIR, HEADS * HDIM), PAIR ** -0.5, 0.5),
        "gate_bias": scatter_about(key_of[6], (2, HEADS * HDIM), 1.0, 4.0, (), jnp.float32),
        "out_weights": scatter_about(key_of[7], (2, HEADS * HDIM, PAIR), (2.0 / (HEADS * HDIM) ** 0.5), 1.0546875),
        "bias_weights": draw_bias_weights(jax.random.fold_in(key_of[9], 71), 0),
    }


EPS = 1e-05
MASKED = 1000000000.0

def as_float(values):
    return values.astype(jnp.float32)

def to_half(values):
    return lax.optimization_barrier(values.astype(jnp.bfloat16))

def layer_norm(values, norm_scale, norm_offset):
    floats = as_float(values)
    centred = floats - lax.optimization_barrier(jnp.mean(floats, axis=-1, keepdims=True))
    inverse = lax.rsqrt(lax.optimization_barrier(jnp.mean(centred * centred, axis=-1, keepdims=True)) + EPS)
    normed = centred * inverse
    return (normed, inverse, to_half(normed * norm_scale + norm_offset))

def norm_backward(grad_normal, normed, inverse, norm_scale):
    grad_hat = grad_normal * norm_scale
    first_mean = lax.optimization_barrier(jnp.mean(grad_hat, axis=-1, keepdims=True))
    second_mean = lax.optimization_barrier(jnp.mean(grad_hat * normed, axis=-1, keepdims=True))
    return inverse * (grad_hat - first_mean - normed * second_mean)

def softmax_rows(logits):
    shifted = logits - lax.optimization_barrier(jnp.max(logits, axis=-1, keepdims=True))
    weights = jnp.exp(shifted)
    return weights / lax.optimization_barrier(jnp.sum(weights, axis=-1, keepdims=True))

def triangle_block(pair_values, grad_output, key_bias, params):
    norm_scale, norm_offset, projection, gate_offset, out_proj, bias_proj = params
    query_scale = 1.0 / math.sqrt(HDIM)
    inner_width = HEADS * HDIM
    normed, inverse, normal_in = layer_norm(pair_values, norm_scale, norm_offset)
    pair_bias = as_float(to_half(jnp.einsum('jkc,ch->hjk', as_float(normal_in), as_float(bias_proj))))
    class_ids = jnp.arange(NRES) // ROW_DEV % N_HEAD
    class_hot = (class_ids[None, :] == jnp.arange(N_HEAD)[:, None]).astype(jnp.float32)
    split_shape = (HEADS, N_ROW, N_HEAD, ROW_DEV)

    def one_row(totals, inputs):
        row_in, row_grad = inputs
        queries = to_half(jnp.dot(row_in, projection[0], preferred_element_type=jnp.float32) * query_scale)
        key_rows = to_half(jnp.dot(row_in, projection[1], preferred_element_type=jnp.float32))
        value_rows = to_half(jnp.dot(row_in, projection[2], preferred_element_type=jnp.float32))
        gate_values = jax.nn.sigmoid(jnp.dot(row_in, projection[3], preferred_element_type=jnp.float32) + gate_offset)
        head_query = as_float(queries).reshape(NRES, HEADS, HDIM).transpose(1, 0, 2)
        head_key = as_float(key_rows).reshape(NRES, HEADS, HDIM).transpose(1, 0, 2)
        head_value = as_float(value_rows).reshape(NRES, HEADS, HDIM).transpose(1, 0, 2)
        logits = jnp.einsum('hjd,hkd->hjk', head_query, head_key) + pair_bias + key_bias
        soft_weights = softmax_rows(logits)
        weights_half = as_float(to_half(soft_weights))
        attended = jnp.einsum('hjk,hkd->jhd', weights_half, head_value).reshape(NRES, inner_width)
        gated_out = to_half(gate_values * attended)
        update = to_half(jnp.dot(gated_out, out_proj, preferred_element_type=jnp.float32))
        grad_gated = jnp.dot(row_grad, out_proj.T, preferred_element_type=jnp.float32)
        grad_att = to_half(grad_gated * gate_values)
        grad_pre = to_half(grad_gated * attended * gate_values * (1.0 - gate_values))
        head_grad = as_float(grad_att).reshape(NRES, HEADS, HDIM).transpose(1, 0, 2)
        grad_weights = jnp.einsum('hjd,hkd->hjk', head_grad, head_value)
        grad_logits = soft_weights * (grad_weights - lax.optimization_barrier(jnp.sum(soft_weights * grad_weights, axis=-1, keepdims=True)))
        logits_half = as_float(to_half(grad_logits))
        grad_queries = to_half(jnp.einsum('hjk,hkd->jhd', logits_half, head_key) * query_scale).reshape(NRES, inner_width)
        blocks_logit = logits_half.reshape(split_shape + (NRES,))
        blocks_query = head_query.reshape(split_shape + (HDIM,))
        blocks_weight = weights_half.reshape(split_shape + (NRES,))
        blocks_grad = head_grad.reshape(split_shape + (HDIM,))
        grad_keys = to_half(jnp.einsum('hbcsk,hbcsd->ckhd', blocks_logit, blocks_query)).reshape(N_HEAD, NRES, inner_width)
        grad_values = to_half(jnp.einsum('hbcsk,hbcsd->ckhd', blocks_weight, blocks_grad)).reshape(N_HEAD, NRES, inner_width)
        key_part = jnp.einsum('cke,fe->ckf', as_float(grad_keys), as_float(projection[1]))
        key_part = key_part + jnp.einsum('cke,fe->ckf', as_float(grad_values), as_float(projection[2]))
        query_part = jnp.dot(grad_queries, projection[0].T, preferred_element_type=jnp.float32)
        query_part = query_part + jnp.dot(grad_pre, projection[3].T, preferred_element_type=jnp.float32)
        partial_value = to_half(key_part + class_hot[:, :, None] * query_part[None])
        grad_row = lax.optimization_barrier(jnp.sum(as_float(partial_value), axis=0))
        bias_sum, grad_qw, grad_kw, grad_vw, grad_gw, grad_ow, grad_gate = totals
        new_totals = (bias_sum + grad_logits, grad_qw + jnp.dot(row_in.T, grad_queries, preferred_element_type=jnp.float32), grad_kw + jnp.einsum('nc,gne->ce', as_float(row_in), as_float(grad_keys)), grad_vw + jnp.einsum('nc,gne->ce', as_float(row_in), as_float(grad_values)), grad_gw + jnp.dot(row_in.T, grad_pre, preferred_element_type=jnp.float32), grad_ow + jnp.dot(gated_out.T, row_grad, preferred_element_type=jnp.float32), grad_gate + lax.optimization_barrier(jnp.sum(as_float(grad_pre), axis=0)))
        return (new_totals, (update, grad_row))
    initial = (jnp.zeros((HEADS, NRES, NRES), jnp.float32), jnp.zeros((PAIR, inner_width), jnp.float32), jnp.zeros((PAIR, inner_width), jnp.float32), jnp.zeros((PAIR, inner_width), jnp.float32), jnp.zeros((PAIR, inner_width), jnp.float32), jnp.zeros((inner_width, PAIR), jnp.float32), jnp.zeros((inner_width,), jnp.float32))
    totals, (updates, grad_rows) = lax.scan(one_row, initial, (normal_in, grad_output))
    bias_sum, grad_qw, grad_kw, grad_vw, grad_gw, grad_ow, grad_gate = totals
    bias_half = as_float(to_half(bias_sum))
    grad_normal = grad_rows + jnp.einsum('hjk,ch->jkc', bias_half, as_float(bias_proj))
    grad_bias_weights = jnp.einsum('jkc,hjk->ch', as_float(normal_in), bias_half)
    grad_pair = norm_backward(grad_normal, normed, inverse, norm_scale)
    grad_scale = lax.optimization_barrier(jnp.sum(grad_normal * normed, axis=(0, 1)))
    grad_offset = lax.optimization_barrier(jnp.sum(grad_normal, axis=(0, 1)))
    weight_grads = (jnp.stack([grad_qw, grad_kw, grad_vw, grad_gw]), grad_gate, grad_ow, grad_bias_weights, grad_scale, grad_offset)
    return (updates, grad_pair, weight_grads)

def reference(pair_input, cotangent, residue_mask, norm_gain, norm_shift, proj_weights, gate_bias, out_weights, bias_weights):
    key_bias = (as_float(residue_mask) - 1.0) * MASKED
    params = [(norm_gain[which], norm_shift[which], proj_weights[which], gate_bias[which], out_weights[which], bias_weights[which]) for which in range(2)]
    updates, unused_grad, unused_weights = triangle_block(pair_input, jnp.zeros_like(cotangent), key_bias, params[0])
    after_first = to_half(as_float(pair_input) + as_float(updates))
    flipped = jnp.transpose(after_first, (1, 0, 2))
    flipped_grad = jnp.transpose(cotangent, (1, 0, 2))
    unused_updates, end_block, end_weights = triangle_block(flipped, flipped_grad, key_bias, params[1])
    end_grad = jnp.transpose(to_half(end_block), (1, 0, 2))
    grad_after = as_float(cotangent) + as_float(end_grad)
    later_updates, start_block, start_weights = triangle_block(pair_input, to_half(grad_after), key_bias, params[0])
    pair_grad = grad_after + start_block
    stacked = [jnp.stack([start_part, end_part]) for start_part, end_part in zip(start_weights, end_weights)]
    return (pair_grad, stacked[0], stacked[1], stacked[2], stacked[3], stacked[4], stacked[5])
```

```python
import math

import jax
import jax.numpy as jnp
from jax import lax
from jax.sharding import Mesh
from jax.sharding import PartitionSpec as P

HEAD = ("head_0", "head_1")
ROW_HEAD = ("row", "head_0", "head_1")


EPS = 1e-05
MASKED = 1000000000.0
LANES = 128


def joined_along(parts, dim):
    parts = jnp.moveaxis(parts, 0, dim)
    dims = parts.shape
    return parts.reshape(*dims[:dim], dims[dim] * dims[dim + 1], *dims[dim + 2 :])


def from_everyone(x, axis):
    length = lax.axis_size(axis)
    return lax.all_to_all(jnp.broadcast_to(x[None], (length, *x.shape)), axis, 0, 0, tiled=True)


def gather_directly(x, axis, dim):
    return joined_along(from_everyone(x, axis), dim)


def split_up(x, dim, length):
    dims = x.shape
    parts = x.reshape(*dims[:dim], length, dims[dim] // length, *dims[dim + 1 :])
    return jnp.moveaxis(parts, dim, 0)


def sent_and_summed(x, axis, dim):
    length = lax.axis_size(axis)
    parts = lax.all_to_all(split_up(x, dim, length), axis, 0, 0, tiled=True)
    return jnp.sum(parts.astype(jnp.float32), axis=0)


def summed_everywhere(parts):
    flat = jnp.concatenate([part.reshape(-1) for part in parts])
    head_count = lax.axis_size(HEAD)
    row_count = lax.axis_size("row")
    head_rows = -(-flat.size // (head_count * LANES))
    padded = jnp.pad(flat, (0, head_count * head_rows * LANES - flat.size))
    arrived = lax.all_to_all(
        padded.reshape(head_count, head_rows, LANES), HEAD, 0, 0, tiled=True
    )
    summed = jnp.sum(arrived, axis=0)
    row_rows = -(-head_rows // (row_count * 4)) * 4
    summed = jnp.pad(summed, ((0, row_count * row_rows - head_rows), (0, 0)))
    arrived = lax.all_to_all(
        summed.reshape(row_count, row_rows, LANES), "row", 0, 0, tiled=True
    )
    own = jnp.sum(arrived, axis=0)
    over_row = from_everyone(own, "row").reshape(row_count * row_rows, LANES)[:head_rows]
    whole = from_everyone(over_row, HEAD).reshape(-1)
    results = []
    start = 0
    for part in parts:
        results.append(whole[start : start + part.size].reshape(part.shape))
        start += part.size
    return results


def joined_exchange(x, axis, axes, splits, concats):
    sizes = [lax.axis_size(a) for a in axes]
    parts = split_up(x, splits[0], sizes[0])
    parts = jnp.moveaxis(split_up(parts, splits[1] + 1, sizes[1]), 0, 1)
    inside = parts.shape[2:]
    parts = parts.reshape(-1, *inside)
    parts = lax.all_to_all(parts, axis, split_axis=0, concat_axis=0, tiled=True)
    parts = joined_along(parts.reshape(*sizes, *inside), concats[0] + 1)
    return joined_along(parts, concats[1])


def layer_norm(values, norm_scale, norm_offset):
    floats = values.astype(jnp.float32)
    centred = floats - jnp.mean(floats, axis=-1, keepdims=True)
    inverse = lax.rsqrt(jnp.mean(centred * centred, axis=-1, keepdims=True) + EPS)
    normed = centred * inverse
    return (normed, inverse, (normed * norm_scale + norm_offset).astype(jnp.bfloat16))


def norm_backward(grad_normal, normed, inverse, norm_scale):
    grad_hat = grad_normal * norm_scale
    first_mean = jnp.mean(grad_hat, axis=-1, keepdims=True)
    second_mean = jnp.mean(grad_hat * normed, axis=-1, keepdims=True)
    return inverse * (grad_hat - first_mean - normed * second_mean)


def class_columns(values, head_index, row_count, head_count, slab_rows):
    leading = values.shape[0]
    shaped = values.reshape(leading, row_count, head_count, slab_rows, values.shape[-1])
    picked = lax.dynamic_index_in_dim(shaped, head_index, axis=2, keepdims=False)
    return picked.reshape(leading, row_count * slab_rows, values.shape[-1])


def forward_block(pair_rows, key_bias, params, layout):
    norm_scale, norm_offset, projection, gate_offset, out_proj, bias_proj = params
    slab_rows, row_count, head_count, head_index = layout
    head_total = bias_proj.shape[1]
    inner_width = projection.shape[2]
    head_size = inner_width // head_total
    query_scale = 1.0 / math.sqrt(head_size)
    normed, inverse, normal_own = layer_norm(pair_rows, norm_scale, norm_offset)
    normal_rows = gather_directly(normal_own, HEAD, 0)
    bias_own = jnp.einsum(
        "snc,ch->hsn", normal_own, bias_proj, preferred_element_type=jnp.float32
    ).astype(jnp.bfloat16)
    bias_query = gather_directly(bias_own, "row", 1)
    normal_query = class_columns(normal_rows, head_index, row_count, head_count, slab_rows)
    block_rows = normal_query.shape[0]
    query_count = normal_query.shape[1]
    key_count = normal_rows.shape[1]
    queries = (
        jnp.dot(normal_query, projection[0], preferred_element_type=jnp.float32) * query_scale
    ).astype(jnp.bfloat16)
    joined_weights = jnp.concatenate([projection[1], projection[2]], axis=1)
    key_value = jnp.dot(normal_rows, joined_weights, preferred_element_type=jnp.float32).astype(
        jnp.bfloat16
    )
    gate_values = jax.nn.sigmoid(
        jnp.dot(normal_query, projection[3], preferred_element_type=jnp.float32) + gate_offset
    )
    head_queries = queries.reshape(block_rows, query_count, head_total, head_size).transpose(
        2, 0, 1, 3
    )
    head_pairs = key_value.reshape(block_rows, key_count, 2, head_total, head_size).transpose(
        2, 3, 0, 1, 4
    )

    def attend(inputs):
        query_head, key_head, value_head, bias_head = inputs
        logits = jnp.einsum(
            "rqd,rnd->rqn", query_head, key_head, preferred_element_type=jnp.float32
        )
        logits = logits + bias_head.astype(jnp.float32)[None] + key_bias
        largest = jnp.max(logits, axis=-1, keepdims=True)
        weights = jnp.exp(logits - largest)
        total = jnp.sum(weights, axis=-1, keepdims=True)
        soft_weights = weights / total
        attended = jnp.einsum(
            "rqn,rnd->rqd",
            soft_weights.astype(jnp.bfloat16),
            value_head,
            preferred_element_type=jnp.float32,
        )
        return ((largest + jnp.log(total))[..., 0], attended)

    log_totals, attended = lax.map(attend, (head_queries, head_pairs[0], head_pairs[1], bias_query))
    attended = attended.transpose(1, 2, 0, 3).reshape(block_rows, query_count, inner_width)
    gated_out = (gate_values * attended).astype(jnp.bfloat16)
    update = jnp.dot(gated_out, out_proj, preferred_element_type=jnp.float32).astype(jnp.bfloat16)
    saved_state = (
        normed,
        inverse,
        normal_own,
        normal_rows,
        normal_query,
        head_queries,
        head_pairs,
        bias_query,
        gate_values,
        attended,
        gated_out,
        log_totals,
    )
    return (saved_state, update)


def backward_block(saved_state, grad_query, key_bias, params, layout):
    norm_scale, norm_offset, projection, gate_offset, out_proj, bias_proj = params
    slab_rows, row_count, head_count, head_index = layout
    (
        normed,
        inverse,
        normal_own,
        normal_rows,
        normal_query,
        head_queries,
        head_pairs,
        bias_query,
        gate_values,
        attended,
        gated_out,
        log_totals,
    ) = saved_state
    channels = normal_own.shape[2]
    head_total, block_rows, query_count, head_size = head_queries.shape
    key_count = normal_rows.shape[1]
    inner_width = head_total * head_size
    query_scale = 1.0 / math.sqrt(head_size)
    grad_gated = jnp.dot(grad_query, out_proj.T, preferred_element_type=jnp.float32)
    grad_att = (grad_gated * gate_values).astype(jnp.bfloat16)
    grad_pre = (grad_gated * attended * gate_values * (1.0 - gate_values)).astype(jnp.bfloat16)
    head_grads = grad_att.reshape(block_rows, query_count, head_total, head_size).transpose(
        2, 0, 1, 3
    )

    def differentiate(inputs):
        total_head, query_head, key_head, value_head, bias_head, grad_head = inputs
        logits = jnp.einsum(
            "rqd,rnd->rqn", query_head, key_head, preferred_element_type=jnp.float32
        )
        logits = logits + bias_head.astype(jnp.float32)[None] + key_bias
        soft_weights = jnp.exp(logits - total_head[..., None])
        grad_weights = jnp.einsum(
            "rqd,rnd->rqn", grad_head, value_head, preferred_element_type=jnp.float32
        )
        grad_logits = soft_weights * (
            grad_weights - jnp.sum(soft_weights * grad_weights, axis=-1, keepdims=True)
        )
        logits_half = grad_logits.astype(jnp.bfloat16)
        grad_queries = (
            jnp.einsum("rqn,rnd->rqd", logits_half, key_head, preferred_element_type=jnp.float32)
            * query_scale
        ).astype(jnp.bfloat16)
        grad_keys = jnp.einsum(
            "rqn,rqd->rnd", logits_half, query_head, preferred_element_type=jnp.float32
        ).astype(jnp.bfloat16)
        grad_values = jnp.einsum(
            "rqn,rqd->rnd",
            soft_weights.astype(jnp.bfloat16),
            grad_head,
            preferred_element_type=jnp.float32,
        ).astype(jnp.bfloat16)
        return (grad_queries, grad_keys, grad_values, jnp.sum(grad_logits, axis=0))

    grad_queries, grad_keys, grad_values, grad_bias = lax.map(
        differentiate,
        (log_totals, head_queries, head_pairs[0], head_pairs[1], bias_query, head_grads),
    )
    grad_queries = grad_queries.transpose(1, 2, 0, 3).reshape(block_rows, query_count, inner_width)
    key_weights = projection[1].reshape(channels, head_total, head_size).transpose(1, 2, 0)
    value_weights = projection[2].reshape(channels, head_total, head_size).transpose(1, 2, 0)
    query_side = jnp.dot(grad_queries, projection[0].T, preferred_element_type=jnp.float32)
    query_side = query_side + jnp.dot(grad_pre, projection[3].T, preferred_element_type=jnp.float32)
    count = slab_rows * lax.axis_size(HEAD)
    term = jnp.einsum("hrnd,hdc->rnc", grad_keys, key_weights, preferred_element_type=jnp.float32)
    term = term + jnp.einsum(
        "hrnd,hdc->rnc", grad_values, value_weights, preferred_element_type=jnp.float32
    )
    shaped = term.reshape(count, row_count, head_count, slab_rows, channels)
    current = lax.dynamic_slice_in_dim(shaped, head_index, 1, 2)
    query_slice = query_side.reshape(count, row_count, 1, slab_rows, channels)
    shaped = lax.dynamic_update_slice_in_dim(shaped, current + query_slice, head_index, 2)
    grad_normal = sent_and_summed(
        shaped.reshape(count, key_count, channels).astype(jnp.bfloat16), HEAD, 0
    )
    bias_total = sent_and_summed(grad_bias.astype(jnp.bfloat16), "row", 1)
    bias_half = bias_total.astype(jnp.bfloat16)
    grad_normal = grad_normal + jnp.einsum(
        "hsn,ch->snc", bias_half, bias_proj, preferred_element_type=jnp.float32
    )
    grad_pair = norm_backward(grad_normal, normed, inverse, norm_scale)
    projection_grads = jnp.stack(
        [
            jnp.einsum(
                "rqc,rqe->ce", normal_query, grad_queries, preferred_element_type=jnp.float32
            ),
            jnp.einsum(
                "rnc,hrnd->chd", normal_rows, grad_keys, preferred_element_type=jnp.float32
            ).reshape(channels, inner_width),
            jnp.einsum(
                "rnc,hrnd->chd", normal_rows, grad_values, preferred_element_type=jnp.float32
            ).reshape(channels, inner_width),
            jnp.einsum("rqc,rqe->ce", normal_query, grad_pre, preferred_element_type=jnp.float32),
        ]
    )
    weight_grads = (
        projection_grads,
        jnp.sum(grad_pre.astype(jnp.float32), axis=(0, 1)),
        jnp.einsum("rqe,rqc->ec", gated_out, grad_query, preferred_element_type=jnp.float32),
        jnp.einsum("snc,hsn->ch", normal_own, bias_half, preferred_element_type=jnp.float32),
        jnp.sum(grad_normal * normed, axis=(0, 1)),
        jnp.sum(grad_normal, axis=(0, 1)),
    )
    return (grad_pair, weight_grads)


def to_queries(grad_rows, layout):
    slab_rows, row_count, head_count, head_index = layout
    channels = grad_rows.shape[2]
    shaped = grad_rows.reshape(slab_rows, row_count, head_count, slab_rows, channels)
    moved = lax.all_to_all(shaped, HEAD, split_axis=2, concat_axis=0, tiled=True)
    return moved.reshape(slab_rows * head_count, row_count * slab_rows, channels)


def local(
    pair_input,
    cotangent,
    residue_mask,
    norm_gain,
    norm_shift,
    proj_weights,
    gate_bias,
    out_weights,
    bias_weights,
):
    slab_rows = pair_input.shape[0]
    channels = pair_input.shape[2]
    row_count = lax.axis_size("row")
    head_count = lax.axis_size(HEAD)
    layout = (slab_rows, row_count, head_count, lax.axis_index(HEAD))
    key_bias = (residue_mask.astype(jnp.float32) - 1.0) * MASKED
    params = [
        (
            norm_gain[which],
            norm_shift[which],
            proj_weights[which],
            gate_bias[which],
            out_weights[which],
            bias_weights[which],
        )
        for which in range(2)
    ]
    first_state, first_update = forward_block(pair_input, key_bias, params[0], layout)
    returned = lax.all_to_all(
        first_update.reshape(slab_rows * head_count, row_count, 1, slab_rows, channels),
        HEAD,
        split_axis=0,
        concat_axis=2,
        tiled=True,
    )
    after_first = (
        pair_input.astype(jnp.float32)
        + returned.reshape(slab_rows, -1, channels).astype(jnp.float32)
    ).astype(jnp.bfloat16)
    joined = jnp.concatenate([after_first, cotangent], axis=2)
    moved = joined_exchange(
        joined.reshape(1, 1, slab_rows, row_count, head_count, slab_rows, 2 * channels),
        ROW_HEAD,
        ("row", HEAD),
        (3, 4),
        (0, 1),
    )
    flipped = moved.reshape(-1, slab_rows, 2 * channels).transpose(1, 0, 2)
    second_state, second_update = forward_block(
        flipped[:, :, :channels], key_bias, params[1], layout
    )
    second_grad, second_weights = backward_block(
        second_state, to_queries(flipped[:, :, channels:], layout), key_bias, params[1], layout
    )
    sent_back = joined_exchange(
        second_grad.astype(jnp.bfloat16).reshape(
            1, 1, slab_rows, row_count, head_count, slab_rows, channels
        ),
        ROW_HEAD,
        ("row", HEAD),
        (3, 4),
        (0, 1),
    )
    end_grad = sent_back.reshape(-1, slab_rows, channels).transpose(1, 0, 2)
    grad_after = cotangent.astype(jnp.float32) + end_grad.astype(jnp.float32)
    start_grad, first_weights = backward_block(
        first_state,
        to_queries(grad_after.astype(jnp.bfloat16), layout),
        key_bias,
        params[0],
        layout,
    )
    pair_grad = grad_after + start_grad
    combined = [
        jnp.stack([start_part, end_part])
        for start_part, end_part in zip(first_weights, second_weights)
    ]
    stacked = summed_everywhere(combined)
    return (pair_grad, stacked[0], stacked[1], stacked[2], stacked[3], stacked[4], stacked[5])


def solution(mesh):
    finer = Mesh(mesh.devices.reshape(mesh.shape["row"], 4, 2), ("row", "head_0", "head_1"))
    in_specs = (P(ROW_HEAD, None, None), P(ROW_HEAD, None, None), P(), P(), P(), P(), P(), P(), P())
    out_specs = (P(ROW_HEAD, None, None), P(), P(), P(), P(), P(), P())
    return jax.shard_map(local, mesh=finer, in_specs=in_specs, out_specs=out_specs, check_vma=False)
```

```python
import math

import jax
import jax.numpy as jnp
from jax import lax
from jax.sharding import Mesh
from jax.sharding import PartitionSpec as P

HEAD = ("head_0", "head_1")
ROW_HEAD = ("row", "head_0", "head_1")


EPS = 1e-05
MASKED = 1000000000.0
LANES = 128


def exchanged(parts, axis):
    return lax.all_to_all(parts, axis, split_axis=0, concat_axis=0, tiled=True)


def to_all(x, axis):
    return jnp.broadcast_to(x[None], (lax.axis_size(axis), *x.shape))


def layer_norm(values, norm_scale, norm_offset):
    floats = values.astype(jnp.float32)
    centred = floats - jnp.mean(floats, axis=-1, keepdims=True)
    inverse = lax.rsqrt(jnp.mean(centred * centred, axis=-1, keepdims=True) + EPS)
    normed = centred * inverse
    return (normed, inverse, (normed * norm_scale + norm_offset).astype(jnp.bfloat16))


def norm_backward(grad_normal, normed, inverse, norm_scale):
    grad_hat = grad_normal * norm_scale
    first_mean = jnp.mean(grad_hat, axis=-1, keepdims=True)
    second_mean = jnp.mean(grad_hat * normed, axis=-1, keepdims=True)
    return inverse * (grad_hat - first_mean - normed * second_mean)


def forward_block(normal_rows, normal_query, bias_query, key_bias, params):
    _, _, projection, gate_offset, out_proj, bias_proj = params
    head_total = bias_proj.shape[1]
    inner_width = projection.shape[2]
    head_size = inner_width // head_total
    query_scale = 1.0 / math.sqrt(head_size)
    block_rows, query_count, _ = normal_query.shape
    key_count = normal_rows.shape[1]
    queries = (
        jnp.dot(normal_query, projection[0], preferred_element_type=jnp.float32) * query_scale
    ).astype(jnp.bfloat16)
    joined_weights = jnp.concatenate([projection[1], projection[2]], axis=1)
    key_value = jnp.dot(normal_rows, joined_weights, preferred_element_type=jnp.float32).astype(
        jnp.bfloat16
    )
    gate_values = jax.nn.sigmoid(
        jnp.dot(normal_query, projection[3], preferred_element_type=jnp.float32) + gate_offset
    )
    head_queries = queries.reshape(block_rows, query_count, head_total, head_size).transpose(
        2, 0, 1, 3
    )
    head_pairs = key_value.reshape(block_rows, key_count, 2, head_total, head_size).transpose(
        2, 3, 0, 1, 4
    )

    def attend(inputs):
        query_head, key_head, value_head, bias_head = inputs
        logits = jnp.einsum(
            "rqd,rnd->rqn", query_head, key_head, preferred_element_type=jnp.float32
        )
        logits = logits + bias_head.astype(jnp.float32)[None] + key_bias
        largest = jnp.max(logits, axis=-1, keepdims=True)
        weights = jnp.exp(logits - largest)
        total = jnp.sum(weights, axis=-1, keepdims=True)
        soft_weights = weights / total
        attended = jnp.einsum(
            "rqn,rnd->rqd",
            soft_weights.astype(jnp.bfloat16),
            value_head,
            preferred_element_type=jnp.float32,
        )
        return ((largest + jnp.log(total))[..., 0], attended)

    log_totals, attended = lax.map(attend, (head_queries, head_pairs[0], head_pairs[1], bias_query))
    attended = attended.transpose(1, 2, 0, 3).reshape(block_rows, query_count, inner_width)
    gated_out = (gate_values * attended).astype(jnp.bfloat16)
    update = jnp.dot(gated_out, out_proj, preferred_element_type=jnp.float32).astype(jnp.bfloat16)
    saved = (head_queries, head_pairs, gate_values, attended, gated_out, log_totals)
    return (saved, update)


def backward_block(saved, normal_rows, normal_query, bias_query, grad_query, key_bias, params):
    _, _, projection, gate_offset, out_proj, bias_proj = params
    head_queries, head_pairs, gate_values, attended, gated_out, log_totals = saved
    channels = normal_rows.shape[2]
    head_total, block_rows, query_count, head_size = head_queries.shape
    key_count = normal_rows.shape[1]
    inner_width = head_total * head_size
    query_scale = 1.0 / math.sqrt(head_size)
    grad_gated = jnp.dot(grad_query, out_proj.T, preferred_element_type=jnp.float32)
    grad_att = (grad_gated * gate_values).astype(jnp.bfloat16)
    grad_pre = (grad_gated * attended * gate_values * (1.0 - gate_values)).astype(jnp.bfloat16)
    head_grads = grad_att.reshape(block_rows, query_count, head_total, head_size).transpose(
        2, 0, 1, 3
    )

    def differentiate(inputs):
        total_head, query_head, key_head, value_head, bias_head, grad_head = inputs
        logits = jnp.einsum(
            "rqd,rnd->rqn", query_head, key_head, preferred_element_type=jnp.float32
        )
        logits = logits + bias_head.astype(jnp.float32)[None] + key_bias
        soft_weights = jnp.exp(logits - total_head[..., None])
        grad_weights = jnp.einsum(
            "rqd,rnd->rqn", grad_head, value_head, preferred_element_type=jnp.float32
        )
        grad_logits = soft_weights * (
            grad_weights - jnp.sum(soft_weights * grad_weights, axis=-1, keepdims=True)
        )
        logits_half = grad_logits.astype(jnp.bfloat16)
        grad_queries = (
            jnp.einsum("rqn,rnd->rqd", logits_half, key_head, preferred_element_type=jnp.float32)
            * query_scale
        ).astype(jnp.bfloat16)
        grad_keys = jnp.einsum(
            "rqn,rqd->rnd", logits_half, query_head, preferred_element_type=jnp.float32
        ).astype(jnp.bfloat16)
        grad_values = jnp.einsum(
            "rqn,rqd->rnd",
            soft_weights.astype(jnp.bfloat16),
            grad_head,
            preferred_element_type=jnp.float32,
        ).astype(jnp.bfloat16)
        return (grad_queries, grad_keys, grad_values, jnp.sum(grad_logits, axis=0))

    grad_queries, grad_keys, grad_values, grad_bias = lax.map(
        differentiate,
        (log_totals, head_queries, head_pairs[0], head_pairs[1], bias_query, head_grads),
    )
    grad_queries = grad_queries.transpose(1, 2, 0, 3).reshape(block_rows, query_count, inner_width)
    key_weights = projection[1].reshape(channels, head_total, head_size).transpose(1, 2, 0)
    value_weights = projection[2].reshape(channels, head_total, head_size).transpose(1, 2, 0)
    query_side = jnp.dot(grad_queries, projection[0].T, preferred_element_type=jnp.float32)
    query_side = query_side + jnp.dot(grad_pre, projection[3].T, preferred_element_type=jnp.float32)
    term = jnp.einsum("hrnd,hdc->rnc", grad_keys, key_weights, preferred_element_type=jnp.float32)
    term = term + jnp.einsum(
        "hrnd,hdc->rnc", grad_values, value_weights, preferred_element_type=jnp.float32
    )
    shaped = term.reshape(block_rows, -1, query_count, channels)
    classes = lax.broadcasted_iota(jnp.int32, (1, shaped.shape[1], 1, 1), 1)
    own_class = classes == lax.axis_index(HEAD)
    partial = (shaped + jnp.where(own_class, query_side[:, None], 0.0)).astype(jnp.bfloat16)
    weight_sums = (
        jnp.einsum("rqc,rqe->ce", normal_query, grad_queries, preferred_element_type=jnp.float32),
        jnp.einsum(
            "rnc,hrnd->chd", normal_rows, grad_keys, preferred_element_type=jnp.float32
        ).reshape(channels, inner_width),
        jnp.einsum(
            "rnc,hrnd->chd", normal_rows, grad_values, preferred_element_type=jnp.float32
        ).reshape(channels, inner_width),
        jnp.einsum("rqc,rqe->ce", normal_query, grad_pre, preferred_element_type=jnp.float32),
        jnp.einsum("rqe,rqc->ec", gated_out, grad_query, preferred_element_type=jnp.float32),
        jnp.sum(grad_pre.astype(jnp.float32), axis=(0, 1))[None],
    )
    return (partial, grad_bias, jnp.concatenate(weight_sums, axis=0))


def padded_rows(x, rows):
    return jnp.pad(x, ((0, 0),) * (x.ndim - 2) + ((0, rows - x.shape[-2]), (0, 0)))


def rounded_up(value, step):
    return -(-value // step) * step


def local(
    pair_input,
    cotangent,
    residue_mask,
    norm_gain,
    norm_shift,
    proj_weights,
    gate_bias,
    out_weights,
    bias_weights,
):
    channels = pair_input.shape[2]
    groups = lax.axis_size("row")
    classes = lax.axis_size(HEAD)
    positions = groups * classes
    head_total = bias_weights.shape[2]
    bias_rows = head_total * positions // LANES
    half = jnp.bfloat16
    key_bias = (residue_mask.astype(jnp.float32) - 1.0) * MASKED
    key_bias = key_bias.reshape(groups, classes).T.reshape(positions)
    params = [
        (
            norm_gain[which],
            norm_shift[which],
            proj_weights[which],
            gate_bias[which],
            out_weights[which],
            bias_weights[which],
        )
        for which in range(2)
    ]

    own_pair = pair_input.reshape(groups, classes, channels).transpose(1, 0, 2)
    normed_own, inverse_own, normal_own = layer_norm(own_pair, norm_gain[0], norm_shift[0])
    normal_flat = normal_own.reshape(positions, channels)
    bias_own = jnp.einsum(
        "nc,ch->hn", normal_flat, bias_weights[0], preferred_element_type=jnp.float32
    ).astype(half)
    own_cotangent = cotangent.reshape(groups, classes, channels)
    arrived = exchanged(
        jnp.concatenate(
            [to_all(normal_flat, HEAD), own_pair, own_cotangent.transpose(1, 0, 2)], axis=1
        ),
        HEAD,
    )
    first_rows = arrived[:, :positions]
    pair_query = arrived[:, positions : positions + groups]
    cotangent_query = arrived[:, positions + groups :]
    first_query = lax.dynamic_index_in_dim(
        first_rows.reshape(classes, classes, groups, channels),
        lax.axis_index(HEAD),
        axis=1,
        keepdims=False,
    )
    arrived = exchanged(
        jnp.concatenate(
            [
                to_all(bias_own.reshape(bias_rows, LANES), "row"),
                own_cotangent,
            ],
            axis=1,
        ),
        "row",
    )
    first_bias = (
        arrived[:, :bias_rows].reshape(groups, head_total, positions).transpose(1, 0, 2)
    )
    second_grad_query = arrived[:, bias_rows:].transpose(1, 0, 2)
    first_saved, update = forward_block(first_rows, first_query, first_bias, key_bias, params[0])

    after_query = (pair_query.astype(jnp.float32) + update.astype(jnp.float32)).astype(half)
    after_normed, after_inverse, after_normal = layer_norm(
        after_query, norm_gain[1], norm_shift[1]
    )
    second_bias_own = jnp.einsum(
        "abc,ch->ahb", after_normal, bias_weights[1], preferred_element_type=jnp.float32
    ).astype(half)
    after_own = exchanged(after_query, HEAD)
    arrived = exchanged(
        jnp.concatenate(
            [
                to_all(second_bias_own.reshape(bias_rows, LANES), "row"),
                after_own.transpose(1, 0, 2),
            ],
            axis=1,
        ),
        "row",
    )
    second_bias = (
        arrived[:, :bias_rows]
        .reshape(groups, classes, head_total * groups)
        .transpose(2, 1, 0)
        .reshape(head_total, groups, positions)
    )
    flipped_query = arrived[:, bias_rows:].transpose(1, 0, 2)
    _, _, second_query = layer_norm(flipped_query, norm_gain[1], norm_shift[1])
    second_rows = (
        exchanged(to_all(second_query, HEAD), HEAD)
        .transpose(1, 0, 2, 3)
        .reshape(classes, positions, channels)
    )
    second_saved, _ = forward_block(second_rows, second_query, second_bias, key_bias, params[1])
    partial, grad_bias, second_sums = backward_block(
        second_saved, second_rows, second_query, second_bias, second_grad_query, key_bias, params[1]
    )

    share_rows = rounded_up(-(-second_sums.shape[0] // classes), 8)
    group_rows = rounded_up(share_rows, groups) // groups

    def shares_of(sums):
        return padded_rows(sums, classes * share_rows).astype(half).reshape(
            classes, share_rows, LANES
        )

    def group_shares_of(arrived_shares):
        summed = jnp.sum(arrived_shares.astype(jnp.float32), axis=0)
        summed = padded_rows(summed, groups * group_rows).astype(half)
        return padded_rows(summed.reshape(groups, group_rows, LANES), rounded_up(group_rows, 8))

    arrived = exchanged(
        jnp.concatenate(
            [
                partial.transpose(1, 0, 2, 3).reshape(classes, positions, channels),
                shares_of(second_sums),
            ],
            axis=1,
        ),
        HEAD,
    )
    grad_flipped = jnp.sum(arrived[:, :positions].astype(jnp.float32), axis=0).astype(half)
    bias_parts = (
        grad_bias.astype(half)
        .reshape(head_total * groups * classes, groups)
        .T.reshape(groups, bias_rows, LANES)
    )
    arrived = exchanged(
        jnp.concatenate(
            [
                bias_parts,
                grad_flipped.reshape(classes, groups, channels).transpose(1, 0, 2),
                group_shares_of(arrived[:, positions:]),
            ],
            axis=1,
        ),
        "row",
    )
    summed = jnp.sum(arrived[:, :bias_rows].astype(jnp.float32), axis=0)
    second_bias_half = summed.reshape(head_total, groups, classes).astype(half)
    second_own = jnp.sum(
        arrived[:, bias_rows + classes : bias_rows + classes + group_rows].astype(jnp.float32),
        axis=0,
    )
    grad_query = exchanged(arrived[:, bias_rows : bias_rows + classes].transpose(1, 0, 2), HEAD)
    grad_normal = grad_query.astype(jnp.float32) + jnp.einsum(
        "hba,ch->abc", second_bias_half, bias_weights[1], preferred_element_type=jnp.float32
    )
    end_query = norm_backward(grad_normal, after_normed, after_inverse, norm_gain[1]).astype(half)
    second_small = jnp.concatenate(
        [
            jnp.einsum(
                "abc,hba->hc", after_normal, second_bias_half, preferred_element_type=jnp.float32
            ),
            jnp.sum(grad_normal * after_normed, axis=(0, 1))[None],
            jnp.sum(grad_normal, axis=(0, 1))[None],
        ],
        axis=0,
    )

    after_grad_query = (
        cotangent_query.astype(jnp.float32) + end_query.astype(jnp.float32)
    ).astype(half)
    partial, grad_bias, first_sums = backward_block(
        first_saved, first_rows, first_query, first_bias, after_grad_query, key_bias, params[0]
    )
    arrived = exchanged(
        jnp.concatenate(
            [
                partial.reshape(classes, positions, channels),
                end_query,
                shares_of(jnp.concatenate([first_sums, second_small], axis=0)),
            ],
            axis=1,
        ),
        HEAD,
    )
    grad_normal = jnp.sum(arrived[:, :positions].astype(jnp.float32), axis=0)
    end_own = arrived[:, positions : positions + groups]
    shares = arrived[:, positions + groups :]
    arrived = exchanged(
        jnp.concatenate(
            [
                grad_bias.astype(half)
                .transpose(1, 0, 2)
                .reshape(groups, bias_rows, LANES),
                group_shares_of(shares),
            ],
            axis=1,
        ),
        "row",
    )
    summed = jnp.sum(arrived[:, :bias_rows].astype(jnp.float32), axis=0)
    bias_half = summed.reshape(head_total, positions).astype(half)
    first_own = jnp.sum(
        arrived[:, bias_rows : bias_rows + group_rows].astype(jnp.float32), axis=0
    )
    grad_normal = grad_normal + jnp.einsum(
        "hn,ch->nc", bias_half, bias_weights[0], preferred_element_type=jnp.float32
    )
    normed_flat = normed_own.reshape(positions, channels)
    start_grad = norm_backward(
        grad_normal, normed_flat, inverse_own.reshape(positions, 1), norm_gain[0]
    )
    moved_grad = (end_own.astype(jnp.float32) + start_grad.reshape(end_own.shape)).transpose(1, 0, 2)
    pair_grad = cotangent.astype(jnp.float32) + moved_grad.reshape(1, positions, channels)
    first_small = jnp.concatenate(
        [
            jnp.einsum("nc,hn->hc", normal_flat, bias_half, preferred_element_type=jnp.float32),
            jnp.sum(grad_normal * normed_flat, axis=0)[None],
            jnp.sum(grad_normal, axis=0)[None],
        ],
        axis=0,
    )

    small_rows = first_small.shape[0]
    tail = jnp.concatenate([first_own, second_own, first_small], axis=0).astype(half)
    tail = padded_rows(tail, rounded_up(tail.shape[0], 8))
    arrived = exchanged(to_all(tail, "row"), "row").astype(jnp.float32)
    whole_rows = groups * group_rows
    shared = jnp.concatenate(
        [
            arrived[:, :group_rows].reshape(whole_rows, LANES)[:share_rows],
            arrived[:, group_rows : 2 * group_rows].reshape(whole_rows, LANES)[:share_rows],
            padded_rows(
                jnp.sum(arrived[:, 2 * group_rows : 2 * group_rows + small_rows], axis=0),
                rounded_up(small_rows, 8),
            ),
        ],
        axis=0,
    )
    arrived = exchanged(to_all(shared, HEAD), HEAD)
    first_whole = arrived[:, :share_rows].reshape(-1, LANES)
    second_whole = arrived[:, share_rows : 2 * share_rows].reshape(-1, LANES)
    first_small = jnp.sum(arrived[:, 2 * share_rows : 2 * share_rows + small_rows], axis=0)
    main_rows = first_sums.shape[0]
    second_small = first_whole[main_rows : main_rows + small_rows]
    proj_rows = 4 * channels

    def both(first, second):
        return jnp.stack([first, second])

    return (
        pair_grad,
        both(first_whole[:proj_rows], second_whole[:proj_rows]).reshape(
            2, 4, channels, -1
        ),
        both(first_whole[main_rows - 1], second_whole[main_rows - 1]),
        both(first_whole[proj_rows : main_rows - 1], second_whole[proj_rows : main_rows - 1]),
        both(first_small[:head_total].T, second_small[:head_total].T),
        both(first_small[head_total], second_small[head_total]),
        both(first_small[head_total + 1], second_small[head_total + 1]),
    )


def solution(mesh):
    finer = Mesh(mesh.devices.reshape(mesh.shape["row"], 4, 2), ("row", "head_0", "head_1"))
    in_specs = (P(ROW_HEAD, None, None), P(ROW_HEAD, None, None), P(), P(), P(), P(), P(), P(), P())
    out_specs = (P(ROW_HEAD, None, None), P(), P(), P(), P(), P(), P())
    return jax.shard_map(local, mesh=finer, in_specs=in_specs, out_specs=out_specs, check_vma=False)
```

```python
import functools
import math

import jax
import jax.numpy as jnp
from jax import lax
from jax.experimental import pallas as pl
from jax.experimental.pallas import tpu as pltpu
from jax.sharding import Mesh
from jax.sharding import PartitionSpec as P

HEAD = ("head_0", "head_1")
ROW_HEAD = ("row", "head_0", "head_1")


EPS = 1e-05
MASKED = 1000000000.0
LANES = 128
INTERPRET = False


def exchanged(parts, axis):
    return lax.all_to_all(parts, axis, split_axis=0, concat_axis=0, tiled=True)


def to_all(x, axis):
    return jnp.broadcast_to(x[None], (lax.axis_size(axis), *x.shape))


def layer_norm(values, norm_scale, norm_offset):
    floats = values.astype(jnp.float32)
    centred = floats - jnp.mean(floats, axis=-1, keepdims=True)
    inverse = lax.rsqrt(jnp.mean(centred * centred, axis=-1, keepdims=True) + EPS)
    normed = centred * inverse
    return (normed, inverse, (normed * norm_scale + norm_offset).astype(jnp.bfloat16))


def norm_backward(grad_normal, normed, inverse, norm_scale):
    grad_hat = grad_normal * norm_scale
    first_mean = jnp.mean(grad_hat, axis=-1, keepdims=True)
    second_mean = jnp.mean(grad_hat * normed, axis=-1, keepdims=True)
    return inverse * (grad_hat - first_mean - normed * second_mean)


def matmul(a, b, a_dim, b_dim):
    return lax.dot_general(
        a, b, (((a_dim,), (b_dim,)), ((), ())), preferred_element_type=jnp.float32
    )


def lanes_of_head(shape, head, head_size):
    lanes = lax.broadcasted_iota(jnp.int32, shape, 1)
    return (lanes >= head * head_size) & (lanes < (head + 1) * head_size)


def spread_heads(values, heads):
    size = values.shape[1] // heads
    kept = [
        jnp.where(lanes_of_head(values.shape, head, size), values, 0.0) for head in range(heads)
    ]
    return jnp.concatenate(kept, axis=0).astype(jnp.bfloat16)


def picked_heads(stacked, heads):
    rows = stacked.shape[0] // heads
    size = stacked.shape[1] // heads
    total = jnp.zeros((rows, stacked.shape[1]), jnp.float32)
    for head in range(heads):
        part = stacked[head * rows : (head + 1) * rows]
        total = jnp.where(lanes_of_head(part.shape, head, size), part, total)
    return total


def attention(x, xq, bias, wq, wkv, wg, gate_offset, heads):
    channels = wq.shape[1]
    scale = 1.0 / math.sqrt(channels // heads)
    queries = spread_heads(
        (matmul(xq, wq, 1, 0) * scale).astype(jnp.bfloat16).astype(jnp.float32), heads
    )
    key_value = matmul(x, wkv, 1, 0).astype(jnp.bfloat16)
    keys = key_value[:, :channels]
    values = key_value[:, channels:]
    gate = jax.nn.sigmoid(matmul(xq, wg, 1, 0) + gate_offset)
    logits = matmul(queries, keys, 1, 1) + bias
    weights = jnp.exp(logits - jnp.max(logits, axis=1, keepdims=True))
    probs = weights / jnp.sum(weights, axis=1, keepdims=True)
    probs_half = probs.astype(jnp.bfloat16)
    attended = picked_heads(matmul(probs_half, values, 1, 0), heads)
    return (queries, keys, values, gate, probs, probs_half, attended)


def split_bias(bias, key_bias, heads):
    count = bias.shape[1] // heads
    parts = [bias[:, head * count : (head + 1) * count] for head in range(heads)]
    return jnp.concatenate(parts, axis=0).astype(jnp.float32) + key_bias


def forward_kernel(heads, positions, class_ref, rows_ref, bias_ref, mask_ref, wq_ref, wkv_ref,
                   wg_ref, wo_ref, gate_ref, after_ref, full_bias):
    groups = after_ref.shape[1]

    @pl.when(pl.program_id(0) == 0)
    def _():
        full_bias[...] = split_bias(bias_ref[...], mask_ref[...], heads)

    x = rows_ref[0, :positions]
    start = pl.multiple_of(class_ref[0] * groups, groups)
    xq = rows_ref[0, pl.ds(start, groups)]
    result = attention(
        x, xq, full_bias[...], wq_ref[...], wkv_ref[...], wg_ref[...], gate_ref[...], heads
    )
    gated = (result[3] * result[6]).astype(jnp.bfloat16)
    update = matmul(gated, wo_ref[...], 1, 0).astype(jnp.bfloat16)
    pair = rows_ref[0, positions : positions + groups]
    after_ref[0] = (pair.astype(jnp.float32) + update.astype(jnp.float32)).astype(jnp.bfloat16)


def backward_kernel(heads, positions, second, share_rows, class_ref, rows_ref, bias_ref, mask_ref,
                    grad_ref, extra_ref, ride_ref, wq_ref, wkv_ref, wg_ref, wo_ref, gate_ref,
                    sent_ref, bias_out_ref, full_bias, bias_sum, weight_sum, share):
    step = pl.program_id(0)
    classes = sent_ref.shape[0]
    groups = positions // classes
    channels = wq_ref.shape[0]
    inner = wq_ref.shape[1]
    own_class = class_ref[0]
    share_start = positions if second else positions + groups

    @pl.when(step == 0)
    def _():
        if second:
            full_bias[...] = bias_ref[...].astype(jnp.float32).T + mask_ref[...]
        else:
            full_bias[...] = split_bias(bias_ref[...], mask_ref[...], heads)
            sent_ref[:, positions : positions + groups] = ride_ref[...]
        bias_sum[...] = jnp.zeros(bias_sum.shape, jnp.float32)
        weight_sum[...] = jnp.zeros(weight_sum.shape, jnp.float32)
        weight_sum[5 * channels : 5 * channels + 8] = extra_ref[...]

    if second:
        x = rows_ref[:, 0].reshape(positions, channels)
        xq = rows_ref[pl.ds(own_class, 1), 0].reshape(groups, channels)
    else:
        x = rows_ref[0, :positions]
        xq = rows_ref[0, pl.ds(pl.multiple_of(own_class * groups, groups), groups)]
    queries, keys, values, gate, probs, probs_half, attended = attention(
        x, xq, full_bias[...], wq_ref[...], wkv_ref[...], wg_ref[...], gate_ref[...], heads
    )
    scale = 1.0 / math.sqrt(inner // heads)
    grad = grad_ref[0]
    gated = (gate * attended).astype(jnp.bfloat16)
    grad_gated = matmul(grad, wo_ref[...], 1, 1)
    grad_att = (grad_gated * gate).astype(jnp.bfloat16).astype(jnp.float32)
    grad_pre = (grad_gated * attended * gate * (1.0 - gate)).astype(jnp.bfloat16)
    grad_heads = spread_heads(grad_att, heads)
    grad_probs = matmul(grad_heads, values, 1, 1)
    grad_logits = probs * (grad_probs - jnp.sum(probs * grad_probs, axis=1, keepdims=True))
    bias_sum[...] += grad_logits
    logits_half = grad_logits.astype(jnp.bfloat16)
    grad_queries = (picked_heads(matmul(logits_half, keys, 1, 0), heads) * scale).astype(
        jnp.bfloat16
    )
    grad_keys = matmul(logits_half, queries, 0, 0).astype(jnp.bfloat16)
    grad_values = matmul(probs_half, grad_heads, 0, 0).astype(jnp.bfloat16)
    grad_pairs = jnp.concatenate([grad_keys, grad_values], axis=1)
    share[...] = matmul(grad_pairs, wkv_ref[...], 1, 1)
    query_side = matmul(grad_queries, wq_ref[...], 1, 1) + matmul(grad_pre, wg_ref[...], 1, 1)
    own_rows = pl.ds(pl.multiple_of(own_class * groups, groups), groups)
    share[own_rows] = share[own_rows] + query_side
    partial = share[...].astype(jnp.bfloat16)
    if second:
        place = pl.ds(pl.multiple_of(step * groups, groups), groups)
        sent_ref[:, place] = partial.reshape(classes, groups, channels)
    else:
        sent_ref[pl.ds(step, 1), :positions] = partial[None]
    pair_sums = matmul(x, grad_pairs, 0, 0)
    weight_sum[:channels] += matmul(xq, grad_queries, 0, 0)
    weight_sum[channels : 2 * channels] += pair_sums[:, :inner]
    weight_sum[2 * channels : 3 * channels] += pair_sums[:, inner:]
    weight_sum[3 * channels : 4 * channels] += matmul(xq, grad_pre, 0, 0)
    weight_sum[4 * channels : 5 * channels] += matmul(gated, grad, 0, 0)
    weight_sum[5 * channels : 5 * channels + 1] += jnp.sum(
        grad_pre.astype(jnp.float32), axis=0, keepdims=True
    )

    @pl.when(step == pl.num_programs(0) - 1)
    def _():
        for peer in range(classes):
            sent_ref[peer, share_start : share_start + share_rows] = weight_sum[
                peer * share_rows : (peer + 1) * share_rows
            ].astype(jnp.bfloat16)
        if second:
            bias_out_ref[...] = bias_sum[...].T.astype(jnp.bfloat16)
        else:
            for head in range(heads):
                bias_out_ref[:, head * positions : (head + 1) * positions] = bias_sum[
                    head * groups : (head + 1) * groups
                ].astype(jnp.bfloat16)


def whole_spec(x):
    return pl.BlockSpec(x.shape, lambda step, n=x.ndim: (0,) * n)


def kernel_weights(params):
    _, _, projection, gate_offset, out_proj, _ = params
    joined = jnp.concatenate([projection[1], projection[2]], axis=1)
    return (projection[0], joined, projection[3], out_proj, gate_offset[None])


def forward_call(own_class, rows, bias, key_bias, params, heads, positions):
    classes, _, channels = rows.shape
    groups = positions // classes
    rest = (bias, key_bias, *kernel_weights(params))
    return pl.pallas_call(
        functools.partial(forward_kernel, heads, positions),
        grid=(classes,),
        in_specs=[
            pl.BlockSpec(memory_space=pltpu.SMEM),
            pl.BlockSpec((1, *rows.shape[1:]), lambda step: (step, 0, 0)),
            *[whole_spec(x) for x in rest],
        ],
        out_specs=pl.BlockSpec((1, groups, channels), lambda step: (step, 0, 0)),
        out_shape=jax.ShapeDtypeStruct((classes, groups, channels), jnp.bfloat16),
        scratch_shapes=[pltpu.VMEM((heads * groups, positions), jnp.float32)],
        compiler_params=pltpu.CompilerParams(dimension_semantics=("arbitrary",)),
        interpret=INTERPRET,
        name="forward_rows",
    )(own_class, rows, *rest)


def backward_call(own_class, rows, bias, key_bias, grad, extra, ride, params, heads, positions,
                  share_rows):
    second = ride is None
    classes, groups, channels = grad.shape
    inner = params[2].shape[2]
    if second:
        ride = jnp.zeros((8, LANES), jnp.bfloat16)
        rows_spec = pl.BlockSpec((classes, 1, groups, channels), lambda step: (0, step, 0, 0))
        bias_shape = (positions, heads * groups)
        sent_rows = positions + share_rows
    else:
        rows_spec = pl.BlockSpec((1, *rows.shape[1:]), lambda step: (step, 0, 0))
        bias_shape = (groups, heads * positions)
        sent_rows = positions + groups + share_rows
    weights = kernel_weights(params)
    sent = jax.ShapeDtypeStruct((classes, sent_rows, channels), jnp.bfloat16)
    bias_out = jax.ShapeDtypeStruct(bias_shape, jnp.bfloat16)
    return pl.pallas_call(
        functools.partial(backward_kernel, heads, positions, second, share_rows),
        grid=(classes,),
        in_specs=[
            pl.BlockSpec(memory_space=pltpu.SMEM),
            rows_spec,
            whole_spec(bias),
            whole_spec(key_bias),
            pl.BlockSpec((1, groups, channels), lambda step: (step, 0, 0)),
            whole_spec(extra),
            whole_spec(ride),
            *[whole_spec(x) for x in weights],
        ],
        out_specs=[whole_spec(sent), whole_spec(bias_out)],
        out_shape=[sent, bias_out],
        scratch_shapes=[
            pltpu.VMEM((heads * groups, positions), jnp.float32),
            pltpu.VMEM((heads * groups, positions), jnp.float32),
            pltpu.VMEM((classes * share_rows, channels), jnp.float32),
            pltpu.VMEM((positions, channels), jnp.float32),
        ],
        compiler_params=pltpu.CompilerParams(dimension_semantics=("arbitrary",)),
        interpret=INTERPRET,
        name="backward_second" if second else "backward_first",
    )(own_class, rows, bias, key_bias, grad, extra, ride, *weights)


def padded_rows(x, rows):
    return jnp.pad(x, ((0, 0),) * (x.ndim - 2) + ((0, rows - x.shape[-2]), (0, 0)))


def rounded_up(value, step):
    return -(-value // step) * step


def local(
    pair_input,
    cotangent,
    residue_mask,
    norm_gain,
    norm_shift,
    proj_weights,
    gate_bias,
    out_weights,
    bias_weights,
):
    channels = pair_input.shape[2]
    groups = lax.axis_size("row")
    classes = lax.axis_size(HEAD)
    positions = groups * classes
    head_total = bias_weights.shape[2]
    bias_rows = head_total * positions // LANES
    half = jnp.bfloat16
    key_bias = (residue_mask.astype(jnp.float32) - 1.0) * MASKED
    key_bias = key_bias.reshape(groups, classes).T.reshape(1, positions)
    own_class = lax.axis_index(HEAD).astype(jnp.int32).reshape(1)
    main_rows = 5 * channels + 1
    share_rows = rounded_up(-(-(main_rows + head_total + 2) // classes), 16)
    group_rows = rounded_up(share_rows, groups) // groups
    params = [
        (
            norm_gain[which],
            norm_shift[which],
            proj_weights[which],
            gate_bias[which],
            out_weights[which],
            bias_weights[which],
        )
        for which in range(2)
    ]

    own_pair = pair_input.reshape(groups, classes, channels).transpose(1, 0, 2)
    normed_own, inverse_own, normal_own = layer_norm(own_pair, norm_gain[0], norm_shift[0])
    normal_flat = normal_own.reshape(positions, channels)
    bias_own = jnp.einsum(
        "nc,ch->hn", normal_flat, bias_weights[0], preferred_element_type=jnp.float32
    ).astype(half)
    own_cotangent = cotangent.reshape(groups, classes, channels)
    arrived = exchanged(
        jnp.concatenate(
            [to_all(normal_flat, HEAD), own_pair, own_cotangent.transpose(1, 0, 2)], axis=1
        ),
        HEAD,
    )
    first_rows = arrived
    cotangent_query = arrived[:, positions + groups :]
    arrived = exchanged(
        jnp.concatenate(
            [
                to_all(bias_own.reshape(bias_rows, LANES), "row"),
                own_cotangent,
            ],
            axis=1,
        ),
        "row",
    )
    first_bias = arrived[:, :bias_rows].reshape(groups, head_total * positions)
    second_grad_query = arrived[:, bias_rows:].transpose(1, 0, 2)

    after_query = forward_call(
        own_class, first_rows, first_bias, key_bias, params[0], head_total, positions
    )
    after_normed, after_inverse, after_normal = layer_norm(
        after_query, norm_gain[1], norm_shift[1]
    )
    second_bias_own = jnp.einsum(
        "abc,ch->ahb", after_normal, bias_weights[1], preferred_element_type=jnp.float32
    ).astype(half)
    after_own = exchanged(after_query, HEAD)
    arrived = exchanged(
        jnp.concatenate(
            [
                to_all(second_bias_own.reshape(bias_rows, LANES), "row"),
                after_own.transpose(1, 0, 2),
            ],
            axis=1,
        ),
        "row",
    )
    second_bias = (
        arrived[:, :bias_rows]
        .reshape(groups, classes, head_total * groups)
        .transpose(1, 0, 2)
        .reshape(positions, head_total * groups)
    )
    flipped_query = arrived[:, bias_rows:].transpose(1, 0, 2)
    _, _, second_query = layer_norm(flipped_query, norm_gain[1], norm_shift[1])
    second_rows = exchanged(to_all(second_query, HEAD), HEAD)
    sent, bias_parts = backward_call(
        own_class,
        second_rows.reshape(classes, classes, groups, channels),
        second_bias,
        key_bias,
        second_grad_query,
        jnp.zeros((8, LANES), jnp.float32),
        None,
        params[1],
        head_total,
        positions,
        share_rows,
    )

    def group_shares_of(arrived_shares):
        summed = jnp.sum(arrived_shares.astype(jnp.float32), axis=0)
        summed = padded_rows(summed, groups * group_rows).astype(half)
        return padded_rows(summed.reshape(groups, group_rows, LANES), rounded_up(group_rows, 8))

    arrived = exchanged(sent, HEAD)
    grad_flipped = jnp.sum(arrived[:, :positions].astype(jnp.float32), axis=0).astype(half)
    bias_parts = (
        bias_parts.reshape(classes, groups, head_total * groups)
        .transpose(1, 0, 2)
        .reshape(groups, bias_rows, LANES)
    )
    arrived = exchanged(
        jnp.concatenate(
            [
                bias_parts,
                grad_flipped.reshape(classes, groups, channels).transpose(1, 0, 2),
                group_shares_of(arrived[:, positions:]),
            ],
            axis=1,
        ),
        "row",
    )
    summed = jnp.sum(arrived[:, :bias_rows].astype(jnp.float32), axis=0)
    second_bias_half = summed.reshape(classes, head_total, groups).astype(half)
    second_own = jnp.sum(
        arrived[:, bias_rows + classes : bias_rows + classes + group_rows].astype(jnp.float32),
        axis=0,
    )
    grad_query = exchanged(arrived[:, bias_rows : bias_rows + classes].transpose(1, 0, 2), HEAD)
    grad_normal = grad_query.astype(jnp.float32) + jnp.einsum(
        "ahb,ch->abc", second_bias_half, bias_weights[1], preferred_element_type=jnp.float32
    )
    end_query = norm_backward(grad_normal, after_normed, after_inverse, norm_gain[1]).astype(half)
    second_small = jnp.concatenate(
        [
            jnp.einsum(
                "abc,ahb->hc", after_normal, second_bias_half, preferred_element_type=jnp.float32
            ),
            jnp.sum(grad_normal * after_normed, axis=(0, 1))[None],
            jnp.sum(grad_normal, axis=(0, 1))[None],
        ],
        axis=0,
    )

    after_grad_query = (
        cotangent_query.astype(jnp.float32) + end_query.astype(jnp.float32)
    ).astype(half)
    extra = jnp.pad(second_small, ((1, 7 - second_small.shape[0]), (0, 0)))
    sent, bias_parts = backward_call(
        own_class,
        first_rows,
        first_bias,
        key_bias,
        after_grad_query,
        extra,
        end_query,
        params[0],
        head_total,
        positions,
        share_rows,
    )
    arrived = exchanged(sent, HEAD)
    grad_normal = jnp.sum(arrived[:, :positions].astype(jnp.float32), axis=0)
    end_own = arrived[:, positions : positions + groups]
    shares = arrived[:, positions + groups :]
    arrived = exchanged(
        jnp.concatenate(
            [
                bias_parts.reshape(groups, bias_rows, LANES),
                group_shares_of(shares),
            ],
            axis=1,
        ),
        "row",
    )
    summed = jnp.sum(arrived[:, :bias_rows].astype(jnp.float32), axis=0)
    bias_half = summed.reshape(head_total, positions).astype(half)
    first_own = jnp.sum(
        arrived[:, bias_rows : bias_rows + group_rows].astype(jnp.float32), axis=0
    )
    grad_normal = grad_normal + jnp.einsum(
        "hn,ch->nc", bias_half, bias_weights[0], preferred_element_type=jnp.float32
    )
    normed_flat = normed_own.reshape(positions, channels)
    start_grad = norm_backward(
        grad_normal, normed_flat, inverse_own.reshape(positions, 1), norm_gain[0]
    )
    moved_grad = (end_own.astype(jnp.float32) + start_grad.reshape(end_own.shape)).transpose(1, 0, 2)
    pair_grad = cotangent.astype(jnp.float32) + moved_grad.reshape(1, positions, channels)
    first_small = jnp.concatenate(
        [
            jnp.einsum("nc,hn->hc", normal_flat, bias_half, preferred_element_type=jnp.float32),
            jnp.sum(grad_normal * normed_flat, axis=0)[None],
            jnp.sum(grad_normal, axis=0)[None],
        ],
        axis=0,
    )

    small_rows = first_small.shape[0]
    tail = jnp.concatenate([first_own, second_own, first_small], axis=0).astype(half)
    tail = padded_rows(tail, rounded_up(tail.shape[0], 8))
    arrived = exchanged(to_all(tail, "row"), "row").astype(jnp.float32)
    whole_rows = groups * group_rows
    shared = jnp.concatenate(
        [
            arrived[:, :group_rows].reshape(whole_rows, LANES)[:share_rows],
            arrived[:, group_rows : 2 * group_rows].reshape(whole_rows, LANES)[:share_rows],
            padded_rows(
                jnp.sum(arrived[:, 2 * group_rows : 2 * group_rows + small_rows], axis=0),
                rounded_up(small_rows, 8),
            ),
        ],
        axis=0,
    )
    arrived = exchanged(to_all(shared, HEAD), HEAD)
    first_whole = arrived[:, :share_rows].reshape(-1, LANES)
    second_whole = arrived[:, share_rows : 2 * share_rows].reshape(-1, LANES)
    first_small = jnp.sum(arrived[:, 2 * share_rows : 2 * share_rows + small_rows], axis=0)
    second_small = first_whole[main_rows : main_rows + small_rows]
    proj_rows = 4 * channels

    def both(first, second):
        return jnp.stack([first, second])

    return (
        pair_grad,
        both(first_whole[:proj_rows], second_whole[:proj_rows]).reshape(
            2, 4, channels, -1
        ),
        both(first_whole[main_rows - 1], second_whole[main_rows - 1]),
        both(first_whole[proj_rows : main_rows - 1], second_whole[proj_rows : main_rows - 1]),
        both(first_small[:head_total].T, second_small[:head_total].T),
        both(first_small[head_total], second_small[head_total]),
        both(first_small[head_total + 1], second_small[head_total + 1]),
    )


def solution(mesh):
    finer = Mesh(mesh.devices.reshape(mesh.shape["row"], 4, 2), ("row", "head_0", "head_1"))
    in_specs = (P(ROW_HEAD, None, None), P(ROW_HEAD, None, None), P(), P(), P(), P(), P(), P(), P())
    out_specs = (P(ROW_HEAD, None, None), P(), P(), P(), P(), P(), P())
    return jax.shard_map(local, mesh=finer, in_specs=in_specs, out_specs=out_specs, check_vma=False)
```

```python
import functools
import math

import jax
import jax.numpy as jnp
from jax import lax
from jax.experimental import pallas as pl
from jax.experimental.pallas import tpu as pltpu
from jax.sharding import Mesh
from jax.sharding import PartitionSpec as P


HEAD = ("head_0", "head_1")
ROW_HEAD = ("row", "head_0", "head_1")


EPS = 1e-05
MASKED = 1000000000.0
LANES = 128
INTERPRET = False


def exchanged(parts, axis):
    return lax.all_to_all(parts, axis, split_axis=0, concat_axis=0, tiled=True)


def shifted_exchange(parts):
    count = parts.shape[0]
    pieces = [parts[0]]
    for shift in range(1, count):
        pairs = [(at, (at + shift) % count) for at in range(count)]
        pieces.append(lax.ppermute(parts[shift], HEAD, pairs))
    return pieces


def rolled(x, by):
    return lax.dynamic_slice_in_dim(jnp.concatenate([x, x]), by, x.shape[0], axis=0)


def place_kernel(own_ref, *refs):
    count = len(refs) - 1
    for shift in range(count):
        place = lax.rem(own_ref[0] + (count - shift), count)
        refs[-1][pl.ds(place, 1)] = refs[shift][...][None]


def placed(own_class, pieces):
    return pl.pallas_call(
        place_kernel,
        in_specs=[
            pl.BlockSpec(memory_space=pltpu.SMEM),
            *[pl.BlockSpec(memory_space=pltpu.VMEM) for _ in pieces],
        ],
        out_specs=pl.BlockSpec(memory_space=pltpu.VMEM),
        out_shape=jax.ShapeDtypeStruct((len(pieces), *pieces[0].shape), pieces[0].dtype),
        interpret=INTERPRET,
        name="place_pieces",
    )(own_class, *pieces)


def summed(pieces):
    total = pieces[0].astype(jnp.float32)
    for piece in pieces[1:]:
        total = total + piece.astype(jnp.float32)
    return total


def to_all(x, axis):
    return jnp.broadcast_to(x[None], (lax.axis_size(axis), *x.shape))


def layer_norm(values, norm_scale, norm_offset):
    floats = values.astype(jnp.float32)
    centred = floats - jnp.mean(floats, axis=-1, keepdims=True)
    inverse = lax.rsqrt(jnp.mean(centred * centred, axis=-1, keepdims=True) + EPS)
    normed = centred * inverse
    return (normed, inverse, (normed * norm_scale + norm_offset).astype(jnp.bfloat16))


def norm_backward(grad_normal, normed, inverse, norm_scale):
    grad_hat = grad_normal * norm_scale
    first_mean = jnp.mean(grad_hat, axis=-1, keepdims=True)
    second_mean = jnp.mean(grad_hat * normed, axis=-1, keepdims=True)
    return inverse * (grad_hat - first_mean - normed * second_mean)


def matmul(a, b, a_dim, b_dim):
    return lax.dot_general(
        a, b, (((a_dim,), (b_dim,)), ((), ())), preferred_element_type=jnp.float32
    )


def lanes_of_head(shape, head, head_size):
    lanes = lax.broadcasted_iota(jnp.int32, shape, 1)
    return (lanes >= head * head_size) & (lanes < (head + 1) * head_size)


def spread_heads(values, heads):
    size = values.shape[1] // heads
    kept = [
        jnp.where(lanes_of_head(values.shape, head, size), values, 0.0) for head in range(heads)
    ]
    return jnp.concatenate(kept, axis=0).astype(jnp.bfloat16)


def picked_heads(stacked, heads):
    rows = stacked.shape[0] // heads
    size = stacked.shape[1] // heads
    total = jnp.zeros((rows, stacked.shape[1]), jnp.float32)
    for head in range(heads):
        part = stacked[head * rows : (head + 1) * rows]
        total = jnp.where(lanes_of_head(part.shape, head, size), part, total)
    return total


def attention(x, xq, bias, wq, wkv, wg, gate_offset, heads):
    channels = wq.shape[1]
    scale = 1.0 / math.sqrt(channels // heads)
    queries = spread_heads(
        (matmul(xq, wq, 1, 0) * scale).astype(jnp.bfloat16).astype(jnp.float32), heads
    )
    key_value = matmul(x, wkv, 1, 0).astype(jnp.bfloat16)
    keys = key_value[:, :channels]
    values = key_value[:, channels:]
    gate = jax.nn.sigmoid(matmul(xq, wg, 1, 0) + gate_offset)
    logits = matmul(queries, keys, 1, 1) + bias
    weights = jnp.exp(logits - jnp.max(logits, axis=1, keepdims=True))
    probs = weights / jnp.sum(weights, axis=1, keepdims=True)
    probs_half = probs.astype(jnp.bfloat16)
    attended = picked_heads(matmul(probs_half, values, 1, 0), heads)
    return (queries, keys, values, gate, probs, probs_half, attended)


def split_bias(bias, key_bias, heads):
    count = bias.shape[1] // heads
    parts = [bias[:, head * count : (head + 1) * count] for head in range(heads)]
    return jnp.concatenate(parts, axis=0).astype(jnp.float32) + key_bias


def forward_kernel(heads, positions, class_ref, rows_ref, bias_ref, mask_ref, wq_ref, wkv_ref,
                   wg_ref, wo_ref, gate_ref, after_ref, full_bias):
    groups = after_ref.shape[1]

    @pl.when(pl.program_id(0) == 0)
    def _():
        full_bias[...] = split_bias(bias_ref[...], mask_ref[...], heads)

    x = rows_ref[0, :positions]
    start = pl.multiple_of(class_ref[0] * groups, groups)
    xq = rows_ref[0, pl.ds(start, groups)]
    result = attention(
        x, xq, full_bias[...], wq_ref[...], wkv_ref[...], wg_ref[...], gate_ref[...], heads
    )
    gated = (result[3] * result[6]).astype(jnp.bfloat16)
    update = matmul(gated, wo_ref[...], 1, 0).astype(jnp.bfloat16)
    pair = rows_ref[0, positions : positions + groups]
    after_ref[0] = (pair.astype(jnp.float32) + update.astype(jnp.float32)).astype(jnp.bfloat16)


def backward_kernel(heads, positions, second, share_rows, class_ref, rows_ref, bias_ref, mask_ref,
                    grad_ref, extra_ref, ride_ref, wq_ref, wkv_ref, wg_ref, wo_ref, gate_ref,
                    sent_ref, bias_out_ref, full_bias, bias_sum, weight_sum, share):
    step = pl.program_id(0)
    classes = sent_ref.shape[0]
    groups = positions // classes
    channels = wq_ref.shape[0]
    inner = wq_ref.shape[1]
    own_class = class_ref[0]
    share_start = positions if second else positions + groups

    @pl.when(step == 0)
    def _():
        if second:
            full_bias[...] = bias_ref[...].astype(jnp.float32).T + mask_ref[...]
        else:
            full_bias[...] = split_bias(bias_ref[...], mask_ref[...], heads)
            for peer in range(classes):
                slot = lax.rem(peer + classes - own_class, classes)
                sent_ref[pl.ds(slot, 1), positions : positions + groups] = ride_ref[peer][None]
        bias_sum[...] = jnp.zeros(bias_sum.shape, jnp.float32)
        weight_sum[...] = jnp.zeros(weight_sum.shape, jnp.float32)
        weight_sum[5 * channels : 5 * channels + 8] = extra_ref[...]

    if second:
        x = rows_ref[:, 0].reshape(positions, channels)
        xq = rows_ref[pl.ds(own_class, 1), 0].reshape(groups, channels)
    else:
        x = rows_ref[0, :positions]
        xq = rows_ref[0, pl.ds(pl.multiple_of(own_class * groups, groups), groups)]
    queries, keys, values, gate, probs, probs_half, attended = attention(
        x, xq, full_bias[...], wq_ref[...], wkv_ref[...], wg_ref[...], gate_ref[...], heads
    )
    scale = 1.0 / math.sqrt(inner // heads)
    grad = grad_ref[0]
    gated = (gate * attended).astype(jnp.bfloat16)
    grad_gated = matmul(grad, wo_ref[...], 1, 1)
    grad_att = (grad_gated * gate).astype(jnp.bfloat16).astype(jnp.float32)
    grad_pre = (grad_gated * attended * gate * (1.0 - gate)).astype(jnp.bfloat16)
    grad_heads = spread_heads(grad_att, heads)
    grad_probs = matmul(grad_heads, values, 1, 1)
    grad_logits = probs * (grad_probs - jnp.sum(probs * grad_probs, axis=1, keepdims=True))
    bias_sum[...] += grad_logits
    logits_half = grad_logits.astype(jnp.bfloat16)
    grad_queries = (picked_heads(matmul(logits_half, keys, 1, 0), heads) * scale).astype(
        jnp.bfloat16
    )
    grad_keys = matmul(logits_half, queries, 0, 0).astype(jnp.bfloat16)
    grad_values = matmul(probs_half, grad_heads, 0, 0).astype(jnp.bfloat16)
    grad_pairs = jnp.concatenate([grad_keys, grad_values], axis=1)
    share[...] = matmul(grad_pairs, wkv_ref[...], 1, 1)
    query_side = matmul(grad_queries, wq_ref[...], 1, 1) + matmul(grad_pre, wg_ref[...], 1, 1)
    own_rows = pl.ds(pl.multiple_of(own_class * groups, groups), groups)
    share[own_rows] = share[own_rows] + query_side
    partial = share[...].astype(jnp.bfloat16)
    if second:
        place = pl.ds(pl.multiple_of(step * groups, groups), groups)
        for peer in range(classes):
            slot = lax.rem(peer + classes - own_class, classes)
            sent_ref[pl.ds(slot, 1), place] = partial[peer * groups : (peer + 1) * groups][None]
    else:
        slot = lax.rem(step + classes - own_class, classes)
        sent_ref[pl.ds(slot, 1), :positions] = partial[None]
    pair_sums = matmul(x, grad_pairs, 0, 0)
    weight_sum[:channels] += matmul(xq, grad_queries, 0, 0)
    weight_sum[channels : 2 * channels] += pair_sums[:, :inner]
    weight_sum[2 * channels : 3 * channels] += pair_sums[:, inner:]
    weight_sum[3 * channels : 4 * channels] += matmul(xq, grad_pre, 0, 0)
    weight_sum[4 * channels : 5 * channels] += matmul(gated, grad, 0, 0)
    weight_sum[5 * channels : 5 * channels + 1] += jnp.sum(
        grad_pre.astype(jnp.float32), axis=0, keepdims=True
    )

    @pl.when(step == pl.num_programs(0) - 1)
    def _():
        for peer in range(classes):
            slot = lax.rem(peer + classes - own_class, classes)
            sent_ref[pl.ds(slot, 1), share_start : share_start + share_rows] = weight_sum[
                peer * share_rows : (peer + 1) * share_rows
            ].astype(jnp.bfloat16)[None]
        if second:
            bias_out_ref[...] = bias_sum[...].T.astype(jnp.bfloat16)
        else:
            for head in range(heads):
                bias_out_ref[:, head * positions : (head + 1) * positions] = bias_sum[
                    head * groups : (head + 1) * groups
                ].astype(jnp.bfloat16)


def whole_spec(x):
    return pl.BlockSpec(x.shape, lambda step, n=x.ndim: (0,) * n)


def kernel_weights(params):
    _, _, projection, gate_offset, out_proj, _ = params
    joined = jnp.concatenate([projection[1], projection[2]], axis=1)
    return (projection[0], joined, projection[3], out_proj, gate_offset[None])


def forward_call(own_class, rows, bias, key_bias, params, heads, positions):
    classes, _, channels = rows.shape
    groups = positions // classes
    rest = (bias, key_bias, *kernel_weights(params))
    return pl.pallas_call(
        functools.partial(forward_kernel, heads, positions),
        grid=(classes,),
        in_specs=[
            pl.BlockSpec(memory_space=pltpu.SMEM),
            pl.BlockSpec((1, *rows.shape[1:]), lambda step: (step, 0, 0)),
            *[whole_spec(x) for x in rest],
        ],
        out_specs=pl.BlockSpec((1, groups, channels), lambda step: (step, 0, 0)),
        out_shape=jax.ShapeDtypeStruct((classes, groups, channels), jnp.bfloat16),
        scratch_shapes=[pltpu.VMEM((heads * groups, positions), jnp.float32)],
        compiler_params=pltpu.CompilerParams(dimension_semantics=("arbitrary",)),
        interpret=INTERPRET,
        name="forward_rows",
    )(own_class, rows, *rest)


def backward_call(own_class, rows, bias, key_bias, grad, extra, ride, params, heads, positions,
                  share_rows):
    second = ride is None
    classes, groups, channels = grad.shape
    if second:
        ride = jnp.zeros((8, LANES), jnp.bfloat16)
        rows_spec = pl.BlockSpec((classes, 1, groups, channels), lambda step: (0, step, 0, 0))
        bias_shape = (positions, heads * groups)
        sent_rows = positions + share_rows
    else:
        rows_spec = pl.BlockSpec((1, *rows.shape[1:]), lambda step: (step, 0, 0))
        bias_shape = (groups, heads * positions)
        sent_rows = positions + groups + share_rows
    weights = kernel_weights(params)
    sent = jax.ShapeDtypeStruct((classes, sent_rows, channels), jnp.bfloat16)
    bias_out = jax.ShapeDtypeStruct(bias_shape, jnp.bfloat16)
    return pl.pallas_call(
        functools.partial(backward_kernel, heads, positions, second, share_rows),
        grid=(classes,),
        in_specs=[
            pl.BlockSpec(memory_space=pltpu.SMEM),
            rows_spec,
            whole_spec(bias),
            whole_spec(key_bias),
            pl.BlockSpec((1, groups, channels), lambda step: (step, 0, 0)),
            whole_spec(extra),
            whole_spec(ride),
            *[whole_spec(x) for x in weights],
        ],
        out_specs=[whole_spec(sent), whole_spec(bias_out)],
        out_shape=[sent, bias_out],
        scratch_shapes=[
            pltpu.VMEM((heads * groups, positions), jnp.float32),
            pltpu.VMEM((heads * groups, positions), jnp.float32),
            pltpu.VMEM((classes * share_rows, channels), jnp.float32),
            pltpu.VMEM((positions, channels), jnp.float32),
        ],
        compiler_params=pltpu.CompilerParams(dimension_semantics=("arbitrary",)),
        interpret=INTERPRET,
        name="backward_second" if second else "backward_first",
    )(own_class, rows, bias, key_bias, grad, extra, ride, *weights)


def padded_rows(x, rows):
    return jnp.pad(x, ((0, 0),) * (x.ndim - 2) + ((0, rows - x.shape[-2]), (0, 0)))


def rounded_up(value, step):
    return -(-value // step) * step


def local(
    pair_input,
    cotangent,
    residue_mask,
    norm_gain,
    norm_shift,
    proj_weights,
    gate_bias,
    out_weights,
    bias_weights,
):
    channels = pair_input.shape[2]
    groups = lax.axis_size("row")
    classes = lax.axis_size(HEAD)
    positions = groups * classes
    head_total = bias_weights.shape[2]
    bias_rows = head_total * positions // LANES
    half = jnp.bfloat16
    key_bias = (residue_mask.astype(jnp.float32) - 1.0) * MASKED
    key_bias = key_bias.reshape(groups, classes).T.reshape(1, positions)
    own_class = lax.axis_index(HEAD).astype(jnp.int32).reshape(1)
    main_rows = 5 * channels + 1
    share_rows = rounded_up(-(-(main_rows + head_total + 2) // classes), 16)
    group_rows = rounded_up(share_rows, groups) // groups
    params = [
        (
            norm_gain[which],
            norm_shift[which],
            proj_weights[which],
            gate_bias[which],
            out_weights[which],
            bias_weights[which],
        )
        for which in range(2)
    ]

    own_pair = pair_input.reshape(groups, classes, channels).transpose(1, 0, 2)
    normed_own, inverse_own, normal_own = layer_norm(own_pair, norm_gain[0], norm_shift[0])
    normal_flat = normal_own.reshape(positions, channels)
    bias_own = jnp.einsum(
        "nc,ch->hn", normal_flat, bias_weights[0], preferred_element_type=jnp.float32
    ).astype(half)
    own_cotangent = cotangent.reshape(groups, classes, channels)
    class_parts = jnp.concatenate([own_pair, own_cotangent.transpose(1, 0, 2)], axis=1)
    class_parts = rolled(class_parts, own_class[0])
    pieces = shifted_exchange(jnp.concatenate([to_all(normal_flat, HEAD), class_parts], axis=1))
    first_rows = placed(own_class, pieces)
    cotangent_query = first_rows[:, positions + groups :]
    arrived = exchanged(
        jnp.concatenate(
            [
                to_all(bias_own.reshape(bias_rows, LANES), "row"),
                own_cotangent,
            ],
            axis=1,
        ),
        "row",
    )
    first_bias = arrived[:, :bias_rows].reshape(groups, head_total * positions)
    second_grad_query = arrived[:, bias_rows:].transpose(1, 0, 2)

    after_query = forward_call(
        own_class, first_rows, first_bias, key_bias, params[0], head_total, positions
    )
    after_normed, after_inverse, after_normal = layer_norm(
        after_query, norm_gain[1], norm_shift[1]
    )
    second_bias_own = jnp.einsum(
        "abc,ch->ahb", after_normal, bias_weights[1], preferred_element_type=jnp.float32
    ).astype(half)
    after_own = exchanged(after_query, HEAD)
    arrived = exchanged(
        jnp.concatenate(
            [
                to_all(second_bias_own.reshape(bias_rows, LANES), "row"),
                after_own.transpose(1, 0, 2),
            ],
            axis=1,
        ),
        "row",
    )
    second_bias = (
        arrived[:, :bias_rows]
        .reshape(groups, classes, head_total * groups)
        .transpose(1, 0, 2)
        .reshape(positions, head_total * groups)
    )
    flipped_query = arrived[:, bias_rows:].transpose(1, 0, 2)
    _, _, second_query = layer_norm(flipped_query, norm_gain[1], norm_shift[1])
    second_rows = exchanged(to_all(second_query, HEAD), HEAD)
    sent, bias_parts = backward_call(
        own_class,
        second_rows.reshape(classes, classes, groups, channels),
        second_bias,
        key_bias,
        second_grad_query,
        jnp.zeros((8, LANES), jnp.float32),
        None,
        params[1],
        head_total,
        positions,
        share_rows,
    )

    def group_shares_of(shares):
        padded = padded_rows(shares, groups * group_rows).astype(half)
        return padded.reshape(groups, group_rows, LANES)

    pieces = shifted_exchange(sent)
    bias_parts = (
        bias_parts.reshape(classes, groups, head_total * groups)
        .transpose(1, 0, 2)
        .reshape(groups, bias_rows, LANES)
    )
    bias_arrived = exchanged(bias_parts, "row")
    total = summed(pieces)
    grad_flipped = total[:positions].astype(half)
    second_shares = total[positions:]
    arrived = exchanged(
        grad_flipped.reshape(classes, groups, channels).transpose(1, 0, 2),
        "row",
    )
    bias_total = jnp.sum(bias_arrived.astype(jnp.float32), axis=0)
    second_bias_half = bias_total.reshape(classes, head_total, groups).astype(half)
    grad_query = exchanged(arrived.transpose(1, 0, 2), HEAD)
    grad_normal = grad_query.astype(jnp.float32) + jnp.einsum(
        "ahb,ch->abc", second_bias_half, bias_weights[1], preferred_element_type=jnp.float32
    )
    end_query = norm_backward(grad_normal, after_normed, after_inverse, norm_gain[1]).astype(half)
    second_small = jnp.concatenate(
        [
            jnp.einsum(
                "abc,ahb->hc", after_normal, second_bias_half, preferred_element_type=jnp.float32
            ),
            jnp.sum(grad_normal * after_normed, axis=(0, 1))[None],
            jnp.sum(grad_normal, axis=(0, 1))[None],
        ],
        axis=0,
    )

    after_grad_query = (
        cotangent_query.astype(jnp.float32) + end_query.astype(jnp.float32)
    ).astype(half)
    extra = jnp.pad(second_small, ((1, 7 - second_small.shape[0]), (0, 0)))
    sent, bias_parts = backward_call(
        own_class,
        first_rows,
        first_bias,
        key_bias,
        after_grad_query,
        extra,
        end_query,
        params[0],
        head_total,
        positions,
        share_rows,
    )
    pieces = shifted_exchange(sent)
    bias_arrived = exchanged(bias_parts.reshape(groups, bias_rows, LANES), "row")
    grad_normal = summed([piece[:positions] for piece in pieces])
    end_own = rolled(
        jnp.stack([piece[positions : positions + groups] for piece in pieces[::-1]]),
        classes - 1 - own_class[0],
    )
    first_shares = summed([piece[positions + groups :] for piece in pieces])
    group_shares = jnp.concatenate(
        [group_shares_of(first_shares), group_shares_of(second_shares)], axis=1
    )
    shares_arrived = exchanged(padded_rows(group_shares, rounded_up(2 * group_rows, 8)), "row")
    shares_total = jnp.sum(shares_arrived[:, : 2 * group_rows].astype(jnp.float32), axis=0)
    bias_total = jnp.sum(bias_arrived.astype(jnp.float32), axis=0)
    bias_half = bias_total.reshape(head_total, positions).astype(half)
    grad_normal = grad_normal + jnp.einsum(
        "hn,ch->nc", bias_half, bias_weights[0], preferred_element_type=jnp.float32
    )
    normed_flat = normed_own.reshape(positions, channels)
    start_grad = norm_backward(
        grad_normal, normed_flat, inverse_own.reshape(positions, 1), norm_gain[0]
    )
    moved_grad = (end_own.astype(jnp.float32) + start_grad.reshape(end_own.shape)).transpose(1, 0, 2)
    pair_grad = cotangent.astype(jnp.float32) + moved_grad.reshape(1, positions, channels)
    first_small = jnp.concatenate(
        [
            jnp.einsum("nc,hn->hc", normal_flat, bias_half, preferred_element_type=jnp.float32),
            jnp.sum(grad_normal * normed_flat, axis=0)[None],
            jnp.sum(grad_normal, axis=0)[None],
        ],
        axis=0,
    )

    small_rows = first_small.shape[0]
    tail = jnp.concatenate([shares_total, first_small], axis=0).astype(half)
    tail = padded_rows(tail, rounded_up(tail.shape[0], 8))
    arrived = exchanged(to_all(tail, "row"), "row")
    whole_rows = groups * group_rows
    shared = jnp.concatenate(
        [
            arrived[:, :group_rows].reshape(whole_rows, LANES)[:share_rows],
            arrived[:, group_rows : 2 * group_rows].reshape(whole_rows, LANES)[:share_rows],
            padded_rows(
                jnp.sum(
                    arrived[:, 2 * group_rows : 2 * group_rows + small_rows].astype(jnp.float32),
                    axis=0,
                ).astype(half),
                rounded_up(small_rows, 8),
            ),
        ],
        axis=0,
    )
    arrived = exchanged(to_all(shared, HEAD), HEAD).astype(jnp.float32)
    first_whole = arrived[:, :share_rows].reshape(-1, LANES)
    second_whole = arrived[:, share_rows : 2 * share_rows].reshape(-1, LANES)
    first_small = jnp.sum(arrived[:, 2 * share_rows : 2 * share_rows + small_rows], axis=0)
    second_small = first_whole[main_rows : main_rows + small_rows]
    proj_rows = 4 * channels

    def both(first, second):
        return jnp.stack([first, second])

    return (
        pair_grad,
        both(first_whole[:proj_rows], second_whole[:proj_rows]).reshape(
            2, 4, channels, -1
        ),
        both(first_whole[main_rows - 1], second_whole[main_rows - 1]),
        both(first_whole[proj_rows : main_rows - 1], second_whole[proj_rows : main_rows - 1]),
        both(first_small[:head_total].T, second_small[:head_total].T),
        both(first_small[head_total], second_small[head_total]),
        both(first_small[head_total + 1], second_small[head_total + 1]),
    )


def solution(mesh):
    finer = Mesh(mesh.devices.reshape(mesh.shape["row"], 4, 2), ("row", "head_0", "head_1"))
    in_specs = (P(ROW_HEAD, None, None), P(ROW_HEAD, None, None), P(), P(), P(), P(), P(), P(), P())
    out_specs = (P(ROW_HEAD, None, None), P(), P(), P(), P(), P(), P())

    return jax.shard_map(local, mesh=finer, in_specs=in_specs, out_specs=out_specs, check_vma=False)
```

```python
import functools
import math

import jax
import jax.numpy as jnp
from jax import lax
from jax.experimental import pallas as pl
from jax.experimental.pallas import tpu as pltpu
from jax.sharding import Mesh
from jax.sharding import PartitionSpec as P


HEAD = ("head_0", "head_1")
ROW_HEAD = ("row", "head_0", "head_1")


EPS = 1e-05
MASKED = 1000000000.0
LANES = 128
INTERPRET = False


def exchanged(parts, axis):
    return lax.all_to_all(parts, axis, split_axis=0, concat_axis=0, tiled=True)


def shifted_exchange(parts):
    count = parts.shape[0]
    pieces = [parts[0]]
    for shift in range(1, count):
        pairs = [(at, (at + shift) % count) for at in range(count)]
        pieces.append(lax.ppermute(parts[shift], HEAD, pairs))
    return pieces


def rolled(x, by):
    return lax.dynamic_slice_in_dim(jnp.concatenate([x, x]), by, x.shape[0], axis=0)


def place_kernel(own_ref, *refs):
    count = len(refs) - 1
    for shift in range(count):
        place = lax.rem(own_ref[0] + (count - shift), count)
        refs[-1][pl.ds(place, 1)] = refs[shift][...][None]


def placed(own_class, pieces):
    return pl.pallas_call(
        place_kernel,
        in_specs=[
            pl.BlockSpec(memory_space=pltpu.SMEM),
            *[pl.BlockSpec(memory_space=pltpu.VMEM) for _ in pieces],
        ],
        out_specs=pl.BlockSpec(memory_space=pltpu.VMEM),
        out_shape=jax.ShapeDtypeStruct((len(pieces), *pieces[0].shape), pieces[0].dtype),
        interpret=INTERPRET,
        name="place_pieces",
    )(own_class, *pieces)


def to_all(x, axis):
    return jnp.broadcast_to(x[None], (lax.axis_size(axis), *x.shape))


def layer_norm(values, norm_scale, norm_offset):
    floats = values.astype(jnp.float32)
    centred = floats - jnp.mean(floats, axis=-1, keepdims=True)
    inverse = lax.rsqrt(jnp.mean(centred * centred, axis=-1, keepdims=True) + EPS)
    normed = centred * inverse
    return (normed, inverse, (normed * norm_scale + norm_offset).astype(jnp.bfloat16))


def norm_backward(grad_normal, normed, inverse, norm_scale):
    grad_hat = grad_normal * norm_scale
    first_mean = jnp.mean(grad_hat, axis=-1, keepdims=True)
    second_mean = jnp.mean(grad_hat * normed, axis=-1, keepdims=True)
    return inverse * (grad_hat - first_mean - normed * second_mean)


def matmul(a, b, a_dim, b_dim):
    return lax.dot_general(
        a, b, (((a_dim,), (b_dim,)), ((), ())), preferred_element_type=jnp.float32
    )


def lanes_of_head(shape, head, head_size):
    lanes = lax.broadcasted_iota(jnp.int32, shape, 1)
    return (lanes >= head * head_size) & (lanes < (head + 1) * head_size)


def spread_heads(values, heads):
    size = values.shape[1] // heads
    kept = [
        jnp.where(lanes_of_head(values.shape, head, size), values, 0.0) for head in range(heads)
    ]
    return jnp.concatenate(kept, axis=0).astype(jnp.bfloat16)


def picked_heads(stacked, heads):
    rows = stacked.shape[0] // heads
    size = stacked.shape[1] // heads
    total = jnp.zeros((rows, stacked.shape[1]), jnp.float32)
    for head in range(heads):
        part = stacked[head * rows : (head + 1) * rows]
        total = jnp.where(lanes_of_head(part.shape, head, size), part, total)
    return total


def attention(x, xq, bias, wq, wkv, wg, gate_offset, heads):
    channels = wq.shape[1]
    scale = 1.0 / math.sqrt(channels // heads)
    queries = spread_heads(
        (matmul(xq, wq, 1, 0) * scale).astype(jnp.bfloat16).astype(jnp.float32), heads
    )
    key_value = matmul(x, wkv, 1, 0).astype(jnp.bfloat16)
    keys = key_value[:, :channels]
    values = key_value[:, channels:]
    gate = jax.nn.sigmoid(matmul(xq, wg, 1, 0) + gate_offset)
    logits = matmul(queries, keys, 1, 1) + bias
    weights = jnp.exp(logits - jnp.max(logits, axis=1, keepdims=True))
    probs = weights / jnp.sum(weights, axis=1, keepdims=True)
    probs_half = probs.astype(jnp.bfloat16)
    attended = picked_heads(matmul(probs_half, values, 1, 0), heads)
    return (queries, keys, values, gate, probs, probs_half, attended)


def split_bias(bias, key_bias, heads):
    count = bias.shape[1] // heads
    parts = [bias[:, head * count : (head + 1) * count] for head in range(heads)]
    return jnp.concatenate(parts, axis=0).astype(jnp.float32) + key_bias


def forward_kernel(heads, positions, class_ref, rows_ref, bias_ref, mask_ref, wq_ref, wkv_ref,
                   wg_ref, wo_ref, gate_ref, gain_ref, shift_ref, after_ref, normal_ref, full_bias):
    groups = after_ref.shape[1]

    @pl.when(pl.program_id(0) == 0)
    def _():
        full_bias[...] = split_bias(bias_ref[...], mask_ref[...], heads)

    x = rows_ref[0, :positions]
    start = pl.multiple_of(class_ref[0] * groups, groups)
    xq = rows_ref[0, pl.ds(start, groups)]
    result = attention(
        x, xq, full_bias[...], wq_ref[...], wkv_ref[...], wg_ref[...], gate_ref[...], heads
    )
    gated = (result[3] * result[6]).astype(jnp.bfloat16)
    update = matmul(gated, wo_ref[...], 1, 0).astype(jnp.bfloat16)
    pair = rows_ref[0, positions : positions + groups]
    after = (pair.astype(jnp.float32) + update.astype(jnp.float32)).astype(jnp.bfloat16)
    after_ref[0] = after
    _, _, normal = layer_norm(after, gain_ref[...], shift_ref[...])
    normal_ref[0] = normal


def backward_kernel(heads, positions, second, share_rows, class_ref, rows_ref, bias_ref, mask_ref,
                    grad_ref, extra_ref, ride_ref, wq_ref, wkv_ref, wg_ref, wo_ref, gate_ref,
                    sent_ref, bias_out_ref, full_bias, bias_sum, weight_sum, share):
    step = pl.program_id(0)
    classes = sent_ref.shape[0]
    groups = positions // classes
    channels = wq_ref.shape[0]
    inner = wq_ref.shape[1]
    own_class = class_ref[0]
    share_start = positions if second else positions + groups

    @pl.when(step == 0)
    def _():
        if second:
            full_bias[...] = bias_ref[...].astype(jnp.float32).T + mask_ref[...]
        else:
            full_bias[...] = split_bias(bias_ref[...], mask_ref[...], heads)
            sent_ref[:, positions : positions + groups] = ride_ref[...]
        bias_sum[...] = jnp.zeros(bias_sum.shape, jnp.float32)
        weight_sum[...] = jnp.zeros(weight_sum.shape, jnp.float32)
        weight_sum[5 * channels : 5 * channels + 8] = extra_ref[...]

    if second:
        x = rows_ref[:, 0].reshape(positions, channels)
        xq = rows_ref[pl.ds(own_class, 1), 0].reshape(groups, channels)
    else:
        x = rows_ref[0, :positions]
        xq = rows_ref[0, pl.ds(pl.multiple_of(own_class * groups, groups), groups)]
    queries, keys, values, gate, probs, probs_half, attended = attention(
        x, xq, full_bias[...], wq_ref[...], wkv_ref[...], wg_ref[...], gate_ref[...], heads
    )
    scale = 1.0 / math.sqrt(inner // heads)
    grad = grad_ref[0]
    gated = (gate * attended).astype(jnp.bfloat16)
    grad_gated = matmul(grad, wo_ref[...], 1, 1)
    grad_att = (grad_gated * gate).astype(jnp.bfloat16).astype(jnp.float32)
    grad_pre = (grad_gated * attended * gate * (1.0 - gate)).astype(jnp.bfloat16)
    grad_heads = spread_heads(grad_att, heads)
    grad_probs = matmul(grad_heads, values, 1, 1)
    grad_logits = probs * (grad_probs - jnp.sum(probs * grad_probs, axis=1, keepdims=True))
    bias_sum[...] += grad_logits
    logits_half = grad_logits.astype(jnp.bfloat16)
    grad_queries = (picked_heads(matmul(logits_half, keys, 1, 0), heads) * scale).astype(
        jnp.bfloat16
    )
    grad_keys = matmul(logits_half, queries, 0, 0).astype(jnp.bfloat16)
    grad_values = matmul(probs_half, grad_heads, 0, 0).astype(jnp.bfloat16)
    grad_pairs = jnp.concatenate([grad_keys, grad_values], axis=1)
    share[...] = matmul(grad_pairs, wkv_ref[...], 1, 1)
    query_side = matmul(grad_queries, wq_ref[...], 1, 1) + matmul(grad_pre, wg_ref[...], 1, 1)
    own_rows = pl.ds(pl.multiple_of(own_class * groups, groups), groups)
    share[own_rows] = share[own_rows] + query_side
    partial = share[...].astype(jnp.bfloat16)
    if second:
        place = pl.ds(pl.multiple_of(step * groups, groups), groups)
        sent_ref[:, place] = partial.reshape(classes, groups, channels)
    else:
        sent_ref[pl.ds(step, 1), :positions] = partial[None]
    pair_sums = matmul(x, grad_pairs, 0, 0)
    weight_sum[:channels] += matmul(xq, grad_queries, 0, 0)
    weight_sum[channels : 2 * channels] += pair_sums[:, :inner]
    weight_sum[2 * channels : 3 * channels] += pair_sums[:, inner:]
    weight_sum[3 * channels : 4 * channels] += matmul(xq, grad_pre, 0, 0)
    weight_sum[4 * channels : 5 * channels] += matmul(gated, grad, 0, 0)
    weight_sum[5 * channels : 5 * channels + 1] += jnp.sum(
        grad_pre.astype(jnp.float32), axis=0, keepdims=True
    )

    @pl.when(step == pl.num_programs(0) - 1)
    def _():
        for peer in range(classes):
            sent_ref[peer, share_start : share_start + share_rows] = weight_sum[
                peer * share_rows : (peer + 1) * share_rows
            ].astype(jnp.bfloat16)
        if second:
            bias_out_ref[...] = bias_sum[...].T.astype(jnp.bfloat16)
        else:
            for head in range(heads):
                bias_out_ref[:, head * positions : (head + 1) * positions] = bias_sum[
                    head * groups : (head + 1) * groups
                ].astype(jnp.bfloat16)


def whole_spec(x):
    return pl.BlockSpec(x.shape, lambda step, n=x.ndim: (0,) * n)


def kernel_weights(params):
    _, _, projection, gate_offset, out_proj, _ = params
    joined = jnp.concatenate([projection[1], projection[2]], axis=1)
    return (projection[0], joined, projection[3], out_proj, gate_offset[None])


def forward_call(own_class, rows, bias, key_bias, params, next_params, heads, positions):
    classes, _, channels = rows.shape
    groups = positions // classes
    rest = (
        bias,
        key_bias,
        *kernel_weights(params),
        next_params[0][None],
        next_params[1][None],
    )
    result_spec = pl.BlockSpec((1, groups, channels), lambda step: (step, 0, 0))
    result = jax.ShapeDtypeStruct((classes, groups, channels), jnp.bfloat16)
    return pl.pallas_call(
        functools.partial(forward_kernel, heads, positions),
        grid=(classes,),
        in_specs=[
            pl.BlockSpec(memory_space=pltpu.SMEM),
            pl.BlockSpec((1, *rows.shape[1:]), lambda step: (step, 0, 0)),
            *[whole_spec(x) for x in rest],
        ],
        out_specs=[result_spec, result_spec],
        out_shape=[result, result],
        scratch_shapes=[pltpu.VMEM((heads * groups, positions), jnp.float32)],
        compiler_params=pltpu.CompilerParams(dimension_semantics=("arbitrary",)),
        interpret=INTERPRET,
        name="forward_rows",
    )(own_class, rows, *rest)


def backward_call(own_class, rows, bias, key_bias, grad, extra, ride, params, heads, positions,
                  share_rows):
    second = ride is None
    classes, groups, channels = grad.shape
    if second:
        ride = jnp.zeros((8, LANES), jnp.bfloat16)
        rows_spec = pl.BlockSpec((classes, 1, groups, channels), lambda step: (0, step, 0, 0))
        bias_shape = (positions, heads * groups)
        sent_rows = positions + share_rows
    else:
        rows_spec = pl.BlockSpec((1, *rows.shape[1:]), lambda step: (step, 0, 0))
        bias_shape = (groups, heads * positions)
        sent_rows = positions + groups + share_rows
    weights = kernel_weights(params)
    sent = jax.ShapeDtypeStruct((classes, sent_rows, channels), jnp.bfloat16)
    bias_out = jax.ShapeDtypeStruct(bias_shape, jnp.bfloat16)
    return pl.pallas_call(
        functools.partial(backward_kernel, heads, positions, second, share_rows),
        grid=(classes,),
        in_specs=[
            pl.BlockSpec(memory_space=pltpu.SMEM),
            rows_spec,
            whole_spec(bias),
            whole_spec(key_bias),
            pl.BlockSpec((1, groups, channels), lambda step: (step, 0, 0)),
            whole_spec(extra),
            whole_spec(ride),
            *[whole_spec(x) for x in weights],
        ],
        out_specs=[whole_spec(sent), whole_spec(bias_out)],
        out_shape=[sent, bias_out],
        scratch_shapes=[
            pltpu.VMEM((heads * groups, positions), jnp.float32),
            pltpu.VMEM((heads * groups, positions), jnp.float32),
            pltpu.VMEM((classes * share_rows, channels), jnp.float32),
            pltpu.VMEM((positions, channels), jnp.float32),
        ],
        compiler_params=pltpu.CompilerParams(dimension_semantics=("arbitrary",)),
        interpret=INTERPRET,
        name="backward_second" if second else "backward_first",
    )(own_class, rows, bias, key_bias, grad, extra, ride, *weights)


def padded_rows(x, rows):
    return jnp.pad(x, ((0, 0),) * (x.ndim - 2) + ((0, rows - x.shape[-2]), (0, 0)))


def rounded_up(value, step):
    return -(-value // step) * step


def local(
    pair_input,
    cotangent,
    residue_mask,
    norm_gain,
    norm_shift,
    proj_weights,
    gate_bias,
    out_weights,
    bias_weights,
):
    channels = pair_input.shape[2]
    groups = lax.axis_size("row")
    classes = lax.axis_size(HEAD)
    positions = groups * classes
    head_total = bias_weights.shape[2]
    bias_rows = head_total * positions // LANES
    half = jnp.bfloat16
    key_bias = (residue_mask.astype(jnp.float32) - 1.0) * MASKED
    key_bias = key_bias.reshape(groups, classes).T.reshape(1, positions)
    own_class = lax.axis_index(HEAD).astype(jnp.int32).reshape(1)
    main_rows = 5 * channels + 1
    share_rows = rounded_up(-(-(main_rows + head_total + 2) // classes), 16)
    group_rows = rounded_up(share_rows, groups) // groups
    params = [
        (
            norm_gain[which],
            norm_shift[which],
            proj_weights[which],
            gate_bias[which],
            out_weights[which],
            bias_weights[which],
        )
        for which in range(2)
    ]

    own_pair = pair_input.reshape(groups, classes, channels).transpose(1, 0, 2)
    normed_own, inverse_own, normal_own = layer_norm(own_pair, norm_gain[0], norm_shift[0])
    normal_flat = normal_own.reshape(positions, channels)
    bias_own = jnp.einsum(
        "nc,ch->hn", normal_flat, bias_weights[0], preferred_element_type=jnp.float32
    ).astype(half)
    own_cotangent = cotangent.reshape(groups, classes, channels)
    class_parts = jnp.concatenate([own_pair, own_cotangent.transpose(1, 0, 2)], axis=1)
    class_parts = rolled(class_parts, own_class[0])
    pieces = shifted_exchange(jnp.concatenate([to_all(normal_flat, HEAD), class_parts], axis=1))
    first_rows = placed(own_class, pieces)
    cotangent_query = first_rows[:, positions + groups :]
    arrived = exchanged(
        jnp.concatenate(
            [
                to_all(bias_own.reshape(bias_rows, LANES), "row"),
                own_cotangent,
            ],
            axis=1,
        ),
        "row",
    )
    first_bias = arrived[:, :bias_rows].reshape(groups, head_total * positions)
    second_grad_query = arrived[:, bias_rows:].transpose(1, 0, 2)

    after_query, after_normal = forward_call(
        own_class, first_rows, first_bias, key_bias, params[0], params[1], head_total, positions
    )
    after_normed, after_inverse, _ = layer_norm(after_query, norm_gain[1], norm_shift[1])
    second_bias_own = jnp.einsum(
        "abc,ch->ahb", after_normal, bias_weights[1], preferred_element_type=jnp.float32
    ).astype(half)
    after_own = exchanged(after_normal, HEAD)
    arrived = exchanged(
        jnp.concatenate(
            [
                to_all(second_bias_own.reshape(bias_rows, LANES), "row"),
                after_own.transpose(1, 0, 2),
            ],
            axis=1,
        ),
        "row",
    )
    second_bias = (
        arrived[:, :bias_rows]
        .reshape(groups, classes, head_total * groups)
        .transpose(1, 0, 2)
        .reshape(positions, head_total * groups)
    )
    second_query = arrived[:, bias_rows:].transpose(1, 0, 2)
    second_rows = exchanged(to_all(second_query, HEAD), HEAD)
    sent, bias_parts = backward_call(
        own_class,
        second_rows.reshape(classes, classes, groups, channels),
        second_bias,
        key_bias,
        second_grad_query,
        jnp.zeros((8, LANES), jnp.float32),
        None,
        params[1],
        head_total,
        positions,
        share_rows,
    )

    def group_shares_of(arrived_shares):
        summed = jnp.sum(arrived_shares.astype(jnp.float32), axis=0)
        summed = padded_rows(summed, groups * group_rows).astype(half)
        return summed.reshape(groups, group_rows, LANES)

    arrived = exchanged(sent, HEAD)
    second_shares = group_shares_of(arrived[:, positions:])
    grad_flipped = jnp.sum(arrived[:, :positions].astype(jnp.float32), axis=0).astype(half)
    bias_parts = (
        bias_parts.reshape(classes, groups, head_total * groups)
        .transpose(1, 0, 2)
        .reshape(groups, bias_rows, LANES)
    )
    arrived = exchanged(
        jnp.concatenate(
            [
                bias_parts,
                grad_flipped.reshape(classes, groups, channels).transpose(1, 0, 2),
            ],
            axis=1,
        ),
        "row",
    )
    summed = jnp.sum(arrived[:, :bias_rows].astype(jnp.float32), axis=0)
    second_bias_half = summed.reshape(classes, head_total, groups).astype(half)
    grad_query = exchanged(arrived[:, bias_rows : bias_rows + classes].transpose(1, 0, 2), HEAD)
    grad_normal = grad_query.astype(jnp.float32) + jnp.einsum(
        "ahb,ch->abc", second_bias_half, bias_weights[1], preferred_element_type=jnp.float32
    )
    end_query = norm_backward(grad_normal, after_normed, after_inverse, norm_gain[1]).astype(half)
    second_small = jnp.concatenate(
        [
            jnp.einsum(
                "abc,ahb->hc", after_normal, second_bias_half, preferred_element_type=jnp.float32
            ),
            jnp.sum(grad_normal * after_normed, axis=(0, 1))[None],
            jnp.sum(grad_normal, axis=(0, 1))[None],
        ],
        axis=0,
    )

    after_grad_query = (
        cotangent_query.astype(jnp.float32) + end_query.astype(jnp.float32)
    ).astype(half)
    extra = jnp.pad(second_small, ((1, 7 - second_small.shape[0]), (0, 0)))
    sent, bias_parts = backward_call(
        own_class,
        first_rows,
        first_bias,
        key_bias,
        after_grad_query,
        extra,
        end_query,
        params[0],
        head_total,
        positions,
        share_rows,
    )
    arrived = exchanged(sent, HEAD)
    grad_normal = jnp.sum(arrived[:, :positions].astype(jnp.float32), axis=0)
    end_own = arrived[:, positions : positions + groups]
    shares = arrived[:, positions + groups :]
    arrived = exchanged(
        jnp.concatenate(
            [
                bias_parts.reshape(groups, bias_rows, LANES),
                padded_rows(
                    jnp.concatenate([group_shares_of(shares), second_shares], axis=1),
                    rounded_up(2 * group_rows, 8),
                ),
            ],
            axis=1,
        ),
        "row",
    )
    summed = jnp.sum(arrived[:, :bias_rows].astype(jnp.float32), axis=0)
    bias_half = summed.reshape(head_total, positions).astype(half)
    shares_total = jnp.sum(
        arrived[:, bias_rows : bias_rows + 2 * group_rows].astype(jnp.float32), axis=0
    )
    grad_normal = grad_normal + jnp.einsum(
        "hn,ch->nc", bias_half, bias_weights[0], preferred_element_type=jnp.float32
    )
    normed_flat = normed_own.reshape(positions, channels)
    start_grad = norm_backward(
        grad_normal, normed_flat, inverse_own.reshape(positions, 1), norm_gain[0]
    )
    moved_grad = (end_own.astype(jnp.float32) + start_grad.reshape(end_own.shape)).transpose(1, 0, 2)
    pair_grad = cotangent.astype(jnp.float32) + moved_grad.reshape(1, positions, channels)
    first_small = jnp.concatenate(
        [
            jnp.einsum("nc,hn->hc", normal_flat, bias_half, preferred_element_type=jnp.float32),
            jnp.sum(grad_normal * normed_flat, axis=0)[None],
            jnp.sum(grad_normal, axis=0)[None],
        ],
        axis=0,
    )

    small_rows = first_small.shape[0]
    tail = jnp.concatenate([shares_total, first_small], axis=0).astype(half)
    tail = padded_rows(tail, rounded_up(tail.shape[0], 8))
    arrived = exchanged(to_all(tail, "row"), "row")
    whole_rows = groups * group_rows
    shared = jnp.concatenate(
        [
            arrived[:, :group_rows].reshape(whole_rows, LANES)[:share_rows],
            arrived[:, group_rows : 2 * group_rows].reshape(whole_rows, LANES)[:share_rows],
            padded_rows(
                jnp.sum(
                    arrived[:, 2 * group_rows : 2 * group_rows + small_rows].astype(jnp.float32),
                    axis=0,
                ).astype(half),
                rounded_up(small_rows, 8),
            ),
        ],
        axis=0,
    )
    arrived = exchanged(to_all(shared, HEAD), HEAD).astype(jnp.float32)
    first_whole = arrived[:, :share_rows].reshape(-1, LANES)
    second_whole = arrived[:, share_rows : 2 * share_rows].reshape(-1, LANES)
    first_small = jnp.sum(arrived[:, 2 * share_rows : 2 * share_rows + small_rows], axis=0)
    second_small = first_whole[main_rows : main_rows + small_rows]
    proj_rows = 4 * channels

    def both(first, second):
        return jnp.stack([first, second])

    return (
        pair_grad,
        both(first_whole[:proj_rows], second_whole[:proj_rows]).reshape(
            2, 4, channels, -1
        ),
        both(first_whole[main_rows - 1], second_whole[main_rows - 1]),
        both(first_whole[proj_rows : main_rows - 1], second_whole[proj_rows : main_rows - 1]),
        both(first_small[:head_total].T, second_small[:head_total].T),
        both(first_small[head_total], second_small[head_total]),
        both(first_small[head_total + 1], second_small[head_total + 1]),
    )


def solution(mesh):
    finer = Mesh(mesh.devices.reshape(mesh.shape["row"], 4, 2), ("row", "head_0", "head_1"))
    in_specs = (P(ROW_HEAD, None, None), P(ROW_HEAD, None, None), P(), P(), P(), P(), P(), P(), P())
    out_specs = (P(ROW_HEAD, None, None), P(), P(), P(), P(), P(), P())

    return jax.shard_map(local, mesh=finer, in_specs=in_specs, out_specs=out_specs, check_vma=False)
```

```python
import functools
import math

import jax
import jax.numpy as jnp
from jax import lax
from jax.experimental import pallas as pl
from jax.experimental.pallas import tpu as pltpu
from jax.sharding import Mesh
from jax.sharding import PartitionSpec as P


HEAD = ("head_0", "head_1")
ROW_HEAD = ("row", "head_0", "head_1")


EPS = 1e-05
MASKED = 1000000000.0
LANES = 128
INTERPRET = False


def exchanged(parts, axis):
    return lax.all_to_all(parts, axis, split_axis=0, concat_axis=0, tiled=True)


def shifted_exchange(parts):
    count = parts.shape[0]
    pieces = [parts[0]]
    for shift in range(1, count):
        pairs = [(at, (at + shift) % count) for at in range(count)]
        pieces.append(lax.ppermute(parts[shift], HEAD, pairs))
    return pieces


def rolled(x, by):
    return lax.dynamic_slice_in_dim(jnp.concatenate([x, x]), by, x.shape[0], axis=0)


def place_kernel(own_ref, *refs):
    count = len(refs) - 1
    for shift in range(count):
        place = lax.rem(own_ref[0] + (count - shift), count)
        refs[-1][pl.ds(place, 1)] = refs[shift][...][None]


def placed(own_class, pieces):
    return pl.pallas_call(
        place_kernel,
        in_specs=[
            pl.BlockSpec(memory_space=pltpu.SMEM),
            *[pl.BlockSpec(memory_space=pltpu.VMEM) for _ in pieces],
        ],
        out_specs=pl.BlockSpec(memory_space=pltpu.VMEM),
        out_shape=jax.ShapeDtypeStruct((len(pieces), *pieces[0].shape), pieces[0].dtype),
        interpret=INTERPRET,
        name="place_pieces",
    )(own_class, *pieces)


def to_all(x, axis):
    return jnp.broadcast_to(x[None], (lax.axis_size(axis), *x.shape))


def layer_norm(values, norm_scale, norm_offset):
    floats = values.astype(jnp.float32)
    centred = floats - jnp.mean(floats, axis=-1, keepdims=True)
    inverse = lax.rsqrt(jnp.mean(centred * centred, axis=-1, keepdims=True) + EPS)
    normed = centred * inverse
    return (normed, inverse, (normed * norm_scale + norm_offset).astype(jnp.bfloat16))


def norm_backward(grad_normal, normed, inverse, norm_scale):
    grad_hat = grad_normal * norm_scale
    first_mean = jnp.mean(grad_hat, axis=-1, keepdims=True)
    second_mean = jnp.mean(grad_hat * normed, axis=-1, keepdims=True)
    return inverse * (grad_hat - first_mean - normed * second_mean)


def matmul(a, b, a_dim, b_dim):
    return lax.dot_general(
        a, b, (((a_dim,), (b_dim,)), ((), ())), preferred_element_type=jnp.float32
    )


def lanes_of_head(shape, head, head_size):
    lanes = lax.broadcasted_iota(jnp.int32, shape, 1)
    return (lanes >= head * head_size) & (lanes < (head + 1) * head_size)


def spread_heads(values, heads):
    size = values.shape[1] // heads
    kept = [
        jnp.where(lanes_of_head(values.shape, head, size), values, 0.0) for head in range(heads)
    ]
    return jnp.concatenate(kept, axis=0).astype(jnp.bfloat16)


def picked_heads(stacked, heads):
    rows = stacked.shape[0] // heads
    size = stacked.shape[1] // heads
    total = jnp.zeros((rows, stacked.shape[1]), jnp.float32)
    for head in range(heads):
        part = stacked[head * rows : (head + 1) * rows]
        total = jnp.where(lanes_of_head(part.shape, head, size), part, total)
    return total


def attention(x, xq, bias, wq, wkv, wg, gate_offset, heads):
    channels = wq.shape[1]
    scale = 1.0 / math.sqrt(channels // heads)
    queries = spread_heads(
        (matmul(xq, wq, 1, 0) * scale).astype(jnp.bfloat16).astype(jnp.float32), heads
    )
    pairs = matmul(x, wkv, 1, 0).astype(jnp.bfloat16)
    keys = pairs[:, :channels]
    values = pairs[:, channels:]
    gate = jax.nn.sigmoid(matmul(xq, wg, 1, 0) + gate_offset)
    logits = matmul(queries, keys, 1, 1) + bias
    weights = jnp.exp(logits - jnp.max(logits, axis=1, keepdims=True))
    probs = weights / jnp.sum(weights, axis=1, keepdims=True)
    probs_half = probs.astype(jnp.bfloat16)
    attended = picked_heads(matmul(probs_half, values, 1, 0), heads)
    return (queries, pairs, probs, gate, attended)


def split_bias(bias, key_bias, heads):
    count = bias.shape[1] // heads
    parts = [bias[:, head * count : (head + 1) * count] for head in range(heads)]
    return jnp.concatenate(parts, axis=0).astype(jnp.float32) + key_bias


def forward_kernel(heads, positions, class_ref, rows_ref, bias_ref, mask_ref, wq_ref, wkv_ref,
                   wg_ref, wo_ref, gate_ref, gain_ref, shift_ref, after_ref, normal_ref, queries_ref, pairs_ref, probs_ref,
                   gates_ref, attended_ref, full_bias):
    groups = after_ref.shape[1]

    @pl.when(pl.program_id(0) == 0)
    def _():
        full_bias[...] = split_bias(bias_ref[...], mask_ref[...], heads)

    x = rows_ref[0, :positions]
    start = pl.multiple_of(class_ref[0] * groups, groups)
    xq = rows_ref[0, pl.ds(start, groups)]
    queries, pairs, probs, gate, attended = attention(
        x, xq, full_bias[...], wq_ref[...], wkv_ref[...], wg_ref[...], gate_ref[...], heads
    )
    queries_ref[0] = queries
    pairs_ref[0] = pairs
    probs_ref[0] = probs
    gates_ref[0] = gate
    attended_ref[0] = attended
    gated = (gate * attended).astype(jnp.bfloat16)
    update = matmul(gated, wo_ref[...], 1, 0).astype(jnp.bfloat16)
    pair = rows_ref[0, positions : positions + groups]
    after = (pair.astype(jnp.float32) + update.astype(jnp.float32)).astype(jnp.bfloat16)
    after_ref[0] = after
    _, _, normal = layer_norm(after, gain_ref[...], shift_ref[...])
    normal_ref[0] = normal


def backward_kernel(heads, positions, second, share_rows, class_ref, rows_ref, grad_ref, wq_ref,
                    wkv_ref, wg_ref, wo_ref, gate_ref, *refs):
    if second:
        bias_ref, mask_ref = refs[:2]
        full_bias = refs[-1]
        sent_ref, bias_out_ref, bias_sum, weight_sum, share = refs[2:-1]
    else:
        queries_ref, pairs_ref, probs_ref, gates_ref, attended_ref, extra_ref, ride_ref = refs[:7]
        sent_ref, bias_out_ref, bias_sum, weight_sum, share = refs[7:]
    step = pl.program_id(0)
    classes = sent_ref.shape[0]
    groups = positions // classes
    channels = wq_ref.shape[0]
    inner = wq_ref.shape[1]
    own_class = class_ref[0]
    share_start = positions if second else positions + groups

    @pl.when(step == 0)
    def _():
        if second:
            full_bias[...] = bias_ref[...].astype(jnp.float32).T + mask_ref[...]
        else:
            sent_ref[:, positions : positions + groups] = ride_ref[...]
        bias_sum[...] = jnp.zeros(bias_sum.shape, jnp.float32)
        weight_sum[...] = jnp.zeros(weight_sum.shape, jnp.float32)
        if not second:
            weight_sum[5 * channels : 5 * channels + 8] = extra_ref[...]

    if second:
        x = rows_ref[:, 0].reshape(positions, channels)
        xq = rows_ref[pl.ds(own_class, 1), 0].reshape(groups, channels)
    else:
        x = rows_ref[0, :positions]
        xq = rows_ref[0, pl.ds(pl.multiple_of(own_class * groups, groups), groups)]
    if second:
        queries, pairs, probs, gate, attended = attention(
            x, xq, full_bias[...], wq_ref[...], wkv_ref[...], wg_ref[...], gate_ref[...], heads
        )
    else:
        queries, pairs, probs, gate, attended = (
            ref[0] for ref in (queries_ref, pairs_ref, probs_ref, gates_ref, attended_ref)
        )
    keys = pairs[:, :inner]
    values = pairs[:, inner:]
    probs_half = probs.astype(jnp.bfloat16)
    scale = 1.0 / math.sqrt(inner // heads)
    grad = grad_ref[0]
    gated = (gate * attended).astype(jnp.bfloat16)
    grad_gated = matmul(grad, wo_ref[...], 1, 1)
    grad_att = (grad_gated * gate).astype(jnp.bfloat16).astype(jnp.float32)
    grad_pre = (grad_gated * attended * gate * (1.0 - gate)).astype(jnp.bfloat16)
    grad_heads = spread_heads(grad_att, heads)
    grad_probs = matmul(grad_heads, values, 1, 1)
    grad_logits = probs * (grad_probs - jnp.sum(probs * grad_probs, axis=1, keepdims=True))
    bias_sum[...] += grad_logits
    logits_half = grad_logits.astype(jnp.bfloat16)
    grad_queries = (picked_heads(matmul(logits_half, keys, 1, 0), heads) * scale).astype(
        jnp.bfloat16
    )
    grad_keys = matmul(logits_half, queries, 0, 0).astype(jnp.bfloat16)
    grad_values = matmul(probs_half, grad_heads, 0, 0).astype(jnp.bfloat16)
    grad_pairs = jnp.concatenate([grad_keys, grad_values], axis=1)
    share[...] = matmul(grad_pairs, wkv_ref[...], 1, 1)
    query_side = matmul(grad_queries, wq_ref[...], 1, 1) + matmul(grad_pre, wg_ref[...], 1, 1)
    own_rows = pl.ds(pl.multiple_of(own_class * groups, groups), groups)
    share[own_rows] = share[own_rows] + query_side
    partial = share[...].astype(jnp.bfloat16)
    if second:
        place = pl.ds(pl.multiple_of(step * groups, groups), groups)
        sent_ref[:, place] = partial.reshape(classes, groups, channels)
    else:
        sent_ref[pl.ds(step, 1), :positions] = partial[None]
    pair_sums = matmul(x, grad_pairs, 0, 0)
    weight_sum[:channels] += matmul(xq, grad_queries, 0, 0)
    weight_sum[channels : 2 * channels] += pair_sums[:, :inner]
    weight_sum[2 * channels : 3 * channels] += pair_sums[:, inner:]
    weight_sum[3 * channels : 4 * channels] += matmul(xq, grad_pre, 0, 0)
    weight_sum[4 * channels : 5 * channels] += matmul(gated, grad, 0, 0)
    weight_sum[5 * channels : 5 * channels + 1] += jnp.sum(
        grad_pre.astype(jnp.float32), axis=0, keepdims=True
    )

    @pl.when(step == pl.num_programs(0) - 1)
    def _():
        for peer in range(classes):
            sent_ref[peer, share_start : share_start + share_rows] = weight_sum[
                peer * share_rows : (peer + 1) * share_rows
            ].astype(jnp.bfloat16)
        if second:
            bias_out_ref[...] = bias_sum[...].T.astype(jnp.bfloat16)
        else:
            for head in range(heads):
                bias_out_ref[:, head * positions : (head + 1) * positions] = bias_sum[
                    head * groups : (head + 1) * groups
                ].astype(jnp.bfloat16)


def whole_spec(x):
    return pl.BlockSpec(x.shape, lambda step, n=x.ndim: (0,) * n)


def kernel_weights(params):
    _, _, projection, gate_offset, out_proj, _ = params
    joined = jnp.concatenate([projection[1], projection[2]], axis=1)
    return (projection[0], joined, projection[3], out_proj, gate_offset[None])


def step_spec(shape):
    return pl.BlockSpec((1, *shape[1:]), lambda step, n=len(shape): (step,) + (0,) * (n - 1))


def forward_call(own_class, rows, bias, key_bias, params, next_params, heads, positions):
    classes, _, channels = rows.shape
    groups = positions // classes
    inner = params[2].shape[2]
    half = jnp.bfloat16
    rest = (
        bias,
        key_bias,
        *kernel_weights(params),
        next_params[0][None],
        next_params[1][None],
    )
    results = [
        jax.ShapeDtypeStruct((classes, groups, channels), half),
        jax.ShapeDtypeStruct((classes, groups, channels), half),
        jax.ShapeDtypeStruct((classes, heads * groups, inner), half),
        jax.ShapeDtypeStruct((classes, positions, 2 * inner), half),
        jax.ShapeDtypeStruct((classes, heads * groups, positions), jnp.float32),
        jax.ShapeDtypeStruct((classes, groups, inner), jnp.float32),
        jax.ShapeDtypeStruct((classes, groups, inner), jnp.float32),
    ]
    return pl.pallas_call(
        functools.partial(forward_kernel, heads, positions),
        grid=(classes,),
        in_specs=[
            pl.BlockSpec(memory_space=pltpu.SMEM),
            step_spec(rows.shape),
            *[whole_spec(x) for x in rest],
        ],
        out_specs=[step_spec(x.shape) for x in results],
        out_shape=results,
        scratch_shapes=[pltpu.VMEM((heads * groups, positions), jnp.float32)],
        compiler_params=pltpu.CompilerParams(dimension_semantics=("arbitrary",)),
        interpret=INTERPRET,
        name="forward_rows",
    )(own_class, rows, *rest)


def backward_call(own_class, rows, grad, params, heads, positions, share_rows, steps, wholes):
    second = not steps
    classes, groups, channels = grad.shape
    scores = pltpu.VMEM((heads * groups, positions), jnp.float32)
    scratch = [
        scores,
        pltpu.VMEM((classes * share_rows, channels), jnp.float32),
        pltpu.VMEM((positions, channels), jnp.float32),
    ]
    if second:
        rows_spec = pl.BlockSpec((classes, 1, groups, channels), lambda step: (0, step, 0, 0))
        bias_shape = (positions, heads * groups)
        sent_rows = positions + share_rows
        scratch.append(scores)
    else:
        rows_spec = step_spec(rows.shape)
        bias_shape = (groups, heads * positions)
        sent_rows = positions + groups + share_rows
    weights = kernel_weights(params)
    sent = jax.ShapeDtypeStruct((classes, sent_rows, channels), jnp.bfloat16)
    bias_out = jax.ShapeDtypeStruct(bias_shape, jnp.bfloat16)
    return pl.pallas_call(
        functools.partial(backward_kernel, heads, positions, second, share_rows),
        grid=(classes,),
        in_specs=[
            pl.BlockSpec(memory_space=pltpu.SMEM),
            rows_spec,
            step_spec(grad.shape),
            *[whole_spec(x) for x in weights],
            *[step_spec(x.shape) for x in steps],
            *[whole_spec(x) for x in wholes],
        ],
        out_specs=[whole_spec(sent), whole_spec(bias_out)],
        out_shape=[sent, bias_out],
        scratch_shapes=scratch,
        compiler_params=pltpu.CompilerParams(dimension_semantics=("arbitrary",)),
        interpret=INTERPRET,
        name="backward_second" if second else "backward_first",
    )(own_class, rows, grad, *weights, *steps, *wholes)


def finish_kernel(share_rows, heads, arrived_ref, proj_ref, gate_ref, out_ref, bias_ref, gain_ref,
                  shift_ref):
    channels = out_ref.shape[1]
    classes = arrived_ref.shape[0]
    small = jnp.sum(arrived_ref[:, 2 * share_rows :].astype(jnp.float32), axis=0)
    main = 5 * channels
    for block in range(2):
        start = block * share_rows
        whole = arrived_ref[:, start : start + share_rows].astype(jnp.float32)
        whole = whole.reshape(classes * share_rows, channels)
        proj_ref[block] = whole[: 4 * channels]
        out_ref[block] = whole[4 * channels : main]
        gate_ref[block : block + 1] = whole[main : main + 1]
        if block == 0:
            late = whole[main + 1 : main + 1 + heads + 2]
        parts = late if block else small[: heads + 2]
        bias_ref[block] = parts[:heads]
        gain_ref[block : block + 1] = parts[heads : heads + 1]
        shift_ref[block : block + 1] = parts[heads + 1 : heads + 2]


def finish_call(arrived, share_rows, heads, channels):
    shapes = [(2, 4 * channels, channels), (2, channels), (2, channels, channels)]
    shapes += [(2, heads, channels), (2, channels), (2, channels)]
    vmem = pl.BlockSpec(memory_space=pltpu.VMEM)
    return pl.pallas_call(
        functools.partial(finish_kernel, share_rows, heads),
        in_specs=[vmem],
        out_specs=[vmem] * len(shapes),
        out_shape=[jax.ShapeDtypeStruct(shape, jnp.float32) for shape in shapes],
        interpret=INTERPRET,
        name="finish_weights",
    )(arrived)


def padded_rows(x, rows):
    return jnp.pad(x, ((0, 0),) * (x.ndim - 2) + ((0, rows - x.shape[-2]), (0, 0)))


def rounded_up(value, step):
    return -(-value // step) * step


def local(
    pair_input,
    cotangent,
    residue_mask,
    norm_gain,
    norm_shift,
    proj_weights,
    gate_bias,
    out_weights,
    bias_weights,
):
    channels = pair_input.shape[2]
    groups = lax.axis_size("row")
    classes = lax.axis_size(HEAD)
    positions = groups * classes
    head_total = bias_weights.shape[2]
    bias_rows = head_total * positions // LANES
    half = jnp.bfloat16
    key_bias = (residue_mask.astype(jnp.float32) - 1.0) * MASKED
    key_bias = key_bias.reshape(groups, classes).T.reshape(1, positions)
    own_class = lax.axis_index(HEAD).astype(jnp.int32).reshape(1)
    main_rows = 5 * channels + 1
    share_rows = rounded_up(-(-(main_rows + head_total + 2) // classes), 16)
    group_rows = rounded_up(share_rows, groups) // groups
    params = [
        (
            norm_gain[which],
            norm_shift[which],
            proj_weights[which],
            gate_bias[which],
            out_weights[which],
            bias_weights[which],
        )
        for which in range(2)
    ]

    own_pair = pair_input.reshape(groups, classes, channels).transpose(1, 0, 2)
    normed_own, inverse_own, normal_own = layer_norm(own_pair, norm_gain[0], norm_shift[0])
    normal_flat = normal_own.reshape(positions, channels)
    bias_own = jnp.einsum(
        "nc,ch->hn", normal_flat, bias_weights[0], preferred_element_type=jnp.float32
    ).astype(half)
    own_cotangent = cotangent.reshape(groups, classes, channels)
    class_parts = jnp.concatenate([own_pair, own_cotangent.transpose(1, 0, 2)], axis=1)
    class_parts = rolled(class_parts, own_class[0])
    pieces = shifted_exchange(jnp.concatenate([to_all(normal_flat, HEAD), class_parts], axis=1))
    first_rows = placed(own_class, pieces)
    cotangent_query = first_rows[:, positions + groups :]
    arrived = exchanged(
        jnp.concatenate(
            [
                to_all(bias_own.reshape(bias_rows, LANES), "row"),
                own_cotangent,
            ],
            axis=1,
        ),
        "row",
    )
    first_bias = arrived[:, :bias_rows].reshape(groups, head_total * positions)
    second_grad_query = arrived[:, bias_rows:].transpose(1, 0, 2)

    after_query, after_normal, *first_saved = forward_call(
        own_class, first_rows, first_bias, key_bias, params[0], params[1], head_total, positions
    )
    after_normed, after_inverse, _ = layer_norm(after_query, norm_gain[1], norm_shift[1])
    second_bias_own = jnp.einsum(
        "abc,ch->ahb", after_normal, bias_weights[1], preferred_element_type=jnp.float32
    ).astype(half)
    after_own = exchanged(after_normal, HEAD)
    arrived = exchanged(
        jnp.concatenate(
            [
                to_all(second_bias_own.reshape(bias_rows, LANES), "row"),
                after_own.transpose(1, 0, 2),
            ],
            axis=1,
        ),
        "row",
    )
    second_bias = (
        arrived[:, :bias_rows]
        .reshape(groups, classes, head_total * groups)
        .transpose(1, 0, 2)
        .reshape(positions, head_total * groups)
    )
    second_query = arrived[:, bias_rows:].transpose(1, 0, 2)
    second_rows = exchanged(to_all(second_query, HEAD), HEAD)
    sent, bias_parts = backward_call(
        own_class,
        second_rows.reshape(classes, classes, groups, channels),
        second_grad_query,
        params[1],
        head_total,
        positions,
        share_rows,
        (),
        (second_bias, key_bias),
    )

    def group_shares_of(arrived_shares):
        summed = jnp.sum(arrived_shares.astype(jnp.float32), axis=0)
        summed = padded_rows(summed, groups * group_rows).astype(half)
        return summed.reshape(groups, group_rows, LANES)

    arrived = exchanged(sent, HEAD)
    second_shares = group_shares_of(arrived[:, positions:])
    grad_flipped = jnp.sum(arrived[:, :positions].astype(jnp.float32), axis=0).astype(half)
    bias_parts = (
        bias_parts.reshape(classes, groups, head_total * groups)
        .transpose(1, 0, 2)
        .reshape(groups, bias_rows, LANES)
    )
    arrived = exchanged(
        jnp.concatenate(
            [
                bias_parts,
                grad_flipped.reshape(classes, groups, channels).transpose(1, 0, 2),
            ],
            axis=1,
        ),
        "row",
    )
    summed = jnp.sum(arrived[:, :bias_rows].astype(jnp.float32), axis=0)
    second_bias_half = summed.reshape(classes, head_total, groups).astype(half)
    grad_query = exchanged(arrived[:, bias_rows : bias_rows + classes].transpose(1, 0, 2), HEAD)
    grad_normal = grad_query.astype(jnp.float32) + jnp.einsum(
        "ahb,ch->abc", second_bias_half, bias_weights[1], preferred_element_type=jnp.float32
    )
    end_query = norm_backward(grad_normal, after_normed, after_inverse, norm_gain[1]).astype(half)
    second_small = jnp.concatenate(
        [
            jnp.einsum(
                "abc,ahb->hc", after_normal, second_bias_half, preferred_element_type=jnp.float32
            ),
            jnp.sum(grad_normal * after_normed, axis=(0, 1))[None],
            jnp.sum(grad_normal, axis=(0, 1))[None],
        ],
        axis=0,
    )

    after_grad_query = (
        cotangent_query.astype(jnp.float32) + end_query.astype(jnp.float32)
    ).astype(half)
    extra = jnp.pad(second_small, ((1, 7 - second_small.shape[0]), (0, 0)))
    sent, bias_parts = backward_call(
        own_class,
        first_rows,
        after_grad_query,
        params[0],
        head_total,
        positions,
        share_rows,
        tuple(first_saved),
        (extra, end_query),
    )
    arrived = exchanged(sent, HEAD)
    grad_normal = jnp.sum(arrived[:, :positions].astype(jnp.float32), axis=0)
    end_own = arrived[:, positions : positions + groups]
    shares = arrived[:, positions + groups :]
    arrived = exchanged(
        jnp.concatenate(
            [
                bias_parts.reshape(groups, bias_rows, LANES),
                padded_rows(
                    jnp.concatenate([group_shares_of(shares), second_shares], axis=1),
                    rounded_up(2 * group_rows, 8),
                ),
            ],
            axis=1,
        ),
        "row",
    )
    summed = jnp.sum(arrived[:, :bias_rows].astype(jnp.float32), axis=0)
    bias_half = summed.reshape(head_total, positions).astype(half)
    shares_total = jnp.sum(
        arrived[:, bias_rows : bias_rows + 2 * group_rows].astype(jnp.float32), axis=0
    )
    grad_normal = grad_normal + jnp.einsum(
        "hn,ch->nc", bias_half, bias_weights[0], preferred_element_type=jnp.float32
    )
    normed_flat = normed_own.reshape(positions, channels)
    start_grad = norm_backward(
        grad_normal, normed_flat, inverse_own.reshape(positions, 1), norm_gain[0]
    )
    moved_grad = (end_own.astype(jnp.float32) + start_grad.reshape(end_own.shape)).transpose(1, 0, 2)
    pair_grad = cotangent.astype(jnp.float32) + moved_grad.reshape(1, positions, channels)
    first_small = jnp.concatenate(
        [
            jnp.einsum("nc,hn->hc", normal_flat, bias_half, preferred_element_type=jnp.float32),
            jnp.sum(grad_normal * normed_flat, axis=0)[None],
            jnp.sum(grad_normal, axis=0)[None],
        ],
        axis=0,
    )

    small_rows = first_small.shape[0]
    tail = jnp.concatenate([shares_total, first_small], axis=0).astype(half)
    tail = padded_rows(tail, rounded_up(tail.shape[0], 8))
    arrived = exchanged(to_all(tail, "row"), "row")
    whole_rows = groups * group_rows
    shared = jnp.concatenate(
        [
            arrived[:, :group_rows].reshape(whole_rows, LANES)[:share_rows],
            arrived[:, group_rows : 2 * group_rows].reshape(whole_rows, LANES)[:share_rows],
            padded_rows(
                jnp.sum(
                    arrived[:, 2 * group_rows : 2 * group_rows + small_rows].astype(jnp.float32),
                    axis=0,
                ).astype(half),
                rounded_up(small_rows, 8),
            ),
        ],
        axis=0,
    )
    arrived = exchanged(to_all(shared, HEAD), HEAD)
    proj_grad, gate_grad, out_grad, bias_grad, gain_grad, shift_grad = finish_call(
        arrived, share_rows, head_total, channels
    )
    return (
        pair_grad,
        proj_grad.reshape(2, 4, channels, -1),
        gate_grad,
        out_grad,
        bias_grad.transpose(0, 2, 1),
        gain_grad,
        shift_grad,
    )


def solution(mesh):
    finer = Mesh(mesh.devices.reshape(mesh.shape["row"], 4, 2), ("row", "head_0", "head_1"))
    in_specs = (P(ROW_HEAD, None, None), P(ROW_HEAD, None, None), P(), P(), P(), P(), P(), P(), P())
    out_specs = (P(ROW_HEAD, None, None), P(), P(), P(), P(), P(), P())

    return jax.shard_map(local, mesh=finer, in_specs=in_specs, out_specs=out_specs, check_vma=False)
```

```python
import functools
import math

import jax
import jax.numpy as jnp
from jax import lax
from jax.experimental import pallas as pl
from jax.experimental.pallas import tpu as pltpu
from jax.sharding import Mesh
from jax.sharding import PartitionSpec as P


HEAD = ("head_0", "head_1")
ROW_HEAD = ("row", "head_0", "head_1")


EPS = 1e-05
MASKED = 1000000000.0
LANES = 128
INTERPRET = False
ROWS = 4


def exchanged(parts, axis):
    return lax.all_to_all(parts, axis, split_axis=0, concat_axis=0, tiled=True)


def shifted_exchange(parts):
    count = len(parts)
    pieces = [parts[0]]
    for shift in range(1, count):
        pairs = [(at, (at + shift) % count) for at in range(count)]
        pieces.append(lax.ppermute(parts[shift], HEAD, pairs))
    return pieces


def place_kernel(own_ref, *refs):
    count = len(refs) - 1
    for shift in range(count):
        place = lax.rem(own_ref[0] + (count - shift), count)
        refs[-1][pl.ds(place, 1)] = refs[shift][...][None]


def placed(own_class, pieces):
    return pl.pallas_call(
        place_kernel,
        in_specs=[
            pl.BlockSpec(memory_space=pltpu.SMEM),
            *[pl.BlockSpec(memory_space=pltpu.VMEM) for _ in pieces],
        ],
        out_specs=pl.BlockSpec(memory_space=pltpu.VMEM),
        out_shape=jax.ShapeDtypeStruct((len(pieces), *pieces[0].shape), pieces[0].dtype),
        interpret=INTERPRET,
        name="place_pieces",
    )(own_class, *pieces)


def to_all(x, axis):
    return jnp.broadcast_to(x[None], (lax.axis_size(axis), *x.shape))


def layer_norm(values, norm_scale, norm_offset):
    floats = values.astype(jnp.float32)
    centred = floats - jnp.mean(floats, axis=-1, keepdims=True)
    inverse = lax.rsqrt(jnp.mean(centred * centred, axis=-1, keepdims=True) + EPS)
    normed = centred * inverse
    return (normed, inverse, (normed * norm_scale + norm_offset).astype(jnp.bfloat16))


def norm_backward(grad_normal, normed, inverse, norm_scale):
    grad_hat = grad_normal * norm_scale
    first_mean = jnp.mean(grad_hat, axis=-1, keepdims=True)
    second_mean = jnp.mean(grad_hat * normed, axis=-1, keepdims=True)
    return inverse * (grad_hat - first_mean - normed * second_mean)


def matmul(a, b, a_dim, b_dim):
    return lax.dot_general(
        a, b, (((a_dim,), (b_dim,)), ((), ())), preferred_element_type=jnp.float32
    )


def lanes_of_head(shape, head, head_size):
    lanes = lax.broadcasted_iota(jnp.int32, shape, 1)
    return (lanes >= head * head_size) & (lanes < (head + 1) * head_size)


def spread_heads(values, heads):
    size = values.shape[1] // heads
    kept = [
        jnp.where(lanes_of_head(values.shape, head, size), values, 0.0) for head in range(heads)
    ]
    return jnp.concatenate(kept, axis=0).astype(jnp.bfloat16)


def picked_heads(stacked, heads):
    rows = stacked.shape[0] // heads
    size = stacked.shape[1] // heads
    total = jnp.zeros((rows, stacked.shape[1]), jnp.float32)
    for head in range(heads):
        part = stacked[head * rows : (head + 1) * rows]
        total = jnp.where(lanes_of_head(part.shape, head, size), part, total)
    return total


def attention(x, xq, bias, wq, wkv, wg, gate_offset, heads):
    channels = wq.shape[1]
    scale = 1.0 / math.sqrt(channels // heads)
    queries = spread_heads(
        (matmul(xq, wq, 1, 0) * scale).astype(jnp.bfloat16).astype(jnp.float32), heads
    )
    pairs = matmul(x, wkv, 1, 0).astype(jnp.bfloat16)
    keys = pairs[:, :channels]
    values = pairs[:, channels:]
    gate = jax.nn.sigmoid(matmul(xq, wg, 1, 0) + gate_offset)
    logits = matmul(queries, keys, 1, 1) + bias
    weights = jnp.exp(logits - jnp.max(logits, axis=1, keepdims=True))
    probs = weights * (1.0 / jnp.sum(weights, axis=1, keepdims=True))
    probs_half = probs.astype(jnp.bfloat16)
    attended = picked_heads(matmul(probs_half, values, 1, 0), heads)
    return (queries, pairs, probs, gate, attended)


def split_bias(bias, key_bias, heads):
    count = bias.shape[1] // heads
    parts = [bias[:, head * count : (head + 1) * count] for head in range(heads)]
    return jnp.concatenate(parts, axis=0).astype(jnp.float32) + key_bias


def forward_kernel(heads, positions, class_ref, rows_ref, bias_ref, mask_ref, wq_ref, wkv_ref,
                   wg_ref, wo_ref, gate_ref, gain_ref, shift_ref, after_ref, normal_ref, queries_ref, pairs_ref, probs_ref,
                   gates_ref, attended_ref, full_bias):
    groups = after_ref.shape[1]

    @pl.when(pl.program_id(0) == 0)
    def _():
        full_bias[...] = split_bias(bias_ref[...], mask_ref[...], heads)

    for row in range(after_ref.shape[0]):
        x = rows_ref[row, :positions]
        start = pl.multiple_of(class_ref[0] * groups, groups)
        xq = rows_ref[row, pl.ds(start, groups)]
        queries, pairs, probs, gate, attended = attention(
            x, xq, full_bias[...], wq_ref[...], wkv_ref[...], wg_ref[...], gate_ref[...], heads
        )
        queries_ref[row] = queries
        pairs_ref[row] = pairs
        probs_ref[row] = probs
        gates_ref[row] = gate
        attended_ref[row] = attended
        gated = (gate * attended).astype(jnp.bfloat16)
        update = matmul(gated, wo_ref[...], 1, 0).astype(jnp.bfloat16)
        pair = rows_ref[row, positions : positions + groups]
        after = (pair.astype(jnp.float32) + update.astype(jnp.float32)).astype(jnp.bfloat16)
        after_ref[row] = after
        _, _, normal = layer_norm(after, gain_ref[...], shift_ref[...])
        normal_ref[row] = normal


def backward_kernel(heads, positions, second, share_rows, class_ref, rows_ref, grad_ref, wq_ref,
                    wkv_ref, wg_ref, wo_ref, gate_ref, *refs):
    if second:
        bias_ref, mask_ref = refs[:2]
        full_bias = refs[-1]
        sent_ref, bias_out_ref, bias_sum, weight_sum, share = refs[2:-1]
    else:
        queries_ref, pairs_ref, probs_ref, gates_ref, attended_ref, extra_ref, ride_ref = refs[:7]
        sent_ref, bias_out_ref, bias_sum, weight_sum, share = refs[7:]
    step = pl.program_id(0)
    classes = sent_ref.shape[0]
    groups = positions // classes
    channels = wq_ref.shape[0]
    inner = wq_ref.shape[1]
    own_class = class_ref[0]
    share_start = positions if second else positions + groups

    @pl.when(step == 0)
    def _():
        if second:
            full_bias[...] = bias_ref[...].astype(jnp.float32).T + mask_ref[...]
        else:
            sent_ref[:, positions : positions + groups] = ride_ref[...]
        bias_sum[...] = jnp.zeros(bias_sum.shape, jnp.float32)
        weight_sum[...] = jnp.zeros(weight_sum.shape, jnp.float32)
        if not second:
            weight_sum[5 * channels : 5 * channels + 8] = extra_ref[...]

    for row in range(grad_ref.shape[0]):
        index = step * grad_ref.shape[0] + row
        if second:
            x = rows_ref[:, row].reshape(positions, channels)
            xq = rows_ref[pl.ds(own_class, 1), row].reshape(groups, channels)
        else:
            x = rows_ref[row, :positions]
            xq = rows_ref[row, pl.ds(pl.multiple_of(own_class * groups, groups), groups)]
        if second:
            queries, pairs, probs, gate, attended = attention(
                x, xq, full_bias[...], wq_ref[...], wkv_ref[...], wg_ref[...], gate_ref[...], heads
            )
        else:
            queries, pairs, probs, gate, attended = (
                ref[row] for ref in (queries_ref, pairs_ref, probs_ref, gates_ref, attended_ref)
            )
        keys = pairs[:, :inner]
        values = pairs[:, inner:]
        probs_half = probs.astype(jnp.bfloat16)
        scale = 1.0 / math.sqrt(inner // heads)
        grad = grad_ref[row]
        gated = (gate * attended).astype(jnp.bfloat16)
        grad_gated = matmul(grad, wo_ref[...], 1, 1)
        grad_att = (grad_gated * gate).astype(jnp.bfloat16).astype(jnp.float32)
        grad_pre = (grad_gated * attended * gate * (1.0 - gate)).astype(jnp.bfloat16)
        grad_heads = spread_heads(grad_att, heads)
        grad_probs = matmul(grad_heads, values, 1, 1)
        grad_logits = probs * (grad_probs - jnp.sum(probs * grad_probs, axis=1, keepdims=True))
        bias_sum[...] += grad_logits
        logits_half = grad_logits.astype(jnp.bfloat16)
        grad_queries = (picked_heads(matmul(logits_half, keys, 1, 0), heads) * scale).astype(
            jnp.bfloat16
        )
        grad_keys = matmul(logits_half, queries, 0, 0).astype(jnp.bfloat16)
        grad_values = matmul(probs_half, grad_heads, 0, 0).astype(jnp.bfloat16)
        grad_pairs = jnp.concatenate([grad_keys, grad_values], axis=1)
        share[row] = matmul(grad_pairs, wkv_ref[...], 1, 1)
        query_side = matmul(grad_queries, wq_ref[...], 1, 1) + matmul(grad_pre, wg_ref[...], 1, 1)
        own_rows = pl.ds(pl.multiple_of(own_class * groups, groups), groups)
        share[row, own_rows] = share[row, own_rows] + query_side
        partial = share[row].astype(jnp.bfloat16)
        if second:
            place = pl.ds(pl.multiple_of(index * groups, groups), groups)
            sent_ref[:, place] = partial.reshape(classes, groups, channels)
        else:
            sent_ref[pl.ds(index, 1), :positions] = partial[None]
        pair_sums = matmul(x, grad_pairs, 0, 0)
        weight_sum[:channels] += matmul(xq, grad_queries, 0, 0)
        weight_sum[channels : 2 * channels] += pair_sums[:, :inner]
        weight_sum[2 * channels : 3 * channels] += pair_sums[:, inner:]
        weight_sum[3 * channels : 4 * channels] += matmul(xq, grad_pre, 0, 0)
        weight_sum[4 * channels : 5 * channels] += matmul(gated, grad, 0, 0)
        weight_sum[5 * channels : 5 * channels + 1] += jnp.sum(
            grad_pre.astype(jnp.float32), axis=0, keepdims=True
        )

    @pl.when(step == pl.num_programs(0) - 1)
    def _():
        for peer in range(classes):
            sent_ref[peer, share_start : share_start + share_rows] = weight_sum[
                peer * share_rows : (peer + 1) * share_rows
            ].astype(jnp.bfloat16)
        if second:
            bias_out_ref[...] = bias_sum[...].T.astype(jnp.bfloat16)
        else:
            for head in range(heads):
                bias_out_ref[:, head * positions : (head + 1) * positions] = bias_sum[
                    head * groups : (head + 1) * groups
                ].astype(jnp.bfloat16)


def whole_spec(x):
    return pl.BlockSpec(x.shape, lambda step, n=x.ndim: (0,) * n)


def kernel_weights(params):
    _, _, projection, gate_offset, out_proj, _ = params
    joined = jnp.concatenate([projection[1], projection[2]], axis=1)
    return (projection[0], joined, projection[3], out_proj, gate_offset[None])


def start_kernel(heads, own_ref, pair_ref, class_cot_ref, cot_ref, gain_ref, shift_ref, wb_ref,
                 row_ref, normed_ref, inverse_ref, *piece_refs):
    classes, groups, channels = pair_ref.shape
    positions = classes * groups
    pair = pair_ref[...].reshape(positions, channels)
    normed, inverse, normal = layer_norm(pair, gain_ref[...], shift_ref[...])
    normed_ref[...] = normed
    inverse_ref[...] = inverse
    bias = matmul(wb_ref[...], normal, 0, 1)
    tiles = positions // min(positions, LANES)
    width = positions // tiles
    lines = [
        bias[head : head + 1, tile * width : (tile + 1) * width]
        for head in range(heads)
        for tile in range(tiles)
    ]
    if width < LANES:
        lines = [jnp.concatenate(lines, axis=1)]
    packed = jnp.concatenate(lines, axis=0).astype(jnp.bfloat16)
    rows = packed.shape[0]
    row_ref[:, :rows] = jnp.broadcast_to(packed[None], (groups, *packed.shape))
    row_ref[:, rows:] = cot_ref[...]
    for shift, piece_ref in enumerate(piece_refs):
        peer = lax.rem(own_ref[0] + shift, classes)
        piece_ref[:positions] = normal
        piece_ref[positions : positions + groups] = pair_ref[pl.ds(peer, 1)][0]
        piece_ref[positions + groups :] = class_cot_ref[pl.ds(peer, 1)][0]


def start_call(own_class, pair, class_cot, cot, params, heads):
    classes, groups, channels = pair.shape
    positions = classes * groups
    rows = heads * positions // LANES + classes
    half = jnp.bfloat16
    vmem = pl.BlockSpec(memory_space=pltpu.VMEM)
    results = [
        jax.ShapeDtypeStruct((groups, rows, channels), half),
        jax.ShapeDtypeStruct((positions, channels), jnp.float32),
        jax.ShapeDtypeStruct((positions, 1), jnp.float32),
    ]
    results += [jax.ShapeDtypeStruct((positions + 2 * groups, channels), half)] * classes
    return pl.pallas_call(
        functools.partial(start_kernel, heads),
        in_specs=[pl.BlockSpec(memory_space=pltpu.SMEM)] + [vmem] * 6,
        out_specs=[vmem] * len(results),
        out_shape=results,
        interpret=INTERPRET,
        name="start_row",
    )(own_class, pair, class_cot, cot, params[0][None], params[1][None], params[5])


def step_spec(shape):
    return pl.BlockSpec((ROWS, *shape[1:]), lambda step, n=len(shape): (step,) + (0,) * (n - 1))


def forward_call(own_class, rows, bias, key_bias, params, next_params, heads, positions):
    classes, _, channels = rows.shape
    groups = positions // classes
    inner = params[2].shape[2]
    half = jnp.bfloat16
    rest = (
        bias,
        key_bias,
        *kernel_weights(params),
        next_params[0][None],
        next_params[1][None],
    )
    results = [
        jax.ShapeDtypeStruct((classes, groups, channels), half),
        jax.ShapeDtypeStruct((classes, groups, channels), half),
        jax.ShapeDtypeStruct((classes, heads * groups, inner), half),
        jax.ShapeDtypeStruct((classes, positions, 2 * inner), half),
        jax.ShapeDtypeStruct((classes, heads * groups, positions), jnp.float32),
        jax.ShapeDtypeStruct((classes, groups, inner), jnp.float32),
        jax.ShapeDtypeStruct((classes, groups, inner), jnp.float32),
    ]
    return pl.pallas_call(
        functools.partial(forward_kernel, heads, positions),
        grid=(classes // ROWS,),
        in_specs=[
            pl.BlockSpec(memory_space=pltpu.SMEM),
            step_spec(rows.shape),
            *[whole_spec(x) for x in rest],
        ],
        out_specs=[step_spec(x.shape) for x in results],
        out_shape=results,
        scratch_shapes=[pltpu.VMEM((heads * groups, positions), jnp.float32)],
        compiler_params=pltpu.CompilerParams(dimension_semantics=("arbitrary",)),
        interpret=INTERPRET,
        name="forward_rows",
    )(own_class, rows, *rest)


def backward_call(own_class, rows, grad, params, heads, positions, share_rows, steps, wholes):
    second = not steps
    classes, groups, channels = grad.shape
    scores = pltpu.VMEM((heads * groups, positions), jnp.float32)
    scratch = [
        scores,
        pltpu.VMEM((classes * share_rows, channels), jnp.float32),
        pltpu.VMEM((ROWS, positions, channels), jnp.float32),
    ]
    if second:
        rows_spec = pl.BlockSpec((classes, ROWS, groups, channels), lambda step: (0, step, 0, 0))
        bias_shape = (positions, heads * groups)
        sent_rows = positions + share_rows
        scratch.append(scores)
    else:
        rows_spec = step_spec(rows.shape)
        bias_shape = (groups, heads * positions)
        sent_rows = positions + groups + share_rows
    weights = kernel_weights(params)
    sent = jax.ShapeDtypeStruct((classes, sent_rows, channels), jnp.bfloat16)
    bias_out = jax.ShapeDtypeStruct(bias_shape, jnp.bfloat16)
    return pl.pallas_call(
        functools.partial(backward_kernel, heads, positions, second, share_rows),
        grid=(classes // ROWS,),
        in_specs=[
            pl.BlockSpec(memory_space=pltpu.SMEM),
            rows_spec,
            step_spec(grad.shape),
            *[whole_spec(x) for x in weights],
            *[step_spec(x.shape) for x in steps],
            *[whole_spec(x) for x in wholes],
        ],
        out_specs=[whole_spec(sent), whole_spec(bias_out)],
        out_shape=[sent, bias_out],
        scratch_shapes=scratch,
        compiler_params=pltpu.CompilerParams(dimension_semantics=("arbitrary",)),
        interpret=INTERPRET,
        name="backward_second" if second else "backward_first",
    )(own_class, rows, grad, *weights, *steps, *wholes)


def finish_kernel(share_rows, heads, arrived_ref, proj_ref, gate_ref, out_ref, bias_ref, gain_ref,
                  shift_ref):
    channels = out_ref.shape[1]
    classes = arrived_ref.shape[0]
    small = jnp.sum(arrived_ref[:, 2 * share_rows :].astype(jnp.float32), axis=0)
    main = 5 * channels
    for block in range(2):
        start = block * share_rows
        whole = arrived_ref[:, start : start + share_rows].astype(jnp.float32)
        whole = whole.reshape(classes * share_rows, channels)
        proj_ref[block] = whole[: 4 * channels]
        out_ref[block] = whole[4 * channels : main]
        gate_ref[block : block + 1] = whole[main : main + 1]
        if block == 0:
            late = whole[main + 1 : main + 1 + heads + 2]
        parts = late if block else small[: heads + 2]
        bias_ref[block] = parts[:heads]
        gain_ref[block : block + 1] = parts[heads : heads + 1]
        shift_ref[block : block + 1] = parts[heads + 1 : heads + 2]


def finish_call(arrived, share_rows, heads, channels):
    shapes = [(2, 4 * channels, channels), (2, channels), (2, channels, channels)]
    shapes += [(2, heads, channels), (2, channels), (2, channels)]
    vmem = pl.BlockSpec(memory_space=pltpu.VMEM)
    return pl.pallas_call(
        functools.partial(finish_kernel, share_rows, heads),
        in_specs=[vmem],
        out_specs=[vmem] * len(shapes),
        out_shape=[jax.ShapeDtypeStruct(shape, jnp.float32) for shape in shapes],
        interpret=INTERPRET,
        name="finish_weights",
    )(arrived)


def padded_rows(x, rows):
    return jnp.pad(x, ((0, 0),) * (x.ndim - 2) + ((0, rows - x.shape[-2]), (0, 0)))


def rounded_up(value, step):
    return -(-value // step) * step


def local(
    pair_input,
    cotangent,
    residue_mask,
    norm_gain,
    norm_shift,
    proj_weights,
    gate_bias,
    out_weights,
    bias_weights,
):
    channels = pair_input.shape[2]
    groups = lax.axis_size("row")
    classes = lax.axis_size(HEAD)
    positions = groups * classes
    head_total = bias_weights.shape[2]
    bias_rows = head_total * positions // LANES
    half = jnp.bfloat16
    key_bias = (residue_mask.astype(jnp.float32) - 1.0) * MASKED
    key_bias = key_bias.reshape(groups, classes).T.reshape(1, positions)
    own_class = lax.axis_index(HEAD).astype(jnp.int32).reshape(1)
    main_rows = 5 * channels + 1
    share_rows = rounded_up(-(-(main_rows + head_total + 2) // classes), 16)
    group_rows = rounded_up(share_rows, groups) // groups
    params = [
        (
            norm_gain[which],
            norm_shift[which],
            proj_weights[which],
            gate_bias[which],
            out_weights[which],
            bias_weights[which],
        )
        for which in range(2)
    ]

    own_pair = pair_input.reshape(groups, classes, channels).transpose(1, 0, 2)
    own_cotangent = cotangent.reshape(groups, classes, channels)
    row_parts, normed_flat, inverse_flat, *parts = start_call(
        own_class,
        own_pair,
        own_cotangent.transpose(1, 0, 2),
        own_cotangent,
        params[0],
        head_total,
    )
    normal_flat = parts[0][:positions]
    pieces = shifted_exchange(parts)
    first_rows = placed(own_class, pieces)
    cotangent_query = first_rows[:, positions + groups :]
    arrived = exchanged(row_parts, "row")
    first_bias = arrived[:, :bias_rows].reshape(groups, head_total * positions)
    second_grad_query = arrived[:, bias_rows:].transpose(1, 0, 2)

    after_query, after_normal, *first_saved = forward_call(
        own_class, first_rows, first_bias, key_bias, params[0], params[1], head_total, positions
    )
    after_normed, after_inverse, _ = layer_norm(after_query, norm_gain[1], norm_shift[1])
    second_bias_own = jnp.einsum(
        "abc,ch->ahb", after_normal, bias_weights[1], preferred_element_type=jnp.float32
    ).astype(half)
    after_own = exchanged(after_normal, HEAD)
    arrived = exchanged(
        jnp.concatenate(
            [
                to_all(second_bias_own.reshape(bias_rows, LANES), "row"),
                after_own.transpose(1, 0, 2),
            ],
            axis=1,
        ),
        "row",
    )
    second_bias = (
        arrived[:, :bias_rows]
        .reshape(groups, classes, head_total * groups)
        .transpose(1, 0, 2)
        .reshape(positions, head_total * groups)
    )
    second_query = arrived[:, bias_rows:].transpose(1, 0, 2)
    second_rows = exchanged(to_all(second_query, HEAD), HEAD)
    sent, bias_parts = backward_call(
        own_class,
        second_rows.reshape(classes, classes, groups, channels),
        second_grad_query,
        params[1],
        head_total,
        positions,
        share_rows,
        (),
        (second_bias, key_bias),
    )

    def group_shares_of(arrived_shares):
        summed = jnp.sum(arrived_shares.astype(jnp.float32), axis=0)
        summed = padded_rows(summed, groups * group_rows).astype(half)
        return summed.reshape(groups, group_rows, LANES)

    arrived = exchanged(sent, HEAD)
    second_shares = group_shares_of(arrived[:, positions:])
    grad_flipped = jnp.sum(arrived[:, :positions].astype(jnp.float32), axis=0).astype(half)
    bias_parts = (
        bias_parts.reshape(classes, groups, head_total * groups)
        .transpose(1, 0, 2)
        .reshape(groups, bias_rows, LANES)
    )
    arrived = exchanged(
        jnp.concatenate(
            [
                bias_parts,
                grad_flipped.reshape(classes, groups, channels).transpose(1, 0, 2),
            ],
            axis=1,
        ),
        "row",
    )
    summed = jnp.sum(arrived[:, :bias_rows].astype(jnp.float32), axis=0)
    second_bias_half = summed.reshape(classes, head_total, groups).astype(half)
    grad_query = exchanged(arrived[:, bias_rows : bias_rows + classes].transpose(1, 0, 2), HEAD)
    grad_normal = grad_query.astype(jnp.float32) + jnp.einsum(
        "ahb,ch->abc", second_bias_half, bias_weights[1], preferred_element_type=jnp.float32
    )
    end_query = norm_backward(grad_normal, after_normed, after_inverse, norm_gain[1]).astype(half)
    second_small = jnp.concatenate(
        [
            jnp.einsum(
                "abc,ahb->hc", after_normal, second_bias_half, preferred_element_type=jnp.float32
            ),
            jnp.sum(grad_normal * after_normed, axis=(0, 1))[None],
            jnp.sum(grad_normal, axis=(0, 1))[None],
        ],
        axis=0,
    )

    after_grad_query = (
        cotangent_query.astype(jnp.float32) + end_query.astype(jnp.float32)
    ).astype(half)
    extra = jnp.pad(second_small, ((1, 7 - second_small.shape[0]), (0, 0)))
    sent, bias_parts = backward_call(
        own_class,
        first_rows,
        after_grad_query,
        params[0],
        head_total,
        positions,
        share_rows,
        tuple(first_saved),
        (extra, end_query),
    )
    arrived = exchanged(sent, HEAD)
    grad_normal = jnp.sum(arrived[:, :positions].astype(jnp.float32), axis=0)
    end_own = arrived[:, positions : positions + groups]
    shares = arrived[:, positions + groups :]
    arrived = exchanged(
        jnp.concatenate(
            [
                bias_parts.reshape(groups, bias_rows, LANES),
                padded_rows(
                    jnp.concatenate([group_shares_of(shares), second_shares], axis=1),
                    rounded_up(2 * group_rows, 8),
                ),
            ],
            axis=1,
        ),
        "row",
    )
    summed = jnp.sum(arrived[:, :bias_rows].astype(jnp.float32), axis=0)
    bias_half = summed.reshape(head_total, positions).astype(half)
    shares_total = jnp.sum(
        arrived[:, bias_rows : bias_rows + 2 * group_rows].astype(jnp.float32), axis=0
    )
    grad_normal = grad_normal + jnp.einsum(
        "hn,ch->nc", bias_half, bias_weights[0], preferred_element_type=jnp.float32
    )
    start_grad = norm_backward(
        grad_normal, normed_flat, inverse_flat, norm_gain[0]
    )
    moved_grad = (end_own.astype(jnp.float32) + start_grad.reshape(end_own.shape)).transpose(1, 0, 2)
    pair_grad = cotangent.astype(jnp.float32) + moved_grad.reshape(1, positions, channels)
    first_small = jnp.concatenate(
        [
            jnp.einsum("nc,hn->hc", normal_flat, bias_half, preferred_element_type=jnp.float32),
            jnp.sum(grad_normal * normed_flat, axis=0)[None],
            jnp.sum(grad_normal, axis=0)[None],
        ],
        axis=0,
    )

    small_rows = first_small.shape[0]
    tail = jnp.concatenate([shares_total, first_small], axis=0).astype(half)
    tail = padded_rows(tail, rounded_up(tail.shape[0], 8))
    arrived = exchanged(to_all(tail, "row"), "row")
    whole_rows = groups * group_rows
    shared = jnp.concatenate(
        [
            arrived[:, :group_rows].reshape(whole_rows, LANES)[:share_rows],
            arrived[:, group_rows : 2 * group_rows].reshape(whole_rows, LANES)[:share_rows],
            padded_rows(
                jnp.sum(
                    arrived[:, 2 * group_rows : 2 * group_rows + small_rows].astype(jnp.float32),
                    axis=0,
                ).astype(half),
                rounded_up(small_rows, 8),
            ),
        ],
        axis=0,
    )
    arrived = exchanged(to_all(shared, HEAD), HEAD)
    proj_grad, gate_grad, out_grad, bias_grad, gain_grad, shift_grad = finish_call(
        arrived, share_rows, head_total, channels
    )
    return (
        pair_grad,
        proj_grad.reshape(2, 4, channels, -1),
        gate_grad,
        out_grad,
        bias_grad.transpose(0, 2, 1),
        gain_grad,
        shift_grad,
    )


def solution(mesh):
    finer = Mesh(mesh.devices.reshape(mesh.shape["row"], 4, 2), ("row", "head_0", "head_1"))
    in_specs = (P(ROW_HEAD, None, None), P(ROW_HEAD, None, None), P(), P(), P(), P(), P(), P(), P())
    out_specs = (P(ROW_HEAD, None, None), P(), P(), P(), P(), P(), P())

    return jax.shard_map(local, mesh=finer, in_specs=in_specs, out_specs=out_specs, check_vma=False)
```

```python
import functools
import math

import jax
import jax.numpy as jnp
from jax import lax
from jax.experimental import pallas as pl
from jax.experimental.pallas import tpu as pltpu
from jax.sharding import Mesh
from jax.sharding import PartitionSpec as P


HEAD = ("head_0", "head_1")
ROW_HEAD = ("row", "head_0", "head_1")


EPS = 1e-05
MASKED = 1000000000.0
LANES = 128
INTERPRET = False
ROWS = 4


def exchanged(parts, axis):
    return lax.all_to_all(parts, axis, split_axis=0, concat_axis=0, tiled=True)


def shifted_exchange(parts):
    count = len(parts)
    pieces = [parts[0]]
    for shift in range(1, count):
        pairs = [(at, (at + shift) % count) for at in range(count)]
        pieces.append(lax.ppermute(parts[shift], HEAD, pairs))
    return pieces


def place_kernel(own_ref, *refs):
    count = len(refs) - 1
    for shift in range(count):
        place = lax.rem(own_ref[0] + (count - shift), count)
        refs[-1][pl.ds(place, 1)] = refs[shift][...][None]


def placed(own_class, pieces):
    return pl.pallas_call(
        place_kernel,
        in_specs=[
            pl.BlockSpec(memory_space=pltpu.SMEM),
            *[pl.BlockSpec(memory_space=pltpu.VMEM) for _ in pieces],
        ],
        out_specs=pl.BlockSpec(memory_space=pltpu.VMEM),
        out_shape=jax.ShapeDtypeStruct((len(pieces), *pieces[0].shape), pieces[0].dtype),
        interpret=INTERPRET,
        name="place_pieces",
    )(own_class, *pieces)


def to_all(x, axis):
    return jnp.broadcast_to(x[None], (lax.axis_size(axis), *x.shape))


def layer_norm(values, norm_scale, norm_offset):
    floats = values.astype(jnp.float32)
    centred = floats - jnp.mean(floats, axis=-1, keepdims=True)
    inverse = lax.rsqrt(jnp.mean(centred * centred, axis=-1, keepdims=True) + EPS)
    normed = centred * inverse
    return (normed, inverse, (normed * norm_scale + norm_offset).astype(jnp.bfloat16))


def norm_backward(grad_normal, normed, inverse, norm_scale):
    grad_hat = grad_normal * norm_scale
    first_mean = jnp.mean(grad_hat, axis=-1, keepdims=True)
    second_mean = jnp.mean(grad_hat * normed, axis=-1, keepdims=True)
    return inverse * (grad_hat - first_mean - normed * second_mean)


def matmul(a, b, a_dim, b_dim):
    return lax.dot_general(
        a, b, (((a_dim,), (b_dim,)), ((), ())), preferred_element_type=jnp.float32
    )


def lanes_of_head(shape, head, head_size):
    lanes = lax.broadcasted_iota(jnp.int32, shape, 1)
    return (lanes >= head * head_size) & (lanes < (head + 1) * head_size)


def spread_heads(values, heads):
    size = values.shape[1] // heads
    kept = [
        jnp.where(lanes_of_head(values.shape, head, size), values, 0.0) for head in range(heads)
    ]
    return jnp.concatenate(kept, axis=0).astype(jnp.bfloat16)


def picked_heads(stacked, heads):
    rows = stacked.shape[0] // heads
    size = stacked.shape[1] // heads
    total = jnp.zeros((rows, stacked.shape[1]), jnp.float32)
    for head in range(heads):
        part = stacked[head * rows : (head + 1) * rows]
        total = jnp.where(lanes_of_head(part.shape, head, size), part, total)
    return total


def attention(x, xq, bias, wq, wkv, wg, gate_offset, heads):
    channels = wq.shape[1]
    scale = 1.0 / math.sqrt(channels // heads)
    queries = spread_heads(
        (matmul(xq, wq, 1, 0) * scale).astype(jnp.bfloat16).astype(jnp.float32), heads
    )
    pairs = matmul(x, wkv, 1, 0).astype(jnp.bfloat16)
    keys = pairs[:, :channels]
    values = pairs[:, channels:]
    gate = jax.nn.sigmoid(matmul(xq, wg, 1, 0) + gate_offset)
    logits = matmul(queries, keys, 1, 1) + bias
    weights = jnp.exp(logits - jnp.max(logits, axis=1, keepdims=True))
    probs = weights * (1.0 / jnp.sum(weights, axis=1, keepdims=True))
    probs_half = probs.astype(jnp.bfloat16)
    attended = picked_heads(matmul(probs_half, values, 1, 0), heads)
    return (queries, pairs, probs, gate, attended)


def split_bias(bias, key_bias, heads):
    count = bias.shape[1] // heads
    parts = [bias[:, head * count : (head + 1) * count] for head in range(heads)]
    return jnp.concatenate(parts, axis=0).astype(jnp.float32) + key_bias


def forward_kernel(heads, positions, class_ref, rows_ref, bias_ref, mask_ref, wq_ref, wkv_ref,
                   wg_ref, wo_ref, gate_ref, gain_ref, shift_ref, after_ref, normal_ref, queries_ref, pairs_ref, probs_ref,
                   gates_ref, attended_ref, full_bias):
    groups = after_ref.shape[1]

    @pl.when(pl.program_id(0) == 0)
    def _():
        full_bias[...] = split_bias(bias_ref[...], mask_ref[...], heads)

    for row in range(after_ref.shape[0]):
        x = rows_ref[row, :positions]
        start = pl.multiple_of(class_ref[0] * groups, groups)
        xq = rows_ref[row, pl.ds(start, groups)]
        queries, pairs, probs, gate, attended = attention(
            x, xq, full_bias[...], wq_ref[...], wkv_ref[...], wg_ref[...], gate_ref[...], heads
        )
        queries_ref[row] = queries
        pairs_ref[row] = pairs
        probs_ref[row] = probs
        gates_ref[row] = gate
        attended_ref[row] = attended
        gated = (gate * attended).astype(jnp.bfloat16)
        update = matmul(gated, wo_ref[...], 1, 0).astype(jnp.bfloat16)
        pair = rows_ref[row, positions : positions + groups]
        after = (pair.astype(jnp.float32) + update.astype(jnp.float32)).astype(jnp.bfloat16)
        after_ref[row] = after
        _, _, normal = layer_norm(after, gain_ref[...], shift_ref[...])
        normal_ref[row] = normal


def backward_kernel(heads, positions, second, share_rows, class_ref, rows_ref, grad_ref, wq_ref,
                    wkv_ref, wg_ref, wo_ref, gate_ref, *refs):
    if second:
        bias_ref, mask_ref = refs[:2]
        full_bias = refs[-1]
        sent_ref, bias_out_ref, bias_sum, weight_sum, share = refs[2:-1]
    else:
        queries_ref, pairs_ref, probs_ref, gates_ref, attended_ref, extra_ref, ride_ref = refs[:7]
        sent_ref, bias_out_ref, bias_sum, weight_sum, share = refs[7:]
    step = pl.program_id(0)
    classes = sent_ref.shape[0]
    groups = positions // classes
    channels = wq_ref.shape[0]
    inner = wq_ref.shape[1]
    own_class = class_ref[0]
    share_start = positions if second else positions + groups

    @pl.when(step == 0)
    def _():
        if second:
            full_bias[...] = bias_ref[...].astype(jnp.float32).T + mask_ref[...]
        else:
            sent_ref[:, positions : positions + groups] = ride_ref[...]
        bias_sum[...] = jnp.zeros(bias_sum.shape, jnp.float32)
        weight_sum[...] = jnp.zeros(weight_sum.shape, jnp.float32)
        if not second:
            weight_sum[5 * channels : 5 * channels + 8] = extra_ref[...]

    for row in range(grad_ref.shape[0]):
        index = step * grad_ref.shape[0] + row
        if second:
            x = rows_ref[:, row].reshape(positions, channels)
            xq = rows_ref[pl.ds(own_class, 1), row].reshape(groups, channels)
        else:
            x = rows_ref[row, :positions]
            xq = rows_ref[row, pl.ds(pl.multiple_of(own_class * groups, groups), groups)]
        if second:
            queries, pairs, probs, gate, attended = attention(
                x, xq, full_bias[...], wq_ref[...], wkv_ref[...], wg_ref[...], gate_ref[...], heads
            )
        else:
            queries, pairs, probs, gate, attended = (
                ref[row] for ref in (queries_ref, pairs_ref, probs_ref, gates_ref, attended_ref)
            )
        keys = pairs[:, :inner]
        values = pairs[:, inner:]
        probs_half = probs.astype(jnp.bfloat16)
        scale = 1.0 / math.sqrt(inner // heads)
        grad = grad_ref[row]
        gated = (gate * attended).astype(jnp.bfloat16)
        grad_gated = matmul(grad, wo_ref[...], 1, 1)
        grad_att = (grad_gated * gate).astype(jnp.bfloat16).astype(jnp.float32)
        grad_pre = (grad_gated * attended * gate * (1.0 - gate)).astype(jnp.bfloat16)
        grad_heads = spread_heads(grad_att, heads)
        grad_probs = matmul(grad_heads, values, 1, 1)
        grad_logits = probs * (grad_probs - jnp.sum(probs * grad_probs, axis=1, keepdims=True))
        bias_sum[...] += grad_logits
        logits_half = grad_logits.astype(jnp.bfloat16)
        grad_queries = (picked_heads(matmul(logits_half, keys, 1, 0), heads) * scale).astype(
            jnp.bfloat16
        )
        grad_keys = matmul(logits_half, queries, 0, 0).astype(jnp.bfloat16)
        grad_values = matmul(probs_half, grad_heads, 0, 0).astype(jnp.bfloat16)
        grad_pairs = jnp.concatenate([grad_keys, grad_values], axis=1)
        share[row] = matmul(grad_pairs, wkv_ref[...], 1, 1)
        query_side = matmul(grad_queries, wq_ref[...], 1, 1) + matmul(grad_pre, wg_ref[...], 1, 1)
        own_rows = pl.ds(pl.multiple_of(own_class * groups, groups), groups)
        share[row, own_rows] = share[row, own_rows] + query_side
        partial = share[row].astype(jnp.bfloat16)
        if second:
            place = pl.ds(pl.multiple_of(index * groups, groups), groups)
            sent_ref[:, place] = partial.reshape(classes, groups, channels)
        else:
            sent_ref[pl.ds(index, 1), :positions] = partial[None]
        pair_sums = matmul(x, grad_pairs, 0, 0)
        weight_sum[:channels] += matmul(xq, grad_queries, 0, 0)
        weight_sum[channels : 2 * channels] += pair_sums[:, :inner]
        weight_sum[2 * channels : 3 * channels] += pair_sums[:, inner:]
        weight_sum[3 * channels : 4 * channels] += matmul(xq, grad_pre, 0, 0)
        weight_sum[4 * channels : 5 * channels] += matmul(gated, grad, 0, 0)
        weight_sum[5 * channels : 5 * channels + 1] += jnp.sum(
            grad_pre.astype(jnp.float32), axis=0, keepdims=True
        )

    @pl.when(step == pl.num_programs(0) - 1)
    def _():
        for peer in range(classes):
            sent_ref[peer, share_start : share_start + share_rows] = weight_sum[
                peer * share_rows : (peer + 1) * share_rows
            ].astype(jnp.bfloat16)
        if second:
            bias_out_ref[...] = bias_sum[...].T.astype(jnp.bfloat16)
        else:
            for head in range(heads):
                bias_out_ref[:, head * positions : (head + 1) * positions] = bias_sum[
                    head * groups : (head + 1) * groups
                ].astype(jnp.bfloat16)


def whole_spec(x):
    return pl.BlockSpec(x.shape, lambda step, n=x.ndim: (0,) * n)


def kernel_weights(params):
    _, _, projection, gate_offset, out_proj, _ = params
    joined = jnp.concatenate([projection[1], projection[2]], axis=1)
    return (projection[0], joined, projection[3], out_proj, gate_offset[None])


def start_kernel(heads, own_ref, pair_ref, cot_ref, gain_ref, shift_ref, wb_ref,
                 row_ref, normed_ref, inverse_ref, *refs):
    piece_refs, plain, ordered = refs[:-2], refs[-2], refs[-1]
    classes = len(piece_refs)
    positions, channels = pair_ref.shape
    groups = positions // classes
    for which, ref in enumerate((pair_ref, cot_ref)):
        first = which * positions
        plain[first : first + positions] = ref[...].astype(jnp.float32)
        for peer in range(classes):
            place = first + peer * groups
            ordered[place : place + groups] = plain[pl.ds(first + peer, groups, stride=classes)]
    pair = ordered[:positions]
    normed, inverse, normal = layer_norm(pair, gain_ref[...], shift_ref[...])
    normed_ref[...] = normed
    inverse_ref[...] = inverse
    bias = matmul(wb_ref[...], normal, 0, 1)
    tiles = positions // min(positions, LANES)
    width = positions // tiles
    lines = [
        bias[head : head + 1, tile * width : (tile + 1) * width]
        for head in range(heads)
        for tile in range(tiles)
    ]
    if width < LANES:
        lines = [jnp.concatenate(lines, axis=1)]
    packed = jnp.concatenate(lines, axis=0).astype(jnp.bfloat16)
    rows = packed.shape[0]
    row_ref[:, :rows] = jnp.broadcast_to(packed[None], (groups, *packed.shape))
    row_ref[:, rows:] = plain[positions:].reshape(groups, classes, channels).astype(jnp.bfloat16)
    for shift, piece_ref in enumerate(piece_refs):
        peer = lax.rem(own_ref[0] + shift, classes)
        piece_ref[:positions] = normal
        place = pl.ds(pl.multiple_of(peer * groups, groups), groups)
        piece_ref[positions : positions + groups] = ordered[place].astype(jnp.bfloat16)
        place = pl.ds(pl.multiple_of(positions + peer * groups, groups), groups)
        piece_ref[positions + groups :] = ordered[place].astype(jnp.bfloat16)


def start_call(own_class, pair, cot, params, heads, classes):
    positions, channels = pair.shape
    groups = positions // classes
    rows = heads * positions // LANES + classes
    half = jnp.bfloat16
    vmem = pl.BlockSpec(memory_space=pltpu.VMEM)
    results = [
        jax.ShapeDtypeStruct((groups, rows, channels), half),
        jax.ShapeDtypeStruct((positions, channels), jnp.float32),
        jax.ShapeDtypeStruct((positions, 1), jnp.float32),
    ]
    results += [jax.ShapeDtypeStruct((positions + 2 * groups, channels), half)] * classes
    return pl.pallas_call(
        functools.partial(start_kernel, heads),
        in_specs=[pl.BlockSpec(memory_space=pltpu.SMEM)] + [vmem] * 5,
        out_specs=[vmem] * len(results),
        out_shape=results,
        scratch_shapes=[pltpu.VMEM((2 * positions, channels), jnp.float32)] * 2,
        interpret=INTERPRET,
        name="start_row",
    )(own_class, pair, cot, params[0][None], params[1][None], params[5])


def step_spec(shape):
    return pl.BlockSpec((ROWS, *shape[1:]), lambda step, n=len(shape): (step,) + (0,) * (n - 1))


def forward_call(own_class, rows, bias, key_bias, params, next_params, heads, positions):
    classes, _, channels = rows.shape
    groups = positions // classes
    inner = params[2].shape[2]
    half = jnp.bfloat16
    rest = (
        bias,
        key_bias,
        *kernel_weights(params),
        next_params[0][None],
        next_params[1][None],
    )
    results = [
        jax.ShapeDtypeStruct((classes, groups, channels), half),
        jax.ShapeDtypeStruct((classes, groups, channels), half),
        jax.ShapeDtypeStruct((classes, heads * groups, inner), half),
        jax.ShapeDtypeStruct((classes, positions, 2 * inner), half),
        jax.ShapeDtypeStruct((classes, heads * groups, positions), jnp.float32),
        jax.ShapeDtypeStruct((classes, groups, inner), jnp.float32),
        jax.ShapeDtypeStruct((classes, groups, inner), jnp.float32),
    ]
    return pl.pallas_call(
        functools.partial(forward_kernel, heads, positions),
        grid=(classes // ROWS,),
        in_specs=[
            pl.BlockSpec(memory_space=pltpu.SMEM),
            step_spec(rows.shape),
            *[whole_spec(x) for x in rest],
        ],
        out_specs=[step_spec(x.shape) for x in results],
        out_shape=results,
        scratch_shapes=[pltpu.VMEM((heads * groups, positions), jnp.float32)],
        compiler_params=pltpu.CompilerParams(dimension_semantics=("arbitrary",)),
        interpret=INTERPRET,
        name="forward_rows",
    )(own_class, rows, *rest)


def backward_call(own_class, rows, grad, params, heads, positions, share_rows, steps, wholes):
    second = not steps
    classes, groups, channels = grad.shape
    scores = pltpu.VMEM((heads * groups, positions), jnp.float32)
    scratch = [
        scores,
        pltpu.VMEM((classes * share_rows, channels), jnp.float32),
        pltpu.VMEM((ROWS, positions, channels), jnp.float32),
    ]
    if second:
        rows_spec = pl.BlockSpec((classes, ROWS, groups, channels), lambda step: (0, step, 0, 0))
        bias_shape = (positions, heads * groups)
        sent_rows = positions + share_rows
        scratch.append(scores)
    else:
        rows_spec = step_spec(rows.shape)
        bias_shape = (groups, heads * positions)
        sent_rows = positions + groups + share_rows
    weights = kernel_weights(params)
    sent = jax.ShapeDtypeStruct((classes, sent_rows, channels), jnp.bfloat16)
    bias_out = jax.ShapeDtypeStruct(bias_shape, jnp.bfloat16)
    return pl.pallas_call(
        functools.partial(backward_kernel, heads, positions, second, share_rows),
        grid=(classes // ROWS,),
        in_specs=[
            pl.BlockSpec(memory_space=pltpu.SMEM),
            rows_spec,
            step_spec(grad.shape),
            *[whole_spec(x) for x in weights],
            *[step_spec(x.shape) for x in steps],
            *[whole_spec(x) for x in wholes],
        ],
        out_specs=[whole_spec(sent), whole_spec(bias_out)],
        out_shape=[sent, bias_out],
        scratch_shapes=scratch,
        compiler_params=pltpu.CompilerParams(dimension_semantics=("arbitrary",)),
        interpret=INTERPRET,
        name="backward_second" if second else "backward_first",
    )(own_class, rows, grad, *weights, *steps, *wholes)


def finish_kernel(share_rows, heads, arrived_ref, proj_ref, gate_ref, out_ref, bias_ref, gain_ref,
                  shift_ref):
    channels = out_ref.shape[1]
    classes = arrived_ref.shape[0]
    small = jnp.sum(arrived_ref[:, 2 * share_rows :].astype(jnp.float32), axis=0)
    main = 5 * channels
    for block in range(2):
        start = block * share_rows
        whole = arrived_ref[:, start : start + share_rows].astype(jnp.float32)
        whole = whole.reshape(classes * share_rows, channels)
        proj_ref[block] = whole[: 4 * channels]
        out_ref[block] = whole[4 * channels : main]
        gate_ref[block : block + 1] = whole[main : main + 1]
        if block == 0:
            late = whole[main + 1 : main + 1 + heads + 2]
        parts = late if block else small[: heads + 2]
        bias_ref[block] = parts[:heads]
        gain_ref[block : block + 1] = parts[heads : heads + 1]
        shift_ref[block : block + 1] = parts[heads + 1 : heads + 2]


def finish_call(arrived, share_rows, heads, channels):
    shapes = [(2, 4 * channels, channels), (2, channels), (2, channels, channels)]
    shapes += [(2, heads, channels), (2, channels), (2, channels)]
    vmem = pl.BlockSpec(memory_space=pltpu.VMEM)
    return pl.pallas_call(
        functools.partial(finish_kernel, share_rows, heads),
        in_specs=[vmem],
        out_specs=[vmem] * len(shapes),
        out_shape=[jax.ShapeDtypeStruct(shape, jnp.float32) for shape in shapes],
        interpret=INTERPRET,
        name="finish_weights",
    )(arrived)


def padded_rows(x, rows):
    return jnp.pad(x, ((0, 0),) * (x.ndim - 2) + ((0, rows - x.shape[-2]), (0, 0)))


def rounded_up(value, step):
    return -(-value // step) * step


def local(
    pair_input,
    cotangent,
    residue_mask,
    norm_gain,
    norm_shift,
    proj_weights,
    gate_bias,
    out_weights,
    bias_weights,
):
    channels = pair_input.shape[2]
    groups = lax.axis_size("row")
    classes = lax.axis_size(HEAD)
    positions = groups * classes
    head_total = bias_weights.shape[2]
    bias_rows = head_total * positions // LANES
    half = jnp.bfloat16
    key_bias = (residue_mask.astype(jnp.float32) - 1.0) * MASKED
    key_bias = key_bias.reshape(groups, classes).T.reshape(1, positions)
    own_class = lax.axis_index(HEAD).astype(jnp.int32).reshape(1)
    main_rows = 5 * channels + 1
    share_rows = rounded_up(-(-(main_rows + head_total + 2) // classes), 16)
    group_rows = rounded_up(share_rows, groups) // groups
    params = [
        (
            norm_gain[which],
            norm_shift[which],
            proj_weights[which],
            gate_bias[which],
            out_weights[which],
            bias_weights[which],
        )
        for which in range(2)
    ]

    row_parts, normed_flat, inverse_flat, *parts = start_call(
        own_class, pair_input[0], cotangent[0], params[0], head_total, classes
    )
    normal_flat = parts[0][:positions]
    pieces = shifted_exchange(parts)
    first_rows = placed(own_class, pieces)
    cotangent_query = first_rows[:, positions + groups :]
    arrived = exchanged(row_parts, "row")
    first_bias = arrived[:, :bias_rows].reshape(groups, head_total * positions)
    second_grad_query = arrived[:, bias_rows:].transpose(1, 0, 2)

    after_query, after_normal, *first_saved = forward_call(
        own_class, first_rows, first_bias, key_bias, params[0], params[1], head_total, positions
    )
    after_normed, after_inverse, _ = layer_norm(after_query, norm_gain[1], norm_shift[1])
    second_bias_own = jnp.einsum(
        "abc,ch->ahb", after_normal, bias_weights[1], preferred_element_type=jnp.float32
    ).astype(half)
    after_own = exchanged(after_normal, HEAD)
    arrived = exchanged(
        jnp.concatenate(
            [
                to_all(second_bias_own.reshape(bias_rows, LANES), "row"),
                after_own.transpose(1, 0, 2),
            ],
            axis=1,
        ),
        "row",
    )
    second_bias = (
        arrived[:, :bias_rows]
        .reshape(groups, classes, head_total * groups)
        .transpose(1, 0, 2)
        .reshape(positions, head_total * groups)
    )
    second_query = arrived[:, bias_rows:].transpose(1, 0, 2)
    second_rows = exchanged(to_all(second_query, HEAD), HEAD)
    sent, bias_parts = backward_call(
        own_class,
        second_rows.reshape(classes, classes, groups, channels),
        second_grad_query,
        params[1],
        head_total,
        positions,
        share_rows,
        (),
        (second_bias, key_bias),
    )

    def group_shares_of(arrived_shares):
        summed = jnp.sum(arrived_shares.astype(jnp.float32), axis=0)
        summed = padded_rows(summed, groups * group_rows).astype(half)
        return summed.reshape(groups, group_rows, LANES)

    arrived = exchanged(sent, HEAD)
    second_shares = group_shares_of(arrived[:, positions:])
    grad_flipped = jnp.sum(arrived[:, :positions].astype(jnp.float32), axis=0).astype(half)
    bias_parts = (
        bias_parts.reshape(classes, groups, head_total * groups)
        .transpose(1, 0, 2)
        .reshape(groups, bias_rows, LANES)
    )
    arrived = exchanged(
        jnp.concatenate(
            [
                bias_parts,
                grad_flipped.reshape(classes, groups, channels).transpose(1, 0, 2),
            ],
            axis=1,
        ),
        "row",
    )
    summed = jnp.sum(arrived[:, :bias_rows].astype(jnp.float32), axis=0)
    second_bias_half = summed.reshape(classes, head_total, groups).astype(half)
    grad_query = exchanged(arrived[:, bias_rows : bias_rows + classes].transpose(1, 0, 2), HEAD)
    grad_normal = grad_query.astype(jnp.float32) + jnp.einsum(
        "ahb,ch->abc", second_bias_half, bias_weights[1], preferred_element_type=jnp.float32
    )
    end_query = norm_backward(grad_normal, after_normed, after_inverse, norm_gain[1]).astype(half)
    second_small = jnp.concatenate(
        [
            jnp.einsum(
                "abc,ahb->hc", after_normal, second_bias_half, preferred_element_type=jnp.float32
            ),
            jnp.sum(grad_normal * after_normed, axis=(0, 1))[None],
            jnp.sum(grad_normal, axis=(0, 1))[None],
        ],
        axis=0,
    )

    after_grad_query = (
        cotangent_query.astype(jnp.float32) + end_query.astype(jnp.float32)
    ).astype(half)
    extra = jnp.pad(second_small, ((1, 7 - second_small.shape[0]), (0, 0)))
    sent, bias_parts = backward_call(
        own_class,
        first_rows,
        after_grad_query,
        params[0],
        head_total,
        positions,
        share_rows,
        tuple(first_saved),
        (extra, end_query),
    )
    arrived = exchanged(sent, HEAD)
    grad_normal = jnp.sum(arrived[:, :positions].astype(jnp.float32), axis=0)
    end_own = arrived[:, positions : positions + groups]
    shares = arrived[:, positions + groups :]
    arrived = exchanged(
        jnp.concatenate(
            [
                bias_parts.reshape(groups, bias_rows, LANES),
                padded_rows(
                    jnp.concatenate([group_shares_of(shares), second_shares], axis=1),
                    rounded_up(2 * group_rows, 8),
                ),
            ],
            axis=1,
        ),
        "row",
    )
    summed = jnp.sum(arrived[:, :bias_rows].astype(jnp.float32), axis=0)
    bias_half = summed.reshape(head_total, positions).astype(half)
    shares_total = jnp.sum(
        arrived[:, bias_rows : bias_rows + 2 * group_rows].astype(jnp.float32), axis=0
    )
    grad_normal = grad_normal + jnp.einsum(
        "hn,ch->nc", bias_half, bias_weights[0], preferred_element_type=jnp.float32
    )
    start_grad = norm_backward(
        grad_normal, normed_flat, inverse_flat, norm_gain[0]
    )
    moved_grad = (end_own.astype(jnp.float32) + start_grad.reshape(end_own.shape)).transpose(1, 0, 2)
    pair_grad = cotangent.astype(jnp.float32) + moved_grad.reshape(1, positions, channels)
    first_small = jnp.concatenate(
        [
            jnp.einsum("nc,hn->hc", normal_flat, bias_half, preferred_element_type=jnp.float32),
            jnp.sum(grad_normal * normed_flat, axis=0)[None],
            jnp.sum(grad_normal, axis=0)[None],
        ],
        axis=0,
    )

    small_rows = first_small.shape[0]
    tail = jnp.concatenate([shares_total, first_small], axis=0).astype(half)
    tail = padded_rows(tail, rounded_up(tail.shape[0], 8))
    arrived = exchanged(to_all(tail, "row"), "row")
    whole_rows = groups * group_rows
    shared = jnp.concatenate(
        [
            arrived[:, :group_rows].reshape(whole_rows, LANES)[:share_rows],
            arrived[:, group_rows : 2 * group_rows].reshape(whole_rows, LANES)[:share_rows],
            padded_rows(
                jnp.sum(
                    arrived[:, 2 * group_rows : 2 * group_rows + small_rows].astype(jnp.float32),
                    axis=0,
                ).astype(half),
                rounded_up(small_rows, 8),
            ),
        ],
        axis=0,
    )
    arrived = exchanged(to_all(shared, HEAD), HEAD)
    proj_grad, gate_grad, out_grad, bias_grad, gain_grad, shift_grad = finish_call(
        arrived, share_rows, head_total, channels
    )
    return (
        pair_grad,
        proj_grad.reshape(2, 4, channels, -1),
        gate_grad,
        out_grad,
        bias_grad.transpose(0, 2, 1),
        gain_grad,
        shift_grad,
    )


def solution(mesh):
    finer = Mesh(mesh.devices.reshape(mesh.shape["row"], 4, 2), ("row", "head_0", "head_1"))
    in_specs = (P(ROW_HEAD, None, None), P(ROW_HEAD, None, None), P(), P(), P(), P(), P(), P(), P())
    out_specs = (P(ROW_HEAD, None, None), P(), P(), P(), P(), P(), P())

    return jax.shard_map(local, mesh=finer, in_specs=in_specs, out_specs=out_specs, check_vma=False)
```
